256 devices in a mesh: gx: 32 (over z, x), gy: 8 (over y, core).
Axes of the slice: x: 4, y: 4, z: 8, core: 2. Of those that a mesh axis runs over, the one named last changes fastest.
Arguments:
- fine_disp: float32 [3, 512, 128, 128], P(None, 'gx', 'gy'), may hold values from -12 to 12
- fine_prev: float32 [3, 512, 128, 128], P(None, 'gx', 'gy'), may hold values from -12 to 12
- coarse_disp: float32 [3, 256, 64, 256], P(None, 'gx', 'gy'), may hold values from -12 to 12
- coarse_prev: float32 [3, 256, 64, 256], P(None, 'gx', 'gy'), may hold values from -12 to 12
- fine_density: float32 [512, 128, 128], P('gx', 'gy'), may hold values from 0.6 to 1.8
- fine_lame: float32 [512, 128, 128], P('gx', 'gy'), may hold values from 0.5 to 2
- fine_rigidity: float32 [512, 128, 128], P('gx', 'gy'), may hold values from 0.3 to 1.5
- fine_metric: float32 [512, 128, 128], P('gx', 'gy'), may hold values from 0.7 to 1.4
- coarse_density: float32 [256, 64, 256], P('gx', 'gy'), may hold values from 0.6 to 1.8
- coarse_lame: float32 [256, 64, 256], P('gx', 'gy'), may hold values from 0.5 to 2
- coarse_rigidity: float32 [256, 64, 256], P('gx', 'gy'), may hold values from 0.3 to 1.5
- coarse_metric: float32 [256, 64, 256], P('gx', 'gy'), may hold values from 0.7 to 1.4
- offsets: int32 [2, 512, 128], P(None, 'gx', 'gy'), may hold values from -1 to 1
Outputs:
- fine_final: float32 [3, 512, 128, 128], P(None, 'gx', 'gy')
- coarse_final: float32 [3, 256, 64, 256], P(None, 'gx', 'gy')
- energy: float32 [3, 2], replicated
The draws below stay inside these ranges and needn't reach their ends.
All inputs are finite; a program needn't handle non-finite values.
Results may differ from the reference program's by a relative error of at most 0.00021.
Values sent between devices are 32-bit elements; how exact they have to be, the bound alone decides.
A program may use at most 64 MiB of HBM per device.

```python
import math
import jax
import jax.numpy as jnp

FZ = 128
STEPS = 3
CZ = 256
NXF = 512
NYF = 128
NXC = 256
NYC = 64


def rough_field(key, cells_x, cells_y, cells_z):
    key_scale, key_rough, key_common = jax.random.split(key, 3)
    blocks_x = (cells_x + 7) // 8
    blocks_y = (cells_y + 7) // 8
    log_scale = jax.random.uniform(key_scale, (blocks_x, blocks_y), jnp.float32, -1.1, 1.1)
    rough_part = jax.random.truncated_normal(key_rough, -4.0, 4.0, (3, cells_x, cells_y, cells_z), jnp.float32)
    amplitude = jnp.repeat(jnp.repeat(jnp.exp(log_scale), 8, axis=0), 8, axis=1)[:cells_x, :cells_y]
    return jnp.clip(rough_part * amplitude[None, :, :, None], -12.0, 12.0)


def draw_fine_disp(key, part):
    return rough_field(jax.random.fold_in(key, 11), NXF, NYF, FZ)


def draw_fine_prev(key, part):
    return rough_field(jax.random.fold_in(key, 12), NXF, NYF, FZ)


def draw_coarse_disp(key, part):
    return rough_field(jax.random.fold_in(key, 13), NXC, NYC, CZ)


def draw_coarse_prev(key, part):
    return rough_field(jax.random.fold_in(key, 14), NXC, NYC, CZ)


def touch_ends(drawn, key, least, top_value):
    spot = [jax.random.randint(jax.random.fold_in(key, axis), (), 0, length) for axis, length in enumerate(drawn.shape)]
    main_axis = drawn.shape.index(max(drawn.shape))
    next_to = spot[:main_axis] + [(spot[main_axis] + 1) % drawn.shape[main_axis]] + spot[main_axis + 1:]
    return drawn.at[tuple(spot)].set(least).at[tuple(next_to)].set(top_value)


def block_scale(own_key, shape, shards, least, top_value):
    loudness = 1.0
    for position, parts in shards:
        steps = jax.random.uniform(jax.random.fold_in(jax.random.fold_in(own_key, 6), position), (parts,), jnp.float32, least / len(shards), top_value / len(shards))
        loudness = loudness * jnp.repeat(jnp.exp(steps), shape[position] // parts).reshape((-1,) + (1,) * (len(shape) - 1 - position))
    return loudness


def setup_inputs(seed: int = 0) -> dict:
    key_of = jax.random.split(jax.random.key(seed), 14)
    return {
        "fine_disp": draw_fine_disp(jax.random.fold_in(key_of[13], 71), 0),
        "fine_prev": draw_fine_prev(jax.random.fold_in(key_of[13], 71), 0),
        "coarse_disp": draw_coarse_disp(jax.random.fold_in(key_of[13], 71), 0),
        "coarse_prev": draw_coarse_prev(jax.random.fold_in(key_of[13], 71), 0),
        "fine_density": jnp.clip(jnp.exp(math.log(1.8) - 1.0986122 * jax.random.uniform(key_of[4], (NXF, NYF, FZ), jnp.float32) ** block_scale(key_of[4], (NXF, NYF, FZ), ((0, 32), (1, 8)), -0.2, 0.2)), 0.6, 1.8),
        "fine_lame": jnp.clip(jnp.exp(math.log(2.0) - 1.3862944 * jax.random.uniform(key_of[5], (NXF, NYF, FZ), jnp.float32) ** block_scale(key_of[5], (NXF, NYF, FZ), ((0, 32), (1, 8)), -0.2, 0.2)), 0.5, 2.0),
        "fine_rigidity": jnp.clip(jnp.exp(math.log(1.5) - 1.60943787 * jax.random.uniform(key_of[6], (NXF, NYF, FZ), jnp.float32) ** block_scale(key_of[6], (NXF, NYF, FZ), ((0, 32), (1, 8)), -0.2, 0.2)), 0.3, 1.5),
        "fine_metric": jnp.clip(jnp.exp(math.log(1.4) - 0.6931472 * jax.random.uniform(key_of[7], (NXF, NYF, FZ), jnp.float32) ** block_scale(key_of[7], (NXF, NYF, FZ), ((0, 32), (1, 8)), -0.2, 0.2)), 0.7, 1.4),
        "coarse_density": jnp.clip(jnp.exp(math.log(1.8) - 1.0986122 * jax.random.uniform(key_of[8], (NXC, NYC, CZ), jnp.float32) ** block_scale(key_of[8], (NXC, NYC, CZ), ((0, 32), (1, 8)), -0.2, 0.2)), 0.6, 1.8),
        "coarse_lame": jnp.clip(jnp.exp(math.log(2.0) - 1.3862944 * jax.random.uniform(key_of[9], (NXC, NYC, CZ), jnp.float32) ** block_scale(key_of[9], (NXC, NYC, CZ), ((0, 32), (1, 8)), -0.2, 0.2)), 0.5, 2.0),
        "coarse_rigidity": jnp.clip(jnp.exp(math.log(1.5) - 1.60943787 * jax.random.uniform(key_of[10], (NXC, NYC, CZ), jnp.float32) ** block_scale(key_of[10], (NXC, NYC, CZ), ((0, 32), (1, 8)), -0.2, 0.2)), 0.3, 1.5),
        "coarse_metric": jnp.clip(jnp.exp(math.log(1.4) - 0.6931472 * jax.random.uniform(key_of[11], (NXC, NYC, CZ), jnp.float32) ** block_scale(key_of[11], (NXC, NYC, CZ), ((0, 32), (1, 8)), -0.2, 0.2)), 0.7, 1.4),
        "offsets": touch_ends(jax.random.randint(key_of[12], (2, NXF, NYF), -1, 2), jax.random.fold_in(key_of[12], 1), -1, 1).astype(jnp.int32),
    }


step_factor = 0.15


def vertical_slope(values):
    middle = 0.5 * (values[..., 2:] - values[..., :-2])
    first = values[..., 1:2] - values[..., 0:1]
    final = values[..., -1:] - values[..., -2:-1]
    return jnp.concatenate([first, middle, final], axis=-1)


def divergence(along_x, along_y, along_z, inverse):
    return 0.5 * (along_x[2:] - along_x[:-2]) + 0.5 * (along_y[:, 2:] - along_y[:, :-2]) + inverse * vertical_slope(along_z)


def interpolate(plane_ext, offsets):
    coarse_x = plane_ext.shape[1] - 4
    coarse_y = plane_ext.shape[2] - 4
    near_x = jnp.where((jnp.arange(2 * coarse_x) % 2) == 0, 0.75, 0.25)[:, None]
    near_y = jnp.where((jnp.arange(2 * coarse_y) % 2) == 0, 0.75, 0.25)[None, :]
    offset_x = offsets[0]
    offset_y = offsets[1]
    summed = jnp.zeros((3, 2 * coarse_x, 2 * coarse_y), plane_ext.dtype)
    for shift_x in (-1, 0, 1, 2):
        weight_x = jnp.where(offset_x == shift_x, near_x, 0.0) + jnp.where(offset_x + 1 == shift_x, 1.0 - near_x, 0.0)
        row_band = jnp.repeat(plane_ext[:, 2 + shift_x:2 + shift_x + coarse_x, :], 2, axis=1)
        for shift_y in (-1, 0, 1, 2):
            weight_y = jnp.where(offset_y == shift_y, near_y, 0.0) + jnp.where(offset_y + 1 == shift_y, 1.0 - near_y, 0.0)
            tile_band = jnp.repeat(row_band[:, :, 2 + shift_y:2 + shift_y + coarse_y], 2, axis=2)
            summed = summed + (weight_x * weight_y)[None] * tile_band
    return summed


def restrict(plane):
    half_x = plane.shape[1] // 2
    half_y = plane.shape[2] // 2
    return 0.25 * jnp.sum(plane.reshape(3, half_x, 2, half_y, 2), axis=(2, 4))


def elastic_rate(extended, mats_ext, div_ext, displace, top_ghost, bottom_ghost, density, lame_first, rigidity):
    wide_ext = mats_ext[0]
    inverse = mats_ext[1, 1:-1, 1:-1]
    face_x = 0.5 * (wide_ext[:-1, 1:-1] + wide_ext[1:, 1:-1])
    flux_x = face_x * (extended[:, 1:, 1:-1] - extended[:, :-1, 1:-1])
    face_y = 0.5 * (wide_ext[1:-1, :-1] + wide_ext[1:-1, 1:])
    flux_y = face_y * (extended[:, 1:-1, 1:] - extended[:, 1:-1, :-1])
    vertical = rigidity * inverse
    face_z = jnp.concatenate([vertical[:, :, :1], 0.5 * (vertical[:, :, :-1] + vertical[:, :, 1:]), vertical[:, :, -1:]], axis=2)
    column = jnp.concatenate([top_ghost[:, :, :, None], displace, bottom_ghost[:, :, :, None]], axis=3)
    flux_z = face_z * (column[:, :, :, 1:] - column[:, :, :, :-1])
    spread = (flux_x[:, 1:] - flux_x[:, :-1]) + (flux_y[:, :, 1:] - flux_y[:, :, :-1]) + (flux_z[:, :, :, 1:] - flux_z[:, :, :, :-1])
    grad_x = 0.5 * (div_ext[2:, 1:-1] - div_ext[:-2, 1:-1])
    grad_y = 0.5 * (div_ext[1:-1, 2:] - div_ext[1:-1, :-2])
    grad_z = inverse * vertical_slope(div_ext[1:-1, 1:-1])
    gradient = jnp.stack([grad_x, grad_y, grad_z])
    return spread * (inverse / density) + ((lame_first + rigidity) / density) * gradient


def energy_part(updated, displace, rate, density, metric, cell_count):
    change = updated - displace
    inner_sum = jnp.sum(change * change - step_factor * updated * rate, axis=0)
    return jnp.sum(density * metric * inner_sum) / cell_count


def reference(fine_disp, fine_prev, coarse_disp, coarse_prev, fine_density, fine_lame, fine_rigidity, fine_metric, coarse_density, coarse_lame, coarse_rigidity, coarse_metric, offsets):
    pad_cells = ((1, 1), (1, 1), (0, 0))
    pad_fields = ((0, 0), (1, 1), (1, 1), (0, 0))
    fine_mats = jnp.pad(jnp.stack([fine_rigidity * fine_metric, 1.0 / fine_metric]), pad_fields)
    coarse_mats = jnp.pad(jnp.stack([coarse_rigidity * coarse_metric, 1.0 / coarse_metric]), pad_fields)
    fine_cells = fine_disp.shape[1] * fine_disp.shape[2] * fine_disp.shape[3]
    coarse_cells = coarse_disp.shape[1] * coarse_disp.shape[2] * coarse_disp.shape[3]
    energies = []
    for step_index in range(STEPS):
        fine_ext = jnp.pad(fine_disp, pad_fields)
        coarse_ext = jnp.pad(coarse_disp, pad_fields)
        fine_div = divergence(fine_ext[0, :, 1:-1], fine_ext[1, 1:-1, :], fine_disp[2], fine_mats[1, 1:-1, 1:-1])
        coarse_div = divergence(coarse_ext[0, :, 1:-1], coarse_ext[1, 1:-1, :], coarse_disp[2], coarse_mats[1, 1:-1, 1:-1])
        fine_div_ext = jnp.pad(fine_div, pad_cells)
        coarse_div_ext = jnp.pad(coarse_div, pad_cells)
        plane_ext = jnp.pad(coarse_disp[:, :, :, 0], ((0, 0), (2, 2), (2, 2)))
        fine_bottom = interpolate(plane_ext, offsets)
        fine_top = fine_disp[:, :, :, 0]
        coarse_top = restrict(fine_disp[:, :, :, -1])
        coarse_bottom = jnp.zeros_like(coarse_top)
        fine_rate = elastic_rate(fine_ext, fine_mats, fine_div_ext, fine_disp, fine_top, fine_bottom, fine_density, fine_lame, fine_rigidity)
        coarse_rate = elastic_rate(coarse_ext, coarse_mats, coarse_div_ext, coarse_disp, coarse_top, coarse_bottom, coarse_density, coarse_lame, coarse_rigidity)
        fine_new = 2.0 * fine_disp - fine_prev + step_factor * fine_rate
        coarse_new = 2.0 * coarse_disp - coarse_prev + step_factor * coarse_rate
        energies.append(jnp.stack([
            energy_part(fine_new, fine_disp, fine_rate, fine_density, fine_metric, fine_cells),
            energy_part(coarse_new, coarse_disp, coarse_rate, coarse_density, coarse_metric, coarse_cells)]))
        fine_prev, fine_disp = fine_disp, fine_new
        coarse_prev, coarse_disp = coarse_disp, coarse_new
    return (fine_disp, coarse_disp, jnp.stack(energies))
```

```python
import functools

import jax
import jax.numpy as jnp
from jax import lax
from jax.experimental import pallas as pl
from jax.experimental.pallas import tpu as pltpu
from jax.sharding import PartitionSpec as P

STEPS = 3
DT = 0.15
MESH = pl.DeviceIdType.MESH
F32 = jnp.float32

R = 2
LO, HI = 0, 1
(WIDE, HALF_A, ISV, GB, GZ, DM, CZU, CZD, CXP, CXM, CYU, CYD, C0) = range(13)
NCOEF = 13


def lanes(shape):
    return lax.broadcasted_iota(jnp.int32, shape, len(shape) - 1)


def subs(shape):
    return lax.broadcasted_iota(jnp.int32, shape, len(shape) - 2)


def spread_row(row):
    return jnp.broadcast_to(row, (8, 128))


def roll(x, shift, axis):
    return pltpu.roll(x, shift % x.shape[axis], axis)


class Fine:
    n = 16
    key = "f"

    @staticmethod
    def load(ref, i, r):
        parts = [ref[pl.ds(16 * i + t, 8 * r, stride=2), :].reshape(1, r, 8, 128) for t in (0, 1)]
        return jnp.concatenate(parts, axis=0)

    @staticmethod
    def store(ref, i, r, value):
        for t in (0, 1):
            ref[pl.ds(16 * i + t, 8 * r, stride=2), :] = value[t].reshape(8 * r, 128)

    @staticmethod
    def k_up(x, last=None):
        moved = roll(x, -1, 3)
        edge = x if last is None else last
        return jnp.where(lanes(x.shape) == 127, edge, moved)

    @staticmethod
    def k_down(x, first=None):
        moved = roll(x, 1, 3)
        edge = x if first is None else first
        return jnp.where(lanes(x.shape) == 0, edge, moved)

    @staticmethod
    def edge_scale(shape):
        k = lanes(shape)
        return jnp.where((k == 0) | (k == 127), 1.0, 0.5).astype(F32)

    @staticmethod
    def row_of(ref, i, r):
        return jnp.concatenate(
            [spread_row(ref[pl.ds(i + m, 1), :]).reshape(1, 8, 128) for m in range(r)], axis=0
        )

    @staticmethod
    def j_up(x, halo):
        s = subs(x.shape[1:])
        moved = jnp.where(s == 7, halo, roll(x[0], -1, 1))
        return jnp.stack([x[1], moved])

    @staticmethod
    def j_down(x, halo):
        s = subs(x.shape[1:])
        moved = jnp.where(s == 0, halo, roll(x[1], 1, 1))
        return jnp.stack([moved, x[0]])

    @staticmethod
    def plane(ref, j):
        return jnp.concatenate([ref[pl.ds(j + 128 * h, 8, stride=16), :] for h in (0, 1)], axis=0)

    @staticmethod
    def plane_k_up(x):
        return jnp.where(lanes(x.shape) == 127, x, roll(x, -1, 1))

    @staticmethod
    def plane_k_down(x):
        return jnp.where(lanes(x.shape) == 0, x, roll(x, 1, 1))

    @staticmethod
    def corner(tile_ref, comp):
        return spread_row(tile_ref[pl.ds(comp, 1), :])

    @staticmethod
    def corner_plane(tile_ref, comp):
        row = spread_row(tile_ref[pl.ds(comp, 1), :])
        return jnp.concatenate([row, row], axis=0)

    @staticmethod
    def corner_row(tile_ref, comp):
        return spread_row(tile_ref[pl.ds(comp, 1), :]).reshape(1, 8, 128)


class Coarse:
    n = 8
    key = "c"

    @staticmethod
    def load(ref, i, r):
        return ref[:, pl.ds(8 * i, 8 * r), :].reshape(2, r, 8, 128)

    @staticmethod
    def store(ref, i, r, value):
        ref[:, pl.ds(8 * i, 8 * r), :] = value.reshape(2, 8 * r, 128)

    @staticmethod
    def k_up(x, last=None):
        moved = roll(x, -1, 3)
        edge = x[1] if last is None else last
        return jnp.where(lanes(x.shape) == 127, jnp.stack([moved[1], edge]), moved)

    @staticmethod
    def k_down(x, first=None):
        moved = roll(x, 1, 3)
        edge = x[0] if first is None else first
        return jnp.where(lanes(x.shape) == 0, jnp.stack([edge, moved[0]]), moved)

    @staticmethod
    def edge_scale(shape):
        k = lanes(shape)
        half = lax.broadcasted_iota(jnp.int32, shape, 0)
        ends = ((k == 0) & (half == 0)) | ((k == 127) & (half == 1))
        return jnp.where(ends, 1.0, 0.5).astype(F32)

    @staticmethod
    def row_of(ref, i, r):
        halves = []
        for h in (0, 1):
            rows = [spread_row(ref[h, pl.ds(i + m, 1), :]).reshape(1, 8, 128) for m in range(r)]
            halves.append(jnp.concatenate(rows, axis=0))
        return jnp.stack(halves)

    @staticmethod
    def j_up(x, halo):
        return jnp.where(subs(x.shape) == 7, halo, roll(x, -1, 2))

    @staticmethod
    def j_down(x, halo):
        return jnp.where(subs(x.shape) == 0, halo, roll(x, 1, 2))

    @staticmethod
    def plane(ref, j):
        return jnp.stack([ref[h, pl.ds(j, 8, stride=8), :] for h in (0, 1)])

    @staticmethod
    def plane_k_up(x):
        return Coarse.k_up(x[:, None])[:, 0]

    @staticmethod
    def plane_k_down(x):
        return Coarse.k_down(x[:, None])[:, 0]

    @staticmethod
    def corner_plane(tile_ref, comp):
        return jnp.stack([spread_row(tile_ref[pl.ds(2 + 2 * comp + h, 1), :]) for h in (0, 1)])

    @staticmethod
    def corner_row(tile_ref, comp):
        rows = [spread_row(tile_ref[pl.ds(2 + 2 * comp + h, 1), :]) for h in (0, 1)]
        return jnp.stack(rows)[:, None]


def plane_roll(level, x, shift):
    return roll(x, shift, 0) if level is Fine else roll(x, shift, 1)


def plane_sub(level, x):
    return subs(x.shape)


def neighbour_rows(level, ref, i, r, step, halo):
    if step > 0:
        if i + r < level.n:
            return level.load(ref, i + 1, r)
        return jnp.concatenate([level.load(ref, i + 1, r - 1), halo()], axis=1)
    if i > 0:
        return level.load(ref, i - 1, r)
    return jnp.concatenate([halo(), level.load(ref, 0, r - 1)], axis=1)


def kernel(nx, ny, group_x, *refs):
    names_in = (
        "fine_disp fine_prev coarse_disp coarse_prev fine_density fine_lame fine_rigidity"
        " fine_metric coarse_density coarse_lame coarse_rigidity coarse_metric"
    ).split()
    hbm = dict(zip(names_in, refs[:12]))
    offsets_ref = refs[12]
    fine_out, coarse_out, energy_out = refs[13:16]
    (
        uf, uc, matf, matc, kf, kc, dvf, dvc, dyf, dyc,
        xhf, xhc, yhf, yhc, ysf, ysc, xmf, xmc, ymf, ymc, ysmf, ysmc,
        pls, plx, ply, cos, cor, weights, ghost, eacc, erow, er1, er2,
        load_sem, out_sem, send_sem, recv_sem, esend, erecv,
    ) = refs[16:]

    gx, gy = lax.axis_index("gx"), lax.axis_index("gy")
    exists = {
        (dx, dy): functools.reduce(
            jnp.logical_and,
            ([gx > 0] if dx < 0 else [gx < nx - 1] if dx > 0 else [])
            + ([gy > 0] if dy < 0 else [gy < ny - 1] if dy > 0 else []),
        )
        for dx in (-1, 0, 1)
        for dy in (-1, 0, 1)
        if (dx, dy) != (0, 0)
    }
    directions = list(exists)
    corners = [d for d in directions if d[0] and d[1]]
    corner_id = {d: n for n, d in enumerate(corners)}

    def flag(direction):
        return jnp.where(exists[direction], 1.0, 0.0).astype(F32)

    def device(direction):
        return {"gx": gx + direction[0], "gy": gy + direction[1]}

    groups = nx // group_x
    gx_hi, gx_lo = gx // group_x, gx % group_x
    n1, n2 = group_x * ny, groups
    me1 = gx_lo * ny + gy

    def peer1(d):
        q = lax.rem(me1 + d, n1)
        return {"gx": gx_hi * group_x + q // ny, "gy": q % ny}

    def peer2(d):
        return {"gx": lax.rem(gx_hi + d, n2) * group_x + gx_lo, "gy": gy}

    barrier = pltpu.get_barrier_semaphore()
    for d in directions:
        @pl.when(exists[d])
        def _(d=d):
            pl.semaphore_signal(barrier, inc=1, device_id=device(d), device_id_type=MESH)

    @pl.loop(1, n1)
    def _(d):
        pl.semaphore_signal(barrier, inc=1, device_id=peer1(d), device_id_type=MESH)

    if n2 > 1:
        @pl.loop(1, n2)
        def _(d):
            pl.semaphore_signal(barrier, inc=1, device_id=peer2(d), device_id_type=MESH)

    loads = {}

    def start_load(name, dst, sem):
        fine = name.startswith("fine")
        src = hbm[name]
        if fine:
            copies = [pltpu.make_async_copy(src, dst, load_sem.at[sem, 0])]
        else:
            lead = (slice(None),) * (len(src.shape) - 2)
            copies = [
                pltpu.make_async_copy(
                    src.at[lead + (slice(None), pl.ds(128 * h, 128))],
                    dst.at[(slice(None), h) if lead else (h,)],
                    load_sem.at[sem, h],
                )
                for h in (0, 1)
            ]
        for c in copies:
            c.start()
        loads[name] = copies

    plan = [
        ("fine_disp", uf.at[1]), ("coarse_disp", uc.at[1]),
        ("fine_rigidity", matf.at[0]), ("coarse_rigidity", matc.at[0]),
        ("fine_metric", matf.at[1]), ("coarse_metric", matc.at[1]),
        ("fine_density", matf.at[2]), ("fine_lame", matf.at[3]),
        ("coarse_density", matc.at[2]), ("coarse_lame", matc.at[3]),
        ("fine_prev", uf.at[0]), ("coarse_prev", uc.at[0]),
    ]
    for sem, (name, dst) in enumerate(plan):
        start_load(name, dst, sem)

    def wait_load(*names):
        for name in names:
            for c in loads[name]:
                c.wait()

    side_of = {-1: LO, 1: HI}

    def messages(s):
        out = []
        u_f, u_c = uf.at[s + 1], uc.at[s + 1]
        for dx in (-1, 1):
            own, far = side_of[dx], side_of[-dx]
            first, second = (0, 1) if dx < 0 else (15, 14)
            out.append(("fx", (dx, 0), u_f.at[:, pl.ds(16 * first, 16)], xhf.at[s, far, pl.ds(0, 3)]))
            out.append(("fx", (dx, 0), u_f.at[0, pl.ds(16 * second, 16)], xhf.at[s, far, 3]))
            first, second = (0, 1) if dx < 0 else (7, 6)
            out.append(("cx", (dx, 0), u_c.at[:, :, pl.ds(8 * first, 8)], xhc.at[s, far, pl.ds(0, 3)]))
            out.append(("cx", (dx, 0), u_c.at[0, :, pl.ds(8 * second, 8)], xhc.at[s, far, 3]))
            out.append(("cp", (dx, 0), pls.at[s], plx.at[s, far]))
            if s == 0:
                first = 0 if dx < 0 else 15
                out.append(("mx", (dx, 0), matf.at[pl.ds(0, 2), pl.ds(16 * first, 16)], xmf.at[far]))
                first = 0 if dx < 0 else 7
                out.append(("mx", (dx, 0), matc.at[pl.ds(0, 2), :, pl.ds(8 * first, 8)], xmc.at[far]))
        for dy in (-1, 1):
            own, far = side_of[dy], side_of[-dy]
            out.append(("fy", (0, dy), ysf.at[s, own], yhf.at[s, far]))
            out.append(("cy", (0, dy), ysc.at[s, own], yhc.at[s, far]))
            out.append(("cp", (0, dy), pls.at[s], ply.at[s, far]))
            if s == 0:
                out.append(("my", (0, dy), ysmf.at[own], ymf.at[far]))
                out.append(("my", (0, dy), ysmc.at[own], ymc.at[far]))
        for d in corners:
            back = corner_id[(-d[0], -d[1])]
            out.append(("co", d, cos.at[s, corner_id[d]], cor.at[s, back]))
        return out

    copies = []
    for s in range(STEPS):
        entries = []
        for n, (group, d, src, dst) in enumerate(messages(s)):
            def copy(src=src, dst=dst, s=s, n=n, d=d):
                return pltpu.make_async_remote_copy(
                    src_ref=src, dst_ref=dst,
                    send_sem=send_sem.at[s, n], recv_sem=recv_sem.at[s, n],
                    device_id=device(d), device_id_type=MESH,
                )

            entries.append((group, d, copy))
        copies.append(entries)

    def run(s, groups_wanted, what, backwards=False):
        for d in directions:
            mine = [c for g, e, c in copies[s] if g in groups_wanted and e == d]
            if mine:
                @pl.when(exists[(-d[0], -d[1]) if backwards else d])
                def _(mine=mine):
                    for c in mine:
                        getattr(c(), what)()

    def send(s, *wanted):
        run(s, wanted, "start")

    def receive(s, *wanted):
        run(s, wanted, "wait_recv", backwards=True)

    def pack_y(level, s):
        u, out = (uf, ysf) if level is Fine else (uc, ysc)
        last = 15 if level is Fine else 7
        for side, (j0, j1) in ((LO, (0, 1)), (HI, (last, last - 1))):
            for c in range(3):
                out[s, side, c] = level.plane(u.at[s + 1, c], j0)
            out[s, side, 3] = level.plane(u.at[s + 1, 1], j1)

    def pack_plane(s):
        lane = lanes((8, 128))
        tile = jnp.zeros((8, 128), F32)
        for c in range(3):
            for i in range(8):
                column = uc[s + 1, c, 0, pl.ds(8 * i, 8), 0:1]
                at = 16 * c + 2 * i
                tile = jnp.where((lane == at) | (lane == at + 1), column, tile)
        pls[s] = tile

    def pack_corners(s):
        for (dx, dy), n in corner_id.items():
            fi, fj = (0 if dx < 0 else 15), (0 if dy < 0 else 15)
            ci, cj = (0 if dx < 0 else 7), (0 if dy < 0 else 7)
            rows = []
            for c in (0, 1):
                rows.append(spread_row(uf[s + 1, c, pl.ds(16 * fi + fj, 1), :]))
            for c in (0, 1):
                for h in (0, 1):
                    rows.append(spread_row(uc[s + 1, c, h, pl.ds(8 * ci + cj, 1), :]))
            for j in ((0, 1) if dy < 0 else (7, 7)):
                rows.append(spread_row(pls[s, pl.ds(j, 1), :]))
            sub = subs((8, 128))
            tile = rows[0]
            for m in range(1, 8):
                tile = jnp.where(sub == m, rows[m], tile)
            cos[s, n] = tile

    for dx in (-1, 1):
        @pl.when(jnp.logical_not(exists[(dx, 0)]))
        def _(side=side_of[dx]):
            for s in range(STEPS):
                xhf[s, side] = jnp.zeros(xhf.shape[2:], F32)
                xhc[s, side] = jnp.zeros(xhc.shape[2:], F32)
                plx[s, side] = jnp.zeros((8, 128), F32)
            xmf[side, 0] = jnp.zeros(xmf.shape[2:], F32)
            xmf[side, 1] = jnp.ones(xmf.shape[2:], F32)
            xmc[side, 0] = jnp.zeros(xmc.shape[2:], F32)
            xmc[side, 1] = jnp.ones(xmc.shape[2:], F32)
    for dy in (-1, 1):
        @pl.when(jnp.logical_not(exists[(0, dy)]))
        def _(side=side_of[dy]):
            for s in range(STEPS):
                yhf[s, side] = jnp.zeros(yhf.shape[2:], F32)
                yhc[s, side] = jnp.zeros(yhc.shape[2:], F32)
                ply[s, side] = jnp.zeros((8, 128), F32)
            ymf[side, 0] = jnp.zeros(ymf.shape[2:], F32)
            ymf[side, 1] = jnp.ones(ymf.shape[2:], F32)
            ymc[side, 0] = jnp.zeros(ymc.shape[2:], F32)
            ymc[side, 1] = jnp.ones(ymc.shape[2:], F32)
    for d in corners:
        @pl.when(jnp.logical_not(exists[d]))
        def _(n=corner_id[d]):
            for s in range(STEPS):
                cor[s, n] = jnp.zeros((8, 128), F32)

    wait_load("fine_disp", "coarse_disp", "fine_rigidity", "coarse_rigidity", "fine_metric",
              "coarse_metric")
    for c in (0, 1):
        for side, jf, jc in ((LO, 0, 0), (HI, 15, 7)):
            ysmf[side, c] = Fine.plane(matf.at[c], jf)
            ysmc[side, c] = Coarse.plane(matc.at[c], jc)
    pack_y(Fine, 0)
    pack_y(Coarse, 0)
    pack_plane(0)
    pack_corners(0)

    greeted = n1 - 1 + n2 - 1
    for d in directions:
        greeted = greeted + jnp.where(exists[d], 1, 0).astype(jnp.int32)
    pl.semaphore_wait(barrier, greeted)

    send(0, "co", "cp", "cx", "cy", "mx", "my", "fx", "fy")

    wait_load("fine_density", "fine_lame", "coarse_density", "coarse_lame")
    lane8 = lanes((8, 128))
    spread = jnp.where(
        (lanes((16, 128)) % 16 == subs((16, 128))) & (lanes((16, 128)) < 48), 1.0, 0.0
    ).astype(F32)
    for t in (0, 1):
        pick = jnp.where(lanes((8, 16)) == 2 * subs((8, 16)) + t, 1.0, 0.0).astype(F32)
        for axis in (0, 1):
            table = offsets_ref[axis].astype(F32)
            turned = lax.dot_general(
                pick, table, (((1,), (1,)), ((), ())), preferred_element_type=F32
            )
            shift = jnp.dot(turned, spread, preferred_element_type=F32)
            if axis == 0:
                near = jnp.where(lane8 % 2 == 0, 0.75, 0.25).astype(F32)
            else:
                near = jnp.full((8, 128), 0.75 if t == 0 else 0.25, F32)
            for m, value in enumerate((-1.0, 0.0, 1.0, 2.0)):
                weights[t, 4 * axis + m] = jnp.where(shift == value, near, 0.0) + jnp.where(
                    shift == value - 1.0, 1.0 - near, 0.0
                )

    levels = (
        (Coarse, uc, matc, kc, dvc, dyc, xhc, yhc, ysc, xmc, ymc),
        (Fine, uf, matf, kf, dvf, dyf, xhf, yhf, ysf, xmf, ymf),
    )
    for level, u, mat, k, dv, dy_, xh, yh, ys, xm, ym in levels:
        for i in range(0, level.n, R):
            rig, met, den, lam = (level.load(mat.at[m], i, R) for m in range(4))
            scale = level.edge_scale(rig.shape)
            inverse = 1.0 / met
            light = DT / den
            a = inverse * light
            vertical = rig * inverse
            b = (lam + rig) * light
            isv = inverse * scale
            half_a = 0.5 * a
            for slot, value in (
                (WIDE, rig * met), (HALF_A, half_a), (ISV, isv), (GB, 0.5 * b), (GZ, b * isv),
                (DM, den * met), (CZU, half_a * (vertical + level.k_up(vertical))),
                (CZD, half_a * (vertical + level.k_down(vertical))),
            ):
                level.store(k.at[slot], i, R, value)

    def halo_row(level, ref):
        if level is Fine:
            return Fine.load(ref, 0, 1)
        return Coarse.load(ref, 0, 1)

    def side_coefficients(level, mat, k, xm, ym):
        for i in range(0, level.n, R):
            w = level.load(k.at[WIDE], i, R)
            ha = level.load(k.at[HALF_A], i, R)

            def outer(side):
                return halo_row(level, xm.at[side, 0]) * halo_row(level, xm.at[side, 1])

            cxp = ha * (w + neighbour_rows(level, k.at[WIDE], i, R, 1, lambda: outer(HI)))
            cxm = ha * (w + neighbour_rows(level, k.at[WIDE], i, R, -1, lambda: outer(LO)))
            up = level.row_of(ym.at[HI, 0], i, R) * level.row_of(ym.at[HI, 1], i, R)
            down = level.row_of(ym.at[LO, 0], i, R) * level.row_of(ym.at[LO, 1], i, R)
            cyu = ha * (w + level.j_up(w, up))
            cyd = ha * (w + level.j_down(w, down))
            total = cxp + cxm + cyu + cyd + level.load(k.at[CZU], i, R) + level.load(k.at[CZD], i, R)
            for slot, value in ((CXP, cxp), (CXM, cxm), (CYU, cyu), (CYD, cyd), (C0, total)):
                level.store(k.at[slot], i, R, value)

    def divergences(s, level, u, mat, k, dv, dy_, xh, yh, ys, xm, ym):
        now = u.at[s + 1]
        n = level.n
        for i in range(0, n, R):
            def halo(side):
                return lambda: halo_row(level, xh.at[s, side, 0])

            px = neighbour_rows(level, now.at[0], i, R, 1, halo(HI))
            mx = neighbour_rows(level, now.at[0], i, R, -1, halo(LO))
            y = level.load(now.at[1], i, R)
            z = level.load(now.at[2], i, R)
            py = level.j_up(y, level.row_of(yh.at[s, HI, 1], i, R))
            my = level.j_down(y, level.row_of(yh.at[s, LO, 1], i, R))
            isv = level.load(k.at[ISV], i, R)
            value = 0.5 * ((px - mx) + (py - my)) + isv * (level.k_up(z) - level.k_down(z))
            level.store(dv, i + 1, R, value)
        for dx, side in side_of.items():
            inside = level.load(now.at[0], 0 if dx < 0 else n - 1, 1)
            beyond = halo_row(level, xh.at[s, side, 3])
            y = halo_row(level, xh.at[s, side, 1])
            z = halo_row(level, xh.at[s, side, 2])
            py = level.j_up(y, level.corner_row(cor.at[s, corner_id[(dx, 1)]], 1))
            my = level.j_down(y, level.corner_row(cor.at[s, corner_id[(dx, -1)]], 1))
            isv = level.edge_scale(z.shape) / halo_row(level, xm.at[side, 1])
            along = (beyond - inside) if dx > 0 else (inside - beyond)
            value = 0.5 * (along + (py - my)) + isv * (level.k_up(z) - level.k_down(z))
            level.store(dv, 0 if dx < 0 else n + 1, 1, value * flag((dx, 0)))
        for dy, side in side_of.items():
            x, z, beyond = yh[s, side, 0], yh[s, side, 2], yh[s, side, 3]
            inside = ys[s, side, 1]
            sub = plane_sub(level, x)
            px = jnp.where(sub == n - 1, level.corner_plane(cor.at[s, corner_id[(1, dy)]], 0),
                           plane_roll(level, x, -1))
            mx = jnp.where(sub == 0, level.corner_plane(cor.at[s, corner_id[(-1, dy)]], 0),
                           plane_roll(level, x, 1))
            isv = level.edge_scale(z.shape) / ym[side, 1]
            along = (beyond - inside) if dy > 0 else (inside - beyond)
            value = 0.5 * (along + (px - mx)) + isv * (level.plane_k_up(z) - level.plane_k_down(z))
            dy_[side] = value * flag((0, dy))

    def fine_ghosts(s):
        sub, lane = subs((8, 128)), lanes((8, 128)) % 16

        def shifted_rows(tile, low, high0, high1):
            return [
                jnp.where(sub == 0, low, roll(tile, 1, 0)),
                tile,
                jnp.where(sub == 7, high0, roll(tile, -1, 0)),
                jnp.where(sub == 7, high1, jnp.where(sub == 6, high0, roll(tile, -2, 0))),
            ]

        def row(ref, j):
            return spread_row(ref[pl.ds(j, 1), :])

        def corner_rows(dx):
            low, high = cor.at[s, corner_id[(dx, -1)]], cor.at[s, corner_id[(dx, 1)]]
            return row(low, 6), row(high, 6), row(high, 7)

        own = shifted_rows(pls[s], row(ply.at[s, LO], 7), row(ply.at[s, HI], 0), row(ply.at[s, HI], 1))
        left = shifted_rows(plx[s, LO], *corner_rows(-1))
        right = shifted_rows(plx[s, HI], *corner_rows(1))
        totals = [jnp.zeros((8, 128), F32) for _ in (0, 1)]
        for mx in range(4):
            inner = [jnp.zeros((8, 128), F32) for _ in (0, 1)]
            for my in range(4):
                if mx == 0:
                    tile = jnp.where(lane < 2, roll(left[my], -14, 1), roll(own[my], 2, 1))
                elif mx == 1:
                    tile = own[my]
                elif mx == 2:
                    tile = jnp.where(lane >= 14, roll(right[my], 14, 1), roll(own[my], -2, 1))
                else:
                    tile = jnp.where(lane >= 12, roll(right[my], 12, 1), roll(own[my], -4, 1))
                for t in (0, 1):
                    inner[t] = inner[t] + weights[t, 4 + my] * tile
            for t in (0, 1):
                totals[t] = totals[t] + weights[t, mx] * inner[t]
        for t in (0, 1):
            ghost[t] = totals[t]

    def fine_last(c, i):
        rows = []
        for t in (0, 1):
            tile = ghost[t]
            rows.append(jnp.stack([roll(tile, 127 - (16 * c + i + m), 1) for m in range(R)]))
        return jnp.stack(rows)

    def coarse_first(s, c, i):
        rows = []
        for m in range(R):
            base = 32 * (i + m)
            parts = [uf[s + 1, c, pl.ds(base + t, 8, stride=2), :] for t in (0, 1, 16, 17)]
            rows.append(0.25 * ((parts[0] + parts[1]) + (parts[2] + parts[3])))
        return roll(jnp.stack(rows), 1, 2)

    def rates(s, i, level, u, mat, k, dv, dy_, xh, yh, ys, xm, ym):
        now, old, new = u.at[s + 1], u.at[s], u.at[s + 2]
        coef = {
            m: level.load(k.at[m], i, R) for m in (GB, GZ, DM, CZU, CZD, CXP, CXM, CYU, CYD, C0)
        }
        d_mid = level.load(dv, i + 1, R)
        gradient = [
            coef[GB] * (level.load(dv, i + 2, R) - level.load(dv, i, R)),
            coef[GB]
            * (
                level.j_up(d_mid, level.row_of(dy_.at[HI], i, R))
                - level.j_down(d_mid, level.row_of(dy_.at[LO], i, R))
            ),
            coef[GZ] * (level.k_up(d_mid) - level.k_down(d_mid)),
        ]
        energy = None
        for c in range(3):
            v = level.load(now.at[c], i, R)

            def halo(side, c=c):
                return lambda: halo_row(level, xh.at[s, side, c])

            px = neighbour_rows(level, now.at[c], i, R, 1, halo(HI))
            mx = neighbour_rows(level, now.at[c], i, R, -1, halo(LO))
            py = level.j_up(v, level.row_of(yh.at[s, HI, c], i, R))
            my = level.j_down(v, level.row_of(yh.at[s, LO, c], i, R))
            if level is Fine:
                pz, mz = level.k_up(v, fine_last(c, i)), level.k_down(v)
            else:
                pz = level.k_up(v, jnp.zeros_like(v[1]))
                mz = level.k_down(v, coarse_first(s, c, i))
            rate = (
                (coef[CXP] * px + coef[CXM] * mx)
                + (coef[CYU] * py + coef[CYD] * my)
                + (coef[CZU] * pz + coef[CZD] * mz)
                - coef[C0] * v
                + gradient[c]
            )
            after = (2.0 * v - level.load(old.at[c], i, R)) + rate
            level.store(new.at[c], i, R, after)
            change = after - v
            part = change * change - after * rate
            energy = part if energy is None else energy + part
        return jnp.sum(coef[DM] * energy, axis=(0, 1))

    def order(level):
        n = level.n
        return [0, n - R] + list(range(R, n - R, R))

    coarse_set, fine_set = levels
    for s in range(STEPS):
        last = s == STEPS - 1
        receive(s, "co", "cp", "cx", "cy")
        if s == 0:
            receive(0, "mx", "my")
            side_coefficients(Coarse, matc, kc, xmc, ymc)
            side_coefficients(Fine, matf, kf, xmf, ymf)
            wait_load("fine_prev", "coarse_prev")
        divergences(s, *coarse_set)
        total = jnp.zeros((8, 128), F32)
        for m, i in enumerate(order(Coarse)):
            total = total + rates(s, i, *coarse_set)
            if m == 1 and not last:
                send(s + 1, "cx")
        eacc[s, 1] = total
        if not last:
            pack_y(Coarse, s + 1)
            pack_plane(s + 1)
            send(s + 1, "cy", "cp")
        fine_ghosts(s)
        receive(s, "fx", "fy")
        divergences(s, *fine_set)
        total = jnp.zeros((8, 128), F32)
        for m, i in enumerate(order(Fine)):
            total = total + rates(s, i, *fine_set)
            if m == 1 and not last:
                pack_corners(s + 1)
                send(s + 1, "co", "fx")
        eacc[s, 0] = total
        if not last:
            pack_y(Fine, s + 1)
            send(s + 1, "fy")

    outs = [pltpu.make_async_copy(uf.at[STEPS + 1], fine_out, out_sem.at[0])]
    for h in (0, 1):
        outs.append(
            pltpu.make_async_copy(
                uc.at[STEPS + 1, :, h], coarse_out.at[:, :, pl.ds(128 * h, 128)], out_sem.at[1 + h]
            )
        )
    for c in outs:
        c.start()

    lane1 = lanes((1, 128))
    row = jnp.zeros((1, 128), F32)
    cells = (nx * ny * 16 * 16 * 128, nx * ny * 8 * 8 * 256)
    for s in range(STEPS):
        for m in (0, 1):
            value = jnp.sum(eacc[s, m], axis=0, keepdims=True)
            value = jnp.sum(value, axis=1, keepdims=True)
            row = jnp.where(lane1 == 2 * s + m, value * (1.0 / cells[m]), row)
    erow[0] = row
    er1[me1] = row

    def reduce(n, me, own, buffer, peer, stage):
        def copy(d):
            return pltpu.make_async_remote_copy(
                src_ref=own, dst_ref=buffer.at[me], send_sem=esend.at[stage],
                recv_sem=erecv.at[stage], device_id=peer(d), device_id_type=MESH,
            )

        @pl.loop(1, n)
        def _(d):
            copy(d).start()

        whole = pltpu.make_async_remote_copy(
            src_ref=buffer.at[pl.ds(0, n - 1)], dst_ref=buffer.at[pl.ds(0, n - 1)],
            send_sem=esend.at[stage], recv_sem=erecv.at[stage], device_id=peer(1),
            device_id_type=MESH,
        )
        whole.wait_recv()
        return whole

    done1 = reduce(n1, me1, erow.at[0], er1, peer1, 0)
    row = er1[0]
    for m in range(1, n1):
        row = row + er1[m]
    done2 = None
    if n2 > 1:
        erow[1] = row
        er2[gx_hi] = row
        done2 = reduce(n2, gx_hi, erow.at[1], er2, peer2, 1)
        row = er2[0]
        for m in range(1, n2):
            row = row + er2[m]
    for s in range(STEPS):
        energy_out[pl.ds(s, 1), :] = roll(row, -2 * s, 1)[:, 0:2]

    done1.wait_send()
    if done2 is not None:
        done2.wait_send()
    for s in range(STEPS):
        run(s, ("co", "cp", "cx", "cy", "mx", "my", "fx", "fy"), "wait_send")
    for c in outs:
        c.wait()


def per_device(nx, ny, group_x, *args):
    args = list(args)
    for m in range(4):
        shape = args[m].shape
        args[m] = args[m].reshape(shape[0], shape[1] * shape[2], shape[3])
    for m in range(4, 12):
        shape = args[m].shape
        args[m] = args[m].reshape(shape[0] * shape[1], shape[2])
    vm, dma = pltpu.VMEM, pltpu.SemaphoreType.DMA
    n1, n2 = group_x * ny, nx // group_x
    scratch = [
        vm((STEPS + 2, 3, 256, 128), F32),
        vm((STEPS + 2, 3, 2, 64, 128), F32),
        vm((4, 256, 128), F32),
        vm((4, 2, 64, 128), F32),
        vm((NCOEF, 256, 128), F32),
        vm((NCOEF, 2, 64, 128), F32),
        vm((18 * 16, 128), F32),
        vm((2, 10 * 8, 128), F32),
        vm((2, 16, 128), F32),
        vm((2, 2, 8, 128), F32),
        vm((STEPS, 2, 4, 16, 128), F32),
        vm((STEPS, 2, 4, 2, 8, 128), F32),
        vm((STEPS, 2, 4, 16, 128), F32),
        vm((STEPS, 2, 4, 2, 8, 128), F32),
        vm((STEPS, 2, 4, 16, 128), F32),
        vm((STEPS, 2, 4, 2, 8, 128), F32),
        vm((2, 2, 16, 128), F32),
        vm((2, 2, 2, 8, 128), F32),
        vm((2, 2, 16, 128), F32),
        vm((2, 2, 2, 8, 128), F32),
        vm((2, 2, 16, 128), F32),
        vm((2, 2, 2, 8, 128), F32),
        vm((STEPS, 8, 128), F32),
        vm((STEPS, 2, 8, 128), F32),
        vm((STEPS, 2, 8, 128), F32),
        vm((STEPS, 4, 8, 128), F32),
        vm((STEPS, 4, 8, 128), F32),
        vm((2, 8, 8, 128), F32),
        vm((2, 8, 128), F32),
        vm((STEPS, 2, 8, 128), F32),
        vm((2, 1, 128), F32),
        vm((n1, 1, 128), F32),
        vm((max(n2, 1), 1, 128), F32),
        dma((12, 2)),
        dma((3,)),
        dma((STEPS, 28)),
        dma((STEPS, 28)),
        dma((2,)),
        dma((2,)),
    ]
    anywhere = pl.BlockSpec(memory_space=pltpu.HBM)
    in_vmem = pl.BlockSpec(memory_space=pltpu.VMEM)
    fine, coarse, energy = pl.pallas_call(
        functools.partial(kernel, nx, ny, group_x),
        out_shape=(
            jax.ShapeDtypeStruct((3, 256, 128), F32),
            jax.ShapeDtypeStruct((3, 64, 256), F32),
            jax.ShapeDtypeStruct((STEPS, 2), F32),
        ),
        in_specs=[anywhere] * 12 + [in_vmem],
        out_specs=(anywhere, anywhere, in_vmem),
        scratch_shapes=scratch,
        compiler_params=pltpu.CompilerParams(
            collective_id=0, has_side_effects=True, vmem_limit_bytes=60 << 20
        ),
        name="leapfrog",
    )(*args)
    return fine.reshape(3, 16, 16, 128), coarse.reshape(3, 8, 8, 256), energy


def solution(mesh):
    nx, ny = mesh.shape["gx"], mesh.shape["gy"]
    group_x = 4 if nx % 4 == 0 else 1
    field, cells = P(None, "gx", "gy", None), P("gx", "gy", None)
    return jax.shard_map(
        functools.partial(per_device, nx, ny, group_x),
        mesh=mesh,
        in_specs=(field,) * 4 + (cells,) * 8 + (P(None, "gx", "gy"),),
        out_specs=(field, field, P()),
        check_vma=False,
    )
```

```python
import functools

import jax
import jax.numpy as jnp
from jax import lax
from jax.experimental import pallas as pl
from jax.experimental.pallas import tpu as pltpu
from jax.sharding import PartitionSpec as P

STEPS = 3
DT = 0.15
MESH = pl.DeviceIdType.MESH
F32 = jnp.float32

R = 2
LO, HI = 0, 1
(WIDE, HALF_A, ISV, GB, GZ, DM, CZU, CZD, CXP, CXM, CYU, CYD, C0) = range(13)
NCOEF = 13


def lanes(shape):
    return lax.broadcasted_iota(jnp.int32, shape, len(shape) - 1)


def subs(shape):
    return lax.broadcasted_iota(jnp.int32, shape, len(shape) - 2)


def spread_row(row):
    return jnp.broadcast_to(row, (8, 128))


def roll(x, shift, axis):
    return pltpu.roll(x, shift % x.shape[axis], axis)


class Fine:
    n = 16
    key = "f"

    @staticmethod
    def load(ref, i, r):
        parts = [ref[pl.ds(16 * i + t, 8 * r, stride=2), :].reshape(1, r, 8, 128) for t in (0, 1)]
        return jnp.concatenate(parts, axis=0)

    @staticmethod
    def store(ref, i, r, value):
        for t in (0, 1):
            ref[pl.ds(16 * i + t, 8 * r, stride=2), :] = value[t].reshape(8 * r, 128)

    @staticmethod
    def k_up(x, last=None):
        moved = roll(x, -1, 3)
        edge = x if last is None else last
        return jnp.where(lanes(x.shape) == 127, edge, moved)

    @staticmethod
    def k_down(x, first=None):
        moved = roll(x, 1, 3)
        edge = x if first is None else first
        return jnp.where(lanes(x.shape) == 0, edge, moved)

    @staticmethod
    def edge_scale(shape):
        k = lanes(shape)
        return jnp.where((k == 0) | (k == 127), 1.0, 0.5).astype(F32)

    @staticmethod
    def row_of(ref, i, r):
        return jnp.concatenate(
            [spread_row(ref[pl.ds(i + m, 1), :]).reshape(1, 8, 128) for m in range(r)], axis=0
        )

    @staticmethod
    def j_up(x, halo):
        s = subs(x.shape[1:])
        moved = jnp.where(s == 7, halo, roll(x[0], -1, 1))
        return jnp.stack([x[1], moved])

    @staticmethod
    def j_down(x, halo):
        s = subs(x.shape[1:])
        moved = jnp.where(s == 0, halo, roll(x[1], 1, 1))
        return jnp.stack([moved, x[0]])

    @staticmethod
    def plane(ref, j):
        return jnp.concatenate([ref[pl.ds(j + 128 * h, 8, stride=16), :] for h in (0, 1)], axis=0)

    @staticmethod
    def plane_k_up(x):
        return jnp.where(lanes(x.shape) == 127, x, roll(x, -1, 1))

    @staticmethod
    def plane_k_down(x):
        return jnp.where(lanes(x.shape) == 0, x, roll(x, 1, 1))

    @staticmethod
    def corner_plane(tile_ref, comp):
        row = spread_row(tile_ref[comp])
        return jnp.concatenate([row, row], axis=0)

    @staticmethod
    def corner_row(tile_ref, comp):
        return spread_row(tile_ref[comp]).reshape(1, 8, 128)


class Coarse:
    n = 8
    key = "c"

    @staticmethod
    def load(ref, i, r):
        return ref[:, pl.ds(8 * i, 8 * r), :].reshape(2, r, 8, 128)

    @staticmethod
    def store(ref, i, r, value):
        ref[:, pl.ds(8 * i, 8 * r), :] = value.reshape(2, 8 * r, 128)

    @staticmethod
    def k_up(x, last=None):
        moved = roll(x, -1, 3)
        edge = x[1] if last is None else last
        return jnp.where(lanes(x.shape) == 127, jnp.stack([moved[1], edge]), moved)

    @staticmethod
    def k_down(x, first=None):
        moved = roll(x, 1, 3)
        edge = x[0] if first is None else first
        return jnp.where(lanes(x.shape) == 0, jnp.stack([edge, moved[0]]), moved)

    @staticmethod
    def edge_scale(shape):
        k = lanes(shape)
        half = lax.broadcasted_iota(jnp.int32, shape, 0)
        ends = ((k == 0) & (half == 0)) | ((k == 127) & (half == 1))
        return jnp.where(ends, 1.0, 0.5).astype(F32)

    @staticmethod
    def row_of(ref, i, r):
        halves = []
        for h in (0, 1):
            rows = [spread_row(ref[h, pl.ds(i + m, 1), :]).reshape(1, 8, 128) for m in range(r)]
            halves.append(jnp.concatenate(rows, axis=0))
        return jnp.stack(halves)

    @staticmethod
    def j_up(x, halo):
        return jnp.where(subs(x.shape) == 7, halo, roll(x, -1, 2))

    @staticmethod
    def j_down(x, halo):
        return jnp.where(subs(x.shape) == 0, halo, roll(x, 1, 2))

    @staticmethod
    def plane(ref, j):
        return jnp.stack([ref[h, pl.ds(j, 8, stride=8), :] for h in (0, 1)])

    @staticmethod
    def plane_k_up(x):
        return Coarse.k_up(x[:, None])[:, 0]

    @staticmethod
    def plane_k_down(x):
        return Coarse.k_down(x[:, None])[:, 0]

    @staticmethod
    def corner_plane(tile_ref, comp):
        return jnp.stack([spread_row(tile_ref[2 * comp + h]) for h in (0, 1)])

    @staticmethod
    def corner_row(tile_ref, comp):
        rows = [spread_row(tile_ref[2 * comp + h]) for h in (0, 1)]
        return jnp.stack(rows)[:, None]


def plane_roll(level, x, shift):
    return roll(x, shift, 0) if level is Fine else roll(x, shift, 1)


def plane_sub(level, x):
    return subs(x.shape)


def neighbour_rows(level, ref, i, r, step, halo):
    if step > 0:
        if i + r < level.n:
            return level.load(ref, i + 1, r)
        return jnp.concatenate([level.load(ref, i + 1, r - 1), halo()], axis=1)
    if i > 0:
        return level.load(ref, i - 1, r)
    return jnp.concatenate([halo(), level.load(ref, 0, r - 1)], axis=1)


def kernel(nx, ny, group_x, *refs):
    names_in = ["fine_disp", "fine_prev", "coarse_disp", "coarse_prev"]
    for name in ("fine", "coarse"):
        names_in += [name + part for part in ("_density", "_lame", "_rigidity", "_metric")]
    hbm = dict(zip(names_in, refs[:12]))
    offsets_hbm = refs[12]
    fine_out, coarse_out, energy_out = refs[13:16]
    (
        uf, uc, matf, matc, kf, kc, dvf, dvc, dyf, dyc,
        xhf, xhc, yhf, yhc, ysf, ysc, xmf, xmc, ymf, ymc, ysmf, ysmc,
        pls, plx, ply, pex, ccs, ccr, fcs, fcr, offsets_ref, weights, ghost, eacc, erow, er1, er2,
        load_sem, send_sem, recv_sem, esend, erecv,
    ) = refs[16:]

    gx, gy = lax.axis_index("gx"), lax.axis_index("gy")
    exists = {
        (dx, dy): functools.reduce(
            jnp.logical_and,
            ([gx > 0] if dx < 0 else [gx < nx - 1] if dx > 0 else [])
            + ([gy > 0] if dy < 0 else [gy < ny - 1] if dy > 0 else []),
        )
        for dx in (-1, 0, 1)
        for dy in (-1, 0, 1)
        if (dx, dy) != (0, 0)
    }
    directions = list(exists)
    corners = [d for d in directions if d[0] and d[1]]
    corner_id = {d: n for n, d in enumerate(corners)}

    def flag(direction):
        return jnp.where(exists[direction], 1.0, 0.0).astype(F32)

    def device(direction):
        return {"gx": gx + direction[0], "gy": gy + direction[1]}

    groups, half = nx // group_x, ny // 2
    gx_hi, gx_lo = gx // group_x, gx % group_x
    chip_y, second = gy // 2, gy % 2 == 1
    first_core = jnp.logical_not(second)
    n1, n2 = group_x * ny, groups
    me1 = gx_lo * ny + gy
    plane_x = [gx_hi * group_x + lax.rem(gx_lo + a, group_x) for a in range(group_x)]
    plane_y = [2 * lax.rem(chip_y + b, half) for b in range(half)]
    line_x = [lax.rem(gx_hi + d, n2) * group_x + gx_lo for d in range(n2)]

    loads = {}

    def start_load(name, dst, sem):
        fine = name.startswith("fine")
        src = hbm[name]
        if fine:
            copies = [pltpu.make_async_copy(src, dst, load_sem.at[sem, 0])]
        else:
            lead = (slice(None),) * (len(src.shape) - 2)
            copies = [
                pltpu.make_async_copy(
                    src.at[lead + (slice(None), pl.ds(128 * h, 128))],
                    dst.at[(slice(None), h) if lead else (h,)],
                    load_sem.at[sem, h],
                )
                for h in (0, 1)
            ]
        for c in copies:
            c.start()
        loads[name] = copies

    plan = [
        ("fine_disp", uf.at[1]), ("coarse_disp", uc.at[1]),
        ("fine_rigidity", matf.at[0]), ("coarse_rigidity", matc.at[0]),
        ("fine_metric", matf.at[1]), ("coarse_metric", matc.at[1]),
        ("fine_density", matf.at[2]), ("fine_lame", matf.at[3]),
        ("coarse_density", matc.at[2]), ("coarse_lame", matc.at[3]),
        ("fine_prev", uf.at[0]), ("coarse_prev", uc.at[0]),
    ]
    for sem, (name, dst) in enumerate(plan):
        start_load(name, dst, sem)

    loads["offsets"] = [pltpu.make_async_copy(offsets_hbm, offsets_ref, load_sem.at[12, 0])]
    loads["offsets"][0].start()

    def wait_load(*names):
        for name in names:
            for c in loads[name]:
                c.wait()

    barrier = pltpu.get_barrier_semaphore()

    def greet(where):
        pl.semaphore_signal(barrier, inc=1, device_id=where, device_id_type=MESH)

    far_first = sorted(range(1, n2), key=lambda d: -min(d, n2 - d))
    for d in far_first:
        greet({"gx": line_x[d], "gy": 2 * chip_y + 1})
    for d in directions:
        @pl.when(exists[d])
        def _(d=d):
            greet(device(d))

    @pl.when(first_core)
    def _():
        greet({"gx": gx, "gy": 2 * chip_y + 1})

    @pl.when(second)
    def _():
        for x in plane_x:
            for y in plane_y:
                if not (x is plane_x[0] and y is plane_y[0]):
                    greet({"gx": x, "gy": y})
                    greet({"gx": x, "gy": y + 1})
        greet({"gx": gx, "gy": 2 * chip_y})

    side_of = {-1: LO, 1: HI}

    def messages(s):
        out = []
        u_f, u_c = uf.at[s + 1], uc.at[s + 1]
        for dx in (-1, 1):
            own, far = side_of[dx], side_of[-dx]
            first, second = (0, 1) if dx < 0 else (15, 14)
            out.append(("fx", (dx, 0), u_f.at[:, pl.ds(16 * first, 16)], xhf.at[s, far, pl.ds(0, 3)]))
            out.append(("fx", (dx, 0), u_f.at[0, pl.ds(16 * second, 16)], xhf.at[s, far, 3]))
            first, second = (0, 1) if dx < 0 else (7, 6)
            out.append(("cx", (dx, 0), u_c.at[:, :, pl.ds(8 * first, 8)], xhc.at[s, far, pl.ds(0, 3)]))
            out.append(("cx", (dx, 0), u_c.at[0, :, pl.ds(8 * second, 8)], xhc.at[s, far, 3]))
            out.append(("cp", (dx, 0), pex.at[s], plx.at[s, far]))
            if s == 0:
                first = 0 if dx < 0 else 15
                out.append(("mf", (dx, 0), matf.at[pl.ds(0, 2), pl.ds(16 * first, 16)], xmf.at[far]))
                first = 0 if dx < 0 else 7
                out.append(("mc", (dx, 0), matc.at[pl.ds(0, 2), :, pl.ds(8 * first, 8)], xmc.at[far]))
        for dy in (-1, 1):
            own, far = side_of[dy], side_of[-dy]
            out.append(("fy", (0, dy), ysf.at[s, own], yhf.at[s, far]))
            out.append(("cy", (0, dy), ysc.at[s, own], yhc.at[s, far]))
            out.append(("cq", (0, dy), pls.at[s], ply.at[s, far]))
            if s == 0:
                out.append(("mf", (0, dy), ysmf.at[own], ymf.at[far]))
                out.append(("mc", (0, dy), ysmc.at[own], ymc.at[far]))
        for d in corners:
            back = corner_id[(-d[0], -d[1])]
            out.append(("co", d, ccs.at[s, corner_id[d]], ccr.at[s, back]))
            out.append(("fo", d, fcs.at[s, corner_id[d]], fcr.at[s, back]))
        return out

    copies = []
    for s in range(STEPS):
        entries = []
        for n, (group, d, src, dst) in enumerate(messages(s)):
            def copy(src=src, dst=dst, s=s, n=n, d=d):
                return pltpu.make_async_remote_copy(
                    src_ref=src, dst_ref=dst,
                    send_sem=send_sem.at[s, n], recv_sem=recv_sem.at[s, n],
                    device_id=device(d), device_id_type=MESH,
                )

            entries.append((group, d, copy))
        copies.append(entries)

    def run(s, groups_wanted, what, backwards=False):
        for d in directions:
            mine = [c for g, e, c in copies[s] if g in groups_wanted and e == d]
            if mine:
                @pl.when(exists[(-d[0], -d[1]) if backwards else d])
                def _(mine=mine):
                    for c in mine:
                        getattr(c(), what)()

    def send(s, *wanted):
        run(s, wanted, "start")

    def receive(s, *wanted):
        run(s, wanted, "wait_recv", backwards=True)

    def pack_y(level, s):
        u, out = (uf, ysf) if level is Fine else (uc, ysc)
        last = 15 if level is Fine else 7
        for side, (j0, j1) in ((LO, (0, 1)), (HI, (last, last - 1))):
            for c in range(3):
                out[s, side, c] = level.plane(u.at[s + 1, c], j0)
            out[s, side, 3] = level.plane(u.at[s + 1, 1], j1)

    def plane_tile(s, tile, rows):
        lane = lanes((8, 128))
        for c in range(3):
            for i in rows:
                column = uc[s + 1, c, 0, pl.ds(8 * i, 8), 0:1]
                at = 16 * c + 2 * i
                tile = jnp.where((lane == at) | (lane == at + 1), column, tile)
        return tile

    def pack_edge(s):
        pex[s] = plane_tile(s, jnp.zeros((8, 128), F32), (0, 1, 7))
        for (dx, dy), n in corner_id.items():
            ci, cj = (0 if dx < 0 else 7), (0 if dy < 0 else 7)
            for c in (0, 1):
                for h in (0, 1):
                    ccs[s, n, 2 * c + h] = uc[s + 1, c, h, pl.ds(8 * ci + cj, 1), :]
            for m, j in enumerate((0, 1) if dy < 0 else (7, 7)):
                ccs[s, n, 4 + m] = pex[s, pl.ds(j, 1), :]

    def pack_plane(s):
        pls[s] = plane_tile(s, pex[s], range(2, 7))

    def pack_corners(s):
        for (dx, dy), n in corner_id.items():
            fi, fj = (0 if dx < 0 else 15), (0 if dy < 0 else 15)
            for c in (0, 1):
                fcs[s, n, c] = uf[s + 1, c, pl.ds(16 * fi + fj, 1), :]

    for dx in (-1, 1):
        @pl.when(jnp.logical_not(exists[(dx, 0)]))
        def _(side=side_of[dx]):
            for s in range(STEPS):
                xhf[s, side] = jnp.zeros(xhf.shape[2:], F32)
                xhc[s, side] = jnp.zeros(xhc.shape[2:], F32)
                plx[s, side] = jnp.zeros((8, 128), F32)
            xmf[side, 0] = jnp.zeros(xmf.shape[2:], F32)
            xmf[side, 1] = jnp.ones(xmf.shape[2:], F32)
            xmc[side, 0] = jnp.zeros(xmc.shape[2:], F32)
            xmc[side, 1] = jnp.ones(xmc.shape[2:], F32)
    for dy in (-1, 1):
        @pl.when(jnp.logical_not(exists[(0, dy)]))
        def _(side=side_of[dy]):
            for s in range(STEPS):
                yhf[s, side] = jnp.zeros(yhf.shape[2:], F32)
                yhc[s, side] = jnp.zeros(yhc.shape[2:], F32)
                ply[s, side] = jnp.zeros((8, 128), F32)
            ymf[side, 0] = jnp.zeros(ymf.shape[2:], F32)
            ymf[side, 1] = jnp.ones(ymf.shape[2:], F32)
            ymc[side, 0] = jnp.zeros(ymc.shape[2:], F32)
            ymc[side, 1] = jnp.ones(ymc.shape[2:], F32)
    for d in corners:
        @pl.when(jnp.logical_not(exists[d]))
        def _(n=corner_id[d]):
            for s in range(STEPS):
                ccr[s, n] = jnp.zeros(ccr.shape[2:], F32)
                fcr[s, n] = jnp.zeros(fcr.shape[2:], F32)

    wait_load("fine_disp", "coarse_disp", "fine_rigidity", "coarse_rigidity", "fine_metric",
              "coarse_metric")
    for c in (0, 1):
        for side, jf, jc in ((LO, 0, 0), (HI, 15, 7)):
            ysmf[side, c] = Fine.plane(matf.at[c], jf)
            ysmc[side, c] = Coarse.plane(matc.at[c], jc)
    pack_y(Fine, 0)
    pack_y(Coarse, 0)
    pack_edge(0)
    pack_plane(0)
    pack_corners(0)

    greeted = jnp.where(second, n1 // 2 - 1 + 2 * (n2 - 1) + 1, n1 // 2).astype(jnp.int32)
    for d in directions:
        greeted = greeted + jnp.where(exists[d], 1, 0).astype(jnp.int32)
    pl.semaphore_wait(barrier, greeted)

    send(0, "cx", "cy", "mc", "co", "cp", "cq")
    send(0, "fo", "mf")
    send(0, "fx", "fy")

    wait_load("fine_density", "fine_lame", "coarse_density", "coarse_lame", "offsets")
    lane8 = lanes((8, 128))
    spread = jnp.where(
        (lanes((16, 128)) % 16 == subs((16, 128))) & (lanes((16, 128)) < 48), 1.0, 0.0
    ).astype(F32)
    for t in (0, 1):
        pick = jnp.where(lanes((8, 16)) == 2 * subs((8, 16)) + t, 1.0, 0.0).astype(F32)
        for axis in (0, 1):
            table = offsets_ref[axis].astype(F32)
            turned = lax.dot_general(
                pick, table, (((1,), (1,)), ((), ())), preferred_element_type=F32
            )
            shift = jnp.dot(turned, spread, preferred_element_type=F32)
            if axis == 0:
                near = jnp.where(lane8 % 2 == 0, 0.75, 0.25).astype(F32)
            else:
                near = jnp.full((8, 128), 0.75 if t == 0 else 0.25, F32)
            for m, value in enumerate((-1.0, 0.0, 1.0, 2.0)):
                weights[t, 4 * axis + m] = jnp.where(shift == value, near, 0.0) + jnp.where(
                    shift == value - 1.0, 1.0 - near, 0.0
                )

    levels = (
        (Coarse, uc, matc, kc, dvc, dyc, xhc, yhc, ysc, xmc, ymc),
        (Fine, uf, matf, kf, dvf, dyf, xhf, yhf, ysf, xmf, ymf),
    )
    for level, u, mat, k, dv, dy_, xh, yh, ys, xm, ym in levels:
        for i in range(0, level.n, R):
            rig, met, den, lam = (level.load(mat.at[m], i, R) for m in range(4))
            scale = level.edge_scale(rig.shape)
            inverse = 1.0 / met
            light = DT / den
            a = inverse * light
            vertical = rig * inverse
            b = (lam + rig) * light
            isv = inverse * scale
            half_a = 0.5 * a
            for slot, value in (
                (WIDE, rig * met), (HALF_A, half_a), (ISV, isv), (GB, 0.5 * b), (GZ, b * isv),
                (DM, den * met), (CZU, half_a * (vertical + level.k_up(vertical))),
                (CZD, half_a * (vertical + level.k_down(vertical))),
            ):
                level.store(k.at[slot], i, R, value)

    def halo_row(level, ref):
        if level is Fine:
            return Fine.load(ref, 0, 1)
        return Coarse.load(ref, 0, 1)

    def side_coefficients(level, mat, k, xm, ym):
        for i in range(0, level.n, R):
            w = level.load(k.at[WIDE], i, R)
            ha = level.load(k.at[HALF_A], i, R)

            def outer(side):
                return halo_row(level, xm.at[side, 0]) * halo_row(level, xm.at[side, 1])

            cxp = ha * (w + neighbour_rows(level, k.at[WIDE], i, R, 1, lambda: outer(HI)))
            cxm = ha * (w + neighbour_rows(level, k.at[WIDE], i, R, -1, lambda: outer(LO)))
            up = level.row_of(ym.at[HI, 0], i, R) * level.row_of(ym.at[HI, 1], i, R)
            down = level.row_of(ym.at[LO, 0], i, R) * level.row_of(ym.at[LO, 1], i, R)
            cyu = ha * (w + level.j_up(w, up))
            cyd = ha * (w + level.j_down(w, down))
            total = cxp + cxm + cyu + cyd + level.load(k.at[CZU], i, R) + level.load(k.at[CZD], i, R)
            for slot, value in ((CXP, cxp), (CXM, cxm), (CYU, cyu), (CYD, cyd), (C0, total)):
                level.store(k.at[slot], i, R, value)

    def divergences(s, level, u, mat, k, dv, dy_, xh, yh, ys, xm, ym):
        cor = fcr if level is Fine else ccr
        now = u.at[s + 1]
        n = level.n
        for i in range(0, n, R):
            def halo(side):
                return lambda: halo_row(level, xh.at[s, side, 0])

            px = neighbour_rows(level, now.at[0], i, R, 1, halo(HI))
            mx = neighbour_rows(level, now.at[0], i, R, -1, halo(LO))
            y = level.load(now.at[1], i, R)
            z = level.load(now.at[2], i, R)
            py = level.j_up(y, level.row_of(yh.at[s, HI, 1], i, R))
            my = level.j_down(y, level.row_of(yh.at[s, LO, 1], i, R))
            isv = level.load(k.at[ISV], i, R)
            value = 0.5 * ((px - mx) + (py - my)) + isv * (level.k_up(z) - level.k_down(z))
            level.store(dv, i + 1, R, value)
        for dx, side in side_of.items():
            inside = level.load(now.at[0], 0 if dx < 0 else n - 1, 1)
            beyond = halo_row(level, xh.at[s, side, 3])
            y = halo_row(level, xh.at[s, side, 1])
            z = halo_row(level, xh.at[s, side, 2])
            py = level.j_up(y, level.corner_row(cor.at[s, corner_id[(dx, 1)]], 1))
            my = level.j_down(y, level.corner_row(cor.at[s, corner_id[(dx, -1)]], 1))
            isv = level.edge_scale(z.shape) / halo_row(level, xm.at[side, 1])
            along = (beyond - inside) if dx > 0 else (inside - beyond)
            value = 0.5 * (along + (py - my)) + isv * (level.k_up(z) - level.k_down(z))
            level.store(dv, 0 if dx < 0 else n + 1, 1, value * flag((dx, 0)))
        for dy, side in side_of.items():
            x, z, beyond = yh[s, side, 0], yh[s, side, 2], yh[s, side, 3]
            inside = ys[s, side, 1]
            sub = plane_sub(level, x)
            px = jnp.where(sub == n - 1, level.corner_plane(cor.at[s, corner_id[(1, dy)]], 0),
                           plane_roll(level, x, -1))
            mx = jnp.where(sub == 0, level.corner_plane(cor.at[s, corner_id[(-1, dy)]], 0),
                           plane_roll(level, x, 1))
            isv = level.edge_scale(z.shape) / ym[side, 1]
            along = (beyond - inside) if dy > 0 else (inside - beyond)
            value = 0.5 * (along + (px - mx)) + isv * (level.plane_k_up(z) - level.plane_k_down(z))
            dy_[side] = value * flag((0, dy))

    def fine_ghosts(s):
        sub, lane = subs((8, 128)), lanes((8, 128)) % 16

        def shifted_rows(tile, low, high0, high1):
            return [
                jnp.where(sub == 0, low, roll(tile, 1, 0)),
                tile,
                jnp.where(sub == 7, high0, roll(tile, -1, 0)),
                jnp.where(sub == 7, high1, jnp.where(sub == 6, high0, roll(tile, -2, 0))),
            ]

        def row(ref, j):
            return spread_row(ref[pl.ds(j, 1), :])

        def corner_rows(dx):
            low, high = ccr.at[s, corner_id[(dx, -1)]], ccr.at[s, corner_id[(dx, 1)]]
            return spread_row(low[4]), spread_row(high[4]), spread_row(high[5])

        own = shifted_rows(pls[s], row(ply.at[s, LO], 7), row(ply.at[s, HI], 0), row(ply.at[s, HI], 1))
        left = shifted_rows(plx[s, LO], *corner_rows(-1))
        right = shifted_rows(plx[s, HI], *corner_rows(1))
        totals = [jnp.zeros((8, 128), F32) for _ in (0, 1)]
        for mx in range(4):
            inner = [jnp.zeros((8, 128), F32) for _ in (0, 1)]
            for my in range(4):
                if mx == 0:
                    tile = jnp.where(lane < 2, roll(left[my], -14, 1), roll(own[my], 2, 1))
                elif mx == 1:
                    tile = own[my]
                elif mx == 2:
                    tile = jnp.where(lane >= 14, roll(right[my], 14, 1), roll(own[my], -2, 1))
                else:
                    tile = jnp.where(lane >= 12, roll(right[my], 12, 1), roll(own[my], -4, 1))
                for t in (0, 1):
                    inner[t] = inner[t] + weights[t, 4 + my] * tile
            for t in (0, 1):
                totals[t] = totals[t] + weights[t, mx] * inner[t]
        for t in (0, 1):
            ghost[t] = totals[t]

    def fine_last(c, i):
        rows = []
        for t in (0, 1):
            tile = ghost[t]
            rows.append(jnp.stack([roll(tile, 127 - (16 * c + i + m), 1) for m in range(R)]))
        return jnp.stack(rows)

    def coarse_first(s, c, i):
        rows = []
        for m in range(R):
            base = 32 * (i + m)
            parts = [uf[s + 1, c, pl.ds(base + t, 8, stride=2), :] for t in (0, 1, 16, 17)]
            rows.append(0.25 * ((parts[0] + parts[1]) + (parts[2] + parts[3])))
        return roll(jnp.stack(rows), 1, 2)

    def rates(s, i, level, u, mat, k, dv, dy_, xh, yh, ys, xm, ym):
        now, old = u.at[s + 1], u.at[s]
        coef = {
            m: level.load(k.at[m], i, R) for m in (GB, GZ, DM, CZU, CZD, CXP, CXM, CYU, CYD, C0)
        }
        d_mid = level.load(dv, i + 1, R)
        gradient = [
            coef[GB] * (level.load(dv, i + 2, R) - level.load(dv, i, R)),
            coef[GB]
            * (
                level.j_up(d_mid, level.row_of(dy_.at[HI], i, R))
                - level.j_down(d_mid, level.row_of(dy_.at[LO], i, R))
            ),
            coef[GZ] * (level.k_up(d_mid) - level.k_down(d_mid)),
        ]
        energy = None
        for c in range(3):
            v = level.load(now.at[c], i, R)

            def halo(side, c=c):
                return lambda: halo_row(level, xh.at[s, side, c])

            px = neighbour_rows(level, now.at[c], i, R, 1, halo(HI))
            mx = neighbour_rows(level, now.at[c], i, R, -1, halo(LO))
            py = level.j_up(v, level.row_of(yh.at[s, HI, c], i, R))
            my = level.j_down(v, level.row_of(yh.at[s, LO, c], i, R))
            if level is Fine:
                pz, mz = level.k_up(v, fine_last(c, i)), level.k_down(v)
            else:
                pz = level.k_up(v, jnp.zeros_like(v[1]))
                mz = level.k_down(v, coarse_first(s, c, i))
            rate = (
                (coef[CXP] * px + coef[CXM] * mx)
                + (coef[CYU] * py + coef[CYD] * my)
                + (coef[CZU] * pz + coef[CZD] * mz)
                - coef[C0] * v
                + gradient[c]
            )
            after = (2.0 * v - level.load(old.at[c], i, R)) + rate
            if s < STEPS - 1:
                level.store(u.at[s + 2, c], i, R, after)
            elif level is Fine:
                level.store(fine_out.at[c], i, R, after)
            else:
                for h in (0, 1):
                    coarse_out[c, pl.ds(8 * i, 8 * R), pl.ds(128 * h, 128)] = after[h].reshape(
                        8 * R, 128
                    )
            change = after - v
            part = change * change - after * rate
            energy = part if energy is None else energy + part
        return jnp.sum(coef[DM] * energy, axis=(0, 1))

    def order(level):
        n = level.n
        return [0, n - R] + list(range(R, n - R, R))

    coarse_set, fine_set = levels
    for s in range(STEPS):
        last = s == STEPS - 1
        receive(s, "cx", "cy", "co")
        if s == 0:
            receive(0, "mc")
            side_coefficients(Coarse, matc, kc, xmc, ymc)
            wait_load("coarse_prev")
        divergences(s, *coarse_set)
        total = jnp.zeros((8, 128), F32)
        for m, i in enumerate(order(Coarse)):
            total = total + rates(s, i, *coarse_set)
            if m == 1 and not last:
                pack_edge(s + 1)
                send(s + 1, "cx", "co", "cp")
        eacc[s, 1] = total
        if not last:
            pack_y(Coarse, s + 1)
            pack_plane(s + 1)
            send(s + 1, "cy", "cq")
        receive(s, "cp", "cq")
        fine_ghosts(s)
        receive(s, "fx", "fy", "fo")
        if s == 0:
            receive(0, "mf")
            side_coefficients(Fine, matf, kf, xmf, ymf)
            wait_load("fine_prev")
        divergences(s, *fine_set)
        total = jnp.zeros((8, 128), F32)
        for m, i in enumerate(order(Fine)):
            total = total + rates(s, i, *fine_set)
            if m == 1 and not last:
                pack_corners(s + 1)
                send(s + 1, "fo", "fx")
        eacc[s, 0] = total
        if not last:
            pack_y(Fine, s + 1)
            send(s + 1, "fy")

    lane1 = lanes((1, 128))
    row = jnp.zeros((1, 128), F32)
    cells = (nx * ny * 16 * 16 * 128, nx * ny * 8 * 8 * 256)
    for s in range(STEPS):
        for m in (0, 1):
            value = jnp.sum(eacc[s, m], axis=0, keepdims=True)
            value = jnp.sum(value, axis=1, keepdims=True)
            row = jnp.where(lane1 == STEPS * m + s, value * (1.0 / cells[m]), row)
    erow[0] = row
    er1[me1] = row

    def rows(buffer, n, stage):
        part = buffer.at[pl.ds(0, n)]
        return pltpu.make_async_remote_copy(
            src_ref=part, dst_ref=part, send_sem=esend.at[stage], recv_sem=erecv.at[stage],
            device_id={"gx": line_x[0], "gy": gy}, device_id_type=MESH,
        )

    def pass_on(stage, slot, where):
        pltpu.make_async_remote_copy(
            src_ref=erow.at[stage], dst_ref=slot, send_sem=esend.at[stage],
            recv_sem=erecv.at[stage], device_id=where, device_id_type=MESH,
        ).start()

    for a in reversed(range(group_x)):
        for b in reversed(range(half)):
            if a or b:
                pass_on(0, er1.at[me1], {"gx": plane_x[a], "gy": plane_y[b] + 1})

    @pl.when(first_core)
    def _():
        pass_on(0, er1.at[me1], {"gx": gx, "gy": 2 * chip_y + 1})

    @pl.when(second)
    def _():
        rows(er1, n1 - 1, 0).wait_recv()
        plane = er1[0]
        for m in range(1, n1):
            plane = plane + er1[m]
        erow[1] = plane
        er2[gx_hi] = plane
        for d in far_first:
            for core in (0, 1):
                pass_on(1, er2.at[gx_hi], {"gx": line_x[d], "gy": 2 * chip_y + core})
        pass_on(1, er2.at[gx_hi], {"gx": gx, "gy": 2 * chip_y})
        if n2 > 1:
            rows(er2, n2 - 1, 1).wait_recv()

    @pl.when(first_core)
    def _():
        rows(er2, n2, 1).wait_recv()

    row = er2[0]
    for m in range(1, n2):
        row = row + er2[m]
    for m in (0, 1):
        energy_out[pl.ds(m, 1), :] = roll(row, -STEPS * m, 1)[:, 0:STEPS]

    @pl.when(second)
    def _():
        rows(er1, n1 // 2 - 1, 0).wait_send()
        rows(er1, 2 * n2 - 1, 1).wait_send()

    @pl.when(first_core)
    def _():
        rows(er1, n1 // 2, 0).wait_send()

    for s in range(STEPS):
        run(s, ("co", "cp", "cq", "fo", "cx", "cy", "mc", "mf", "fx", "fy"), "wait_send")


def hand_out(*refs):
    copies = [pltpu.make_async_copy(refs[n], refs[3 + n], refs[6].at[n]) for n in range(3)]
    for c in copies:
        c.start()
    for c in copies:
        c.wait()


def per_device(nx, ny, group_x, *args):
    args = list(args)
    for m in range(4):
        shape = args[m].shape
        args[m] = args[m].reshape(shape[0], shape[1] * shape[2], shape[3])
    for m in range(4, 12):
        shape = args[m].shape
        args[m] = args[m].reshape(shape[0] * shape[1], shape[2])
    for m in range(13):
        args[m] = pltpu.with_memory_space_constraint(args[m], pltpu.HBM)
    vm, dma = pltpu.VMEM, pltpu.SemaphoreType.DMA
    n1, n2 = group_x * ny, nx // group_x
    scratch = [
        vm((STEPS + 1, 3, 256, 128), F32),
        vm((STEPS + 1, 3, 2, 64, 128), F32),
        vm((4, 256, 128), F32),
        vm((4, 2, 64, 128), F32),
        vm((NCOEF, 256, 128), F32),
        vm((NCOEF, 2, 64, 128), F32),
        vm((18 * 16, 128), F32),
        vm((2, 10 * 8, 128), F32),
        vm((2, 16, 128), F32),
        vm((2, 2, 8, 128), F32),
        vm((STEPS, 2, 4, 16, 128), F32),
        vm((STEPS, 2, 4, 2, 8, 128), F32),
        vm((STEPS, 2, 4, 16, 128), F32),
        vm((STEPS, 2, 4, 2, 8, 128), F32),
        vm((STEPS, 2, 4, 16, 128), F32),
        vm((STEPS, 2, 4, 2, 8, 128), F32),
        vm((2, 2, 16, 128), F32),
        vm((2, 2, 2, 8, 128), F32),
        vm((2, 2, 16, 128), F32),
        vm((2, 2, 2, 8, 128), F32),
        vm((2, 2, 16, 128), F32),
        vm((2, 2, 2, 8, 128), F32),
        vm((STEPS, 8, 128), F32),
        vm((STEPS, 2, 8, 128), F32),
        vm((STEPS, 2, 8, 128), F32),
        vm((STEPS, 8, 128), F32),
        vm((STEPS, 4, 6, 1, 128), F32),
        vm((STEPS, 4, 6, 1, 128), F32),
        vm((STEPS, 4, 2, 1, 128), F32),
        vm((STEPS, 4, 2, 1, 128), F32),
        vm((2, 16, 16), jnp.int32),
        vm((2, 8, 8, 128), F32),
        vm((2, 8, 128), F32),
        vm((STEPS, 2, 8, 128), F32),
        vm((2, 1, 128), F32),
        vm((max(n1, 2 * n2), 1, 128), F32),
        vm((max(n2, 1), 1, 128), F32),
        dma((13, 2)),
        dma((STEPS, 32)),
        dma((STEPS, 32)),
        dma((2,)),
        dma((2,)),
    ]
    anywhere = pl.BlockSpec(memory_space=pltpu.HBM)
    in_vmem = pl.BlockSpec(memory_space=pltpu.VMEM)
    out_shape = (
        jax.ShapeDtypeStruct((3, 256, 128), F32),
        jax.ShapeDtypeStruct((3, 64, 256), F32),
        jax.ShapeDtypeStruct((2, STEPS), F32),
    )
    results = pl.pallas_call(
        functools.partial(kernel, nx, ny, group_x),
        out_shape=out_shape,
        in_specs=[anywhere] * 13,
        out_specs=(in_vmem, in_vmem, in_vmem),
        scratch_shapes=scratch,
        compiler_params=pltpu.CompilerParams(
            collective_id=0, has_side_effects=True, vmem_limit_bytes=32 << 20
        ),
        name="leapfrog",
    )(*args)
    fine, coarse, energy = pl.pallas_call(
        hand_out,
        out_shape=out_shape,
        in_specs=[in_vmem] * 3,
        out_specs=[anywhere] * 3,
        scratch_shapes=[dma((3,))],
        compiler_params=pltpu.CompilerParams(vmem_limit_bytes=1 << 20),
        name="hand_out",
    )(*results)
    energy = energy.T
    return fine.reshape(3, 16, 16, 128), coarse.reshape(3, 8, 8, 256), energy


def solution(mesh):
    nx, ny = mesh.shape["gx"], mesh.shape["gy"]
    group_x = next(m for m in (4, 2, 1) if nx % m == 0)
    field, cells = P(None, "gx", "gy", None), P("gx", "gy", None)
    return jax.shard_map(
        functools.partial(per_device, nx, ny, group_x),
        mesh=mesh,
        in_specs=(field,) * 4 + (cells,) * 8 + (P(None, "gx", "gy"),),
        out_specs=(field, field, P()),
        check_vma=False,
    )
```

```python
import functools

import jax
import jax.numpy as jnp
from jax import lax
from jax.experimental import pallas as pl
from jax.experimental.pallas import tpu as pltpu
from jax.sharding import PartitionSpec as P

STEPS = 3
DT = 0.15
MESH = pl.DeviceIdType.MESH
F32 = jnp.float32

R = 2
LO, HI = 0, 1
(WIDE, HALF_A, ISV, GB, GZ, DM, CZU, CZD, CXP, CXM, CYU, CYD, C0) = range(13)
NCOEF = 13


def lanes(shape):
    return lax.broadcasted_iota(jnp.int32, shape, len(shape) - 1)


def subs(shape):
    return lax.broadcasted_iota(jnp.int32, shape, len(shape) - 2)


def spread_row(row):
    return jnp.broadcast_to(row, (8, 128))


def roll(x, shift, axis):
    return pltpu.roll(x, shift % x.shape[axis], axis)


class Fine:
    n = 16
    key = "f"

    @staticmethod
    def load(ref, i, r):
        parts = [ref[pl.ds(16 * i + t, 8 * r, stride=2), :].reshape(1, r, 8, 128) for t in (0, 1)]
        return jnp.concatenate(parts, axis=0)

    @staticmethod
    def store(ref, i, r, value):
        for t in (0, 1):
            ref[pl.ds(16 * i + t, 8 * r, stride=2), :] = value[t].reshape(8 * r, 128)

    @staticmethod
    def k_up(x, last=None):
        moved = roll(x, -1, 3)
        edge = x if last is None else last
        return jnp.where(lanes(x.shape) == 127, edge, moved)

    @staticmethod
    def k_down(x, first=None):
        moved = roll(x, 1, 3)
        edge = x if first is None else first
        return jnp.where(lanes(x.shape) == 0, edge, moved)

    @staticmethod
    def edge_scale(shape):
        k = lanes(shape)
        return jnp.where((k == 0) | (k == 127), 1.0, 0.5).astype(F32)

    @staticmethod
    def row_of(ref, i, r):
        return jnp.concatenate(
            [spread_row(ref[pl.ds(i + m, 1), :]).reshape(1, 8, 128) for m in range(r)], axis=0
        )

    @staticmethod
    def j_up(x, halo):
        s = subs(x.shape[1:])
        moved = jnp.where(s == 7, halo, roll(x[0], -1, 1))
        return jnp.stack([x[1], moved])

    @staticmethod
    def j_down(x, halo):
        s = subs(x.shape[1:])
        moved = jnp.where(s == 0, halo, roll(x[1], 1, 1))
        return jnp.stack([moved, x[0]])

    @staticmethod
    def plane(ref, j):
        return jnp.concatenate([ref[pl.ds(j + 128 * h, 8, stride=16), :] for h in (0, 1)], axis=0)

    @staticmethod
    def plane_k_up(x):
        return jnp.where(lanes(x.shape) == 127, x, roll(x, -1, 1))

    @staticmethod
    def plane_k_down(x):
        return jnp.where(lanes(x.shape) == 0, x, roll(x, 1, 1))

    @staticmethod
    def corner_plane(tile_ref, comp):
        row = spread_row(tile_ref[comp])
        return jnp.concatenate([row, row], axis=0)

    @staticmethod
    def corner_row(tile_ref, comp):
        return spread_row(tile_ref[comp]).reshape(1, 8, 128)


class Coarse:
    n = 8
    key = "c"

    @staticmethod
    def load(ref, i, r):
        return ref[:, pl.ds(8 * i, 8 * r), :].reshape(2, r, 8, 128)

    @staticmethod
    def store(ref, i, r, value):
        ref[:, pl.ds(8 * i, 8 * r), :] = value.reshape(2, 8 * r, 128)

    @staticmethod
    def k_up(x, last=None):
        moved = roll(x, -1, 3)
        edge = x[1] if last is None else last
        return jnp.where(lanes(x.shape) == 127, jnp.stack([moved[1], edge]), moved)

    @staticmethod
    def k_down(x, first=None):
        moved = roll(x, 1, 3)
        edge = x[0] if first is None else first
        return jnp.where(lanes(x.shape) == 0, jnp.stack([edge, moved[0]]), moved)

    @staticmethod
    def edge_scale(shape):
        k = lanes(shape)
        half = lax.broadcasted_iota(jnp.int32, shape, 0)
        ends = ((k == 0) & (half == 0)) | ((k == 127) & (half == 1))
        return jnp.where(ends, 1.0, 0.5).astype(F32)

    @staticmethod
    def row_of(ref, i, r):
        halves = []
        for h in (0, 1):
            rows = [spread_row(ref[h, pl.ds(i + m, 1), :]).reshape(1, 8, 128) for m in range(r)]
            halves.append(jnp.concatenate(rows, axis=0))
        return jnp.stack(halves)

    @staticmethod
    def j_up(x, halo):
        return jnp.where(subs(x.shape) == 7, halo, roll(x, -1, 2))

    @staticmethod
    def j_down(x, halo):
        return jnp.where(subs(x.shape) == 0, halo, roll(x, 1, 2))

    @staticmethod
    def plane(ref, j):
        return jnp.stack([ref[h, pl.ds(j, 8, stride=8), :] for h in (0, 1)])

    @staticmethod
    def plane_k_up(x):
        return Coarse.k_up(x[:, None])[:, 0]

    @staticmethod
    def plane_k_down(x):
        return Coarse.k_down(x[:, None])[:, 0]

    @staticmethod
    def corner_plane(tile_ref, comp):
        return jnp.stack([spread_row(tile_ref[2 * comp + h]) for h in (0, 1)])

    @staticmethod
    def corner_row(tile_ref, comp):
        rows = [spread_row(tile_ref[2 * comp + h]) for h in (0, 1)]
        return jnp.stack(rows)[:, None]


def plane_roll(level, x, shift):
    return roll(x, shift, 0) if level is Fine else roll(x, shift, 1)


def plane_sub(level, x):
    return subs(x.shape)


def neighbour_rows(level, ref, i, r, step, halo):
    if step > 0:
        if i + r < level.n:
            return level.load(ref, i + 1, r)
        return halo() if r == 1 else jnp.concatenate([level.load(ref, i + 1, r - 1), halo()], axis=1)
    if i > 0:
        return level.load(ref, i - 1, r)
    return halo() if r == 1 else jnp.concatenate([halo(), level.load(ref, 0, r - 1)], axis=1)


def kernel(nx, ny, group_x, *refs):
    names_in = ["fine_disp", "fine_prev", "coarse_disp", "coarse_prev"]
    for name in ("fine", "coarse"):
        names_in += [name + part for part in ("_density", "_lame", "_rigidity", "_metric")]
    hbm = dict(zip(names_in, refs[:12]))
    offsets_hbm = refs[12]
    fine_out, coarse_out, energy_out = refs[13:16]
    (
        uf, uc, matf, matc, kf, kc, dvf, dvc, dyf, dyc,
        xhf, xhc, yhf, yhc, ysf, ysc, xmf, xmc, ymf, ymc, ysmf, ysmc,
        pls, plx, ply, pex, ccs, ccr, cps, cpr, fcs, fcr, offsets_ref, weights, ghost, eacc, erow, er1, er2,
        load_sem, send_sem, recv_sem, esend, erecv, line_sem,
    ) = refs[16:]

    gx, gy = lax.axis_index("gx"), lax.axis_index("gy")
    exists = {
        (dx, dy): functools.reduce(
            jnp.logical_and,
            ([gx > 0] if dx < 0 else [gx < nx - 1] if dx > 0 else [])
            + ([gy > 0] if dy < 0 else [gy < ny - 1] if dy > 0 else []),
        )
        for dx, dy in ((-1, 0), (1, 0), (-1, -1), (-1, 1), (1, -1), (1, 1), (0, -1), (0, 1))
    }
    directions = list(exists)
    corners = [d for d in directions if d[0] and d[1]]
    corner_id = {d: n for n, d in enumerate(corners)}

    def flag(direction):
        return jnp.where(exists[direction], 1.0, 0.0).astype(F32)

    def device(direction):
        return {"gx": gx + direction[0], "gy": gy + direction[1]}

    groups, half = nx // group_x, ny // 2
    gx_hi, gx_lo = gx // group_x, gx % group_x
    chip_y, second = gy // 2, gy % 2 == 1
    first_core = jnp.logical_not(second)
    n1, n2 = group_x * ny, groups
    me1 = gx_lo * ny + gy
    plane_x = [gx_hi * group_x + lax.rem(gx_lo + a, group_x) for a in range(group_x)]
    plane_y = [2 * lax.rem(chip_y + b, half) for b in range(half)]
    line_x = [lax.rem(gx_hi + d, n2) * group_x + gx_lo for d in range(n2)]

    loads = {}

    def start_load(name, dst, sem):
        fine = name.startswith("fine")
        src = hbm[name]
        if fine:
            copies = [pltpu.make_async_copy(src, dst, load_sem.at[sem, 0])]
        else:
            lead = (slice(None),) * (len(src.shape) - 2)
            copies = [
                pltpu.make_async_copy(
                    src.at[lead + (slice(None), pl.ds(128 * h, 128))],
                    dst.at[(slice(None), h) if lead else (h,)],
                    load_sem.at[sem, h],
                )
                for h in (0, 1)
            ]
        for c in copies:
            c.start()
        loads[name] = copies

    plan = [
        ("fine_disp", uf.at[1]), ("coarse_disp", uc.at[1]),
        ("fine_rigidity", matf.at[0]), ("coarse_rigidity", matc.at[0]),
        ("fine_metric", matf.at[1]), ("coarse_metric", matc.at[1]),
        ("fine_density", matf.at[2]), ("fine_lame", matf.at[3]),
        ("coarse_density", matc.at[2]), ("coarse_lame", matc.at[3]),
        ("fine_prev", uf.at[0]), ("coarse_prev", uc.at[0]),
    ]
    for sem, (name, dst) in enumerate(plan):
        start_load(name, dst, sem)

    loads["offsets"] = [pltpu.make_async_copy(offsets_hbm, offsets_ref, load_sem.at[12, 0])]
    loads["offsets"][0].start()

    def wait_load(*names):
        for name in names:
            for c in loads[name]:
                c.wait()

    barrier = pltpu.get_barrier_semaphore()

    def greet(where):
        pl.semaphore_signal(barrier, inc=1, device_id=where, device_id_type=MESH)

    far_first = sorted(range(1, n2), key=lambda d: -min(d, n2 - d))
    by_one = sorted({1, n2 - 1}) if n2 > 1 else []
    by_two = sorted({2, n2 - 2}) if n2 > 3 else []
    for d in by_one:
        greet({"gx": line_x[d], "gy": 2 * chip_y + 1})
    for d in directions:
        @pl.when(exists[d])
        def _(d=d):
            greet(device(d))

    @pl.when(first_core)
    def _():
        greet({"gx": gx, "gy": 2 * chip_y + 1})

    @pl.when(second)
    def _():
        for x in plane_x:
            for y in plane_y:
                if not (x is plane_x[0] and y is plane_y[0]):
                    greet({"gx": x, "gy": y})
                    greet({"gx": x, "gy": y + 1})
        greet({"gx": gx, "gy": 2 * chip_y})

    side_of = {-1: LO, 1: HI}

    def messages(s):
        out = []
        u_f, u_c = uf.at[s + 1], uc.at[s + 1]
        for dx in (-1, 1):
            own, far = side_of[dx], side_of[-dx]
            first, second = (0, 1) if dx < 0 else (15, 14)
            out.append(("fx", (dx, 0), u_f.at[:, pl.ds(16 * first, 16)], xhf.at[s, far, pl.ds(0, 3)]))
            out.append(("fx", (dx, 0), u_f.at[0, pl.ds(16 * second, 16)], xhf.at[s, far, 3]))
            first, second = (0, 1) if dx < 0 else (7, 6)
            out.append(("cx", (dx, 0), u_c.at[:, :, pl.ds(8 * first, 8)], xhc.at[s, far, pl.ds(0, 3)]))
            out.append(("cx", (dx, 0), u_c.at[0, :, pl.ds(8 * second, 8)], xhc.at[s, far, 3]))
            out.append(("cp", (dx, 0), pex.at[s], plx.at[s, far]))
            if s == 0:
                first = 0 if dx < 0 else 15
                out.append(("mf", (dx, 0), matf.at[pl.ds(0, 2), pl.ds(16 * first, 16)], xmf.at[far]))
                first = 0 if dx < 0 else 7
                out.append(("mc", (dx, 0), matc.at[pl.ds(0, 2), :, pl.ds(8 * first, 8)], xmc.at[far]))
        for dy in (-1, 1):
            own, far = side_of[dy], side_of[-dy]
            out.append(("fy", (0, dy), ysf.at[s, own], yhf.at[s, far]))
            out.append(("cy", (0, dy), ysc.at[s, own], yhc.at[s, far]))
            out.append(("cq", (0, dy), pls.at[s], ply.at[s, far]))
            if s == 0:
                out.append(("mf", (0, dy), ysmf.at[own], ymf.at[far]))
                out.append(("mc", (0, dy), ysmc.at[own], ymc.at[far]))
        for d in corners:
            back = corner_id[(-d[0], -d[1])]
            out.append(("co", d, ccs.at[s, corner_id[d]], ccr.at[s, back]))
            out.append(("cp", d, cps.at[s, corner_id[d]], cpr.at[s, back]))
            out.append(("fo", d, fcs.at[s, corner_id[d]], fcr.at[s, back]))
        return out

    copies = []
    for s in range(STEPS):
        entries = []
        for n, (group, d, src, dst) in enumerate(messages(s)):
            def copy(src=src, dst=dst, s=s, n=n, d=d):
                return pltpu.make_async_remote_copy(
                    src_ref=src, dst_ref=dst,
                    send_sem=send_sem.at[s, n], recv_sem=recv_sem.at[s, n],
                    device_id=device(d), device_id_type=MESH,
                )

            entries.append((group, d, copy))
        copies.append(entries)

    def run(s, groups_wanted, what, backwards=False):
        for d in directions:
            mine = [c for g, e, c in copies[s] if g in groups_wanted and e == d]
            if mine:
                @pl.when(exists[(-d[0], -d[1]) if backwards else d])
                def _(mine=mine):
                    for c in mine:
                        getattr(c(), what)()

    def send(s, *wanted):
        run(s, wanted, "start")

    def receive(s, *wanted):
        run(s, wanted, "wait_recv", backwards=True)

    def line_round(stage):
        steps = (by_one, by_two)[stage] if n2 > 3 else []

        @pl.when(second)
        def _():
            for m, d in enumerate(steps):
                pl.semaphore_signal(
                    line_sem.at[stage, m], inc=1,
                    device_id={"gx": line_x[d], "gy": gy}, device_id_type=MESH,
                )

    def line_wait(stage):
        for m in range(len((by_one, by_two)[stage]) if n2 > 3 else 0):
            pl.semaphore_wait(line_sem.at[stage, m], 1)

    def pack_y(level, s):
        u, out = (uf, ysf) if level is Fine else (uc, ysc)
        last = 15 if level is Fine else 7
        for side, (j0, j1) in ((LO, (0, 1)), (HI, (last, last - 1))):
            for c in range(3):
                out[s, side, c] = level.plane(u.at[s + 1, c], j0)
            out[s, side, 3] = level.plane(u.at[s + 1, 1], j1)

    def plane_tile(s, tile, rows):
        lane = lanes((8, 128))
        for c in range(3):
            for i in rows:
                column = uc[s + 1, c, 0, pl.ds(8 * i, 8), 0:1]
                at = 16 * c + 2 * i
                tile = jnp.where((lane == at) | (lane == at + 1), column, tile)
        return tile

    def pack_coarse_corners(s):
        for (dx, dy), n in corner_id.items():
            ci, cj = (0 if dx < 0 else 7), (0 if dy < 0 else 7)
            for c in (0, 1):
                for h in (0, 1):
                    ccs[s, n, 2 * c + h] = uc[s + 1, c, h, pl.ds(8 * ci + cj, 1), :]

    def pack_plane(s):
        edge = plane_tile(s, jnp.zeros((8, 128), F32), (0, 1, 7))
        pex[s] = edge
        pls[s] = plane_tile(s, edge, range(2, 7))
        for (dx, dy), n in corner_id.items():
            for m, j in enumerate((0, 1) if dy < 0 else (7, 7)):
                cps[s, n, m] = edge[j : j + 1]

    def pack_corners(s):
        for (dx, dy), n in corner_id.items():
            fi, fj = (0 if dx < 0 else 15), (0 if dy < 0 else 15)
            for c in (0, 1):
                fcs[s, n, c] = uf[s + 1, c, pl.ds(16 * fi + fj, 1), :]

    for dx in (-1, 1):
        @pl.when(jnp.logical_not(exists[(dx, 0)]))
        def _(side=side_of[dx]):
            for s in range(STEPS):
                xhf[s, side] = jnp.zeros(xhf.shape[2:], F32)
                xhc[s, side] = jnp.zeros(xhc.shape[2:], F32)
                plx[s, side] = jnp.zeros((8, 128), F32)
            xmf[side, 0] = jnp.zeros(xmf.shape[2:], F32)
            xmf[side, 1] = jnp.ones(xmf.shape[2:], F32)
            xmc[side, 0] = jnp.zeros(xmc.shape[2:], F32)
            xmc[side, 1] = jnp.ones(xmc.shape[2:], F32)
    for dy in (-1, 1):
        @pl.when(jnp.logical_not(exists[(0, dy)]))
        def _(side=side_of[dy]):
            for s in range(STEPS):
                yhf[s, side] = jnp.zeros(yhf.shape[2:], F32)
                yhc[s, side] = jnp.zeros(yhc.shape[2:], F32)
                ply[s, side] = jnp.zeros((8, 128), F32)
            ymf[side, 0] = jnp.zeros(ymf.shape[2:], F32)
            ymf[side, 1] = jnp.ones(ymf.shape[2:], F32)
            ymc[side, 0] = jnp.zeros(ymc.shape[2:], F32)
            ymc[side, 1] = jnp.ones(ymc.shape[2:], F32)
    for d in corners:
        @pl.when(jnp.logical_not(exists[d]))
        def _(n=corner_id[d]):
            for s in range(STEPS):
                ccr[s, n] = jnp.zeros(ccr.shape[2:], F32)
                cpr[s, n] = jnp.zeros(cpr.shape[2:], F32)
                fcr[s, n] = jnp.zeros(fcr.shape[2:], F32)

    wait_load("fine_disp", "coarse_disp", "fine_rigidity", "coarse_rigidity", "fine_metric",
              "coarse_metric")
    for c in (0, 1):
        for side, jf, jc in ((LO, 0, 0), (HI, 15, 7)):
            ysmf[side, c] = Fine.plane(matf.at[c], jf)
            ysmc[side, c] = Coarse.plane(matc.at[c], jc)
    pack_y(Fine, 0)
    pack_y(Coarse, 0)
    pack_coarse_corners(0)
    pack_plane(0)
    pack_corners(0)

    greeted = jnp.where(second, n1 // 2 + 2 * len(by_one), n1 // 2).astype(jnp.int32)
    for d in directions:
        greeted = greeted + jnp.where(exists[d], 1, 0).astype(jnp.int32)
    pl.semaphore_wait(barrier, greeted)

    send(0, "co")
    send(0, "cx", "cy", "mc")
    send(0, "fo", "fx", "fy", "mf")
    send(0, "cp", "cq")

    wait_load("fine_density", "fine_lame", "coarse_density", "coarse_lame", "offsets")
    lane8 = lanes((8, 128))
    spread = jnp.where(
        (lanes((16, 128)) % 16 == subs((16, 128))) & (lanes((16, 128)) < 48), 1.0, 0.0
    ).astype(F32)
    for t in (0, 1):
        pick = jnp.where(lanes((8, 16)) == 2 * subs((8, 16)) + t, 1.0, 0.0).astype(F32)
        for axis in (0, 1):
            table = offsets_ref[axis].astype(F32)
            turned = lax.dot_general(
                pick, table, (((1,), (1,)), ((), ())), preferred_element_type=F32
            )
            shift = jnp.dot(turned, spread, preferred_element_type=F32)
            if axis == 0:
                near = jnp.where(lane8 % 2 == 0, 0.75, 0.25).astype(F32)
            else:
                near = jnp.full((8, 128), 0.75 if t == 0 else 0.25, F32)
            for m, value in enumerate((-1.0, 0.0, 1.0, 2.0)):
                weights[t, 4 * axis + m] = jnp.where(shift == value, near, 0.0) + jnp.where(
                    shift == value - 1.0, 1.0 - near, 0.0
                )

    levels = (
        (Coarse, uc, matc, kc, dvc, dyc, xhc, yhc, ysc, xmc, ymc),
        (Fine, uf, matf, kf, dvf, dyf, xhf, yhf, ysf, xmf, ymf),
    )
    for level, u, mat, k, dv, dy_, xh, yh, ys, xm, ym in levels:
        for i in range(0, level.n, R):
            rig, met, den, lam = (level.load(mat.at[m], i, R) for m in range(4))
            scale = level.edge_scale(rig.shape)
            inverse = 1.0 / met
            light = DT / den
            a = inverse * light
            vertical = rig * inverse
            b = (lam + rig) * light
            isv = inverse * scale
            half_a = 0.5 * a
            for slot, value in (
                (WIDE, rig * met), (HALF_A, half_a), (ISV, isv), (GB, 0.5 * b), (GZ, b * isv),
                (DM, den * met), (CZU, half_a * (vertical + level.k_up(vertical))),
                (CZD, half_a * (vertical + level.k_down(vertical))),
            ):
                level.store(k.at[slot], i, R, value)

    def halo_row(level, ref):
        if level is Fine:
            return Fine.load(ref, 0, 1)
        return Coarse.load(ref, 0, 1)

    def side_coefficients(level, mat, k, xm, ym):
        for i in range(0, level.n, R):
            w = level.load(k.at[WIDE], i, R)
            ha = level.load(k.at[HALF_A], i, R)

            def outer(side):
                return halo_row(level, xm.at[side, 0]) * halo_row(level, xm.at[side, 1])

            cxp = ha * (w + neighbour_rows(level, k.at[WIDE], i, R, 1, lambda: outer(HI)))
            cxm = ha * (w + neighbour_rows(level, k.at[WIDE], i, R, -1, lambda: outer(LO)))
            up = level.row_of(ym.at[HI, 0], i, R) * level.row_of(ym.at[HI, 1], i, R)
            down = level.row_of(ym.at[LO, 0], i, R) * level.row_of(ym.at[LO, 1], i, R)
            cyu = ha * (w + level.j_up(w, up))
            cyd = ha * (w + level.j_down(w, down))
            total = cxp + cxm + cyu + cyd + level.load(k.at[CZU], i, R) + level.load(k.at[CZD], i, R)
            for slot, value in ((CXP, cxp), (CXM, cxm), (CYU, cyu), (CYD, cyd), (C0, total)):
                level.store(k.at[slot], i, R, value)

    def row_divergence(s, i, r, level, u, mat, k, dv, dy_, xh, yh, ys, xm, ym):
        now = u.at[s + 1]

        def halo(side):
            return lambda: halo_row(level, xh.at[s, side, 0])

        px = neighbour_rows(level, now.at[0], i, r, 1, halo(HI))
        mx = neighbour_rows(level, now.at[0], i, r, -1, halo(LO))
        y = level.load(now.at[1], i, r)
        z = level.load(now.at[2], i, r)
        py = level.j_up(y, level.row_of(yh.at[s, HI, 1], i, r))
        my = level.j_down(y, level.row_of(yh.at[s, LO, 1], i, r))
        isv = level.load(k.at[ISV], i, r)
        value = 0.5 * ((px - mx) + (py - my)) + isv * (level.k_up(z) - level.k_down(z))
        level.store(dv, i + 1, r, value)

    def x_side_divergence(s, level, u, mat, k, dv, dy_, xh, yh, ys, xm, ym):
        cor = fcr if level is Fine else ccr
        now, n = u.at[s + 1], level.n
        for dx, side in side_of.items():
            inside = level.load(now.at[0], 0 if dx < 0 else n - 1, 1)
            beyond = halo_row(level, xh.at[s, side, 3])
            y = halo_row(level, xh.at[s, side, 1])
            z = halo_row(level, xh.at[s, side, 2])
            py = level.j_up(y, level.corner_row(cor.at[s, corner_id[(dx, 1)]], 1))
            my = level.j_down(y, level.corner_row(cor.at[s, corner_id[(dx, -1)]], 1))
            isv = level.edge_scale(z.shape) / halo_row(level, xm.at[side, 1])
            along = (beyond - inside) if dx > 0 else (inside - beyond)
            value = 0.5 * (along + (py - my)) + isv * (level.k_up(z) - level.k_down(z))
            level.store(dv, 0 if dx < 0 else n + 1, 1, value * flag((dx, 0)))

    def y_side_divergence(s, with_corners, level, u, mat, k, dv, dy_, xh, yh, ys, xm, ym):
        cor = fcr if level is Fine else ccr
        n = level.n
        for dy, side in side_of.items():
            x, z, beyond = yh[s, side, 0], yh[s, side, 2], yh[s, side, 3]
            inside = ys[s, side, 1]
            sub = plane_sub(level, x)
            px, mx = plane_roll(level, x, -1), plane_roll(level, x, 1)
            if with_corners:
                px = jnp.where(sub == n - 1, level.corner_plane(cor.at[s, corner_id[(1, dy)]], 0), px)
                mx = jnp.where(sub == 0, level.corner_plane(cor.at[s, corner_id[(-1, dy)]], 0), mx)
            isv = level.edge_scale(z.shape) / ym[side, 1]
            along = (beyond - inside) if dy > 0 else (inside - beyond)
            value = 0.5 * (along + (px - mx)) + isv * (level.plane_k_up(z) - level.plane_k_down(z))
            dy_[side] = value * flag((0, dy))

    def middle(s, level, *rest):
        n = level.n
        y_side_divergence(s, False, level, *rest)
        row_divergence(s, 1, 1, level, *rest)
        for i in range(2, n - 2, R):
            row_divergence(s, i, R, level, *rest)
        row_divergence(s, n - 2, 1, level, *rest)
        total = jnp.zeros((8, 128), F32)
        for i in range(R, n - R, R):
            total = total + rates(s, i, level, *rest)
        return total

    def outer(s, level, *rest):
        n = level.n
        x_side_divergence(s, level, *rest)
        y_side_divergence(s, True, level, *rest)
        for i in (0, n - 1):
            row_divergence(s, i, 1, level, *rest)
        return rates(s, 0, level, *rest) + rates(s, n - R, level, *rest)

    def fine_ghosts(s):
        sub, lane = subs((8, 128)), lanes((8, 128)) % 16

        def shifted_rows(tile, low, high0, high1):
            return [
                jnp.where(sub == 0, low, roll(tile, 1, 0)),
                tile,
                jnp.where(sub == 7, high0, roll(tile, -1, 0)),
                jnp.where(sub == 7, high1, jnp.where(sub == 6, high0, roll(tile, -2, 0))),
            ]

        def row(ref, j):
            return spread_row(ref[pl.ds(j, 1), :])

        def corner_rows(dx):
            low, high = cpr.at[s, corner_id[(dx, -1)]], cpr.at[s, corner_id[(dx, 1)]]
            return spread_row(low[0]), spread_row(high[0]), spread_row(high[1])

        own = shifted_rows(pls[s], row(ply.at[s, LO], 7), row(ply.at[s, HI], 0), row(ply.at[s, HI], 1))
        left = shifted_rows(plx[s, LO], *corner_rows(-1))
        right = shifted_rows(plx[s, HI], *corner_rows(1))
        totals = [jnp.zeros((8, 128), F32) for _ in (0, 1)]
        for mx in range(4):
            inner = [jnp.zeros((8, 128), F32) for _ in (0, 1)]
            for my in range(4):
                if mx == 0:
                    tile = jnp.where(lane < 2, roll(left[my], -14, 1), roll(own[my], 2, 1))
                elif mx == 1:
                    tile = own[my]
                elif mx == 2:
                    tile = jnp.where(lane >= 14, roll(right[my], 14, 1), roll(own[my], -2, 1))
                else:
                    tile = jnp.where(lane >= 12, roll(right[my], 12, 1), roll(own[my], -4, 1))
                for t in (0, 1):
                    inner[t] = inner[t] + weights[t, 4 + my] * tile
            for t in (0, 1):
                totals[t] = totals[t] + weights[t, mx] * inner[t]
        for t in (0, 1):
            ghost[t] = totals[t]

    def fine_last(c, i):
        rows = []
        for t in (0, 1):
            tile = ghost[t]
            rows.append(jnp.stack([roll(tile, 127 - (16 * c + i + m), 1) for m in range(R)]))
        return jnp.stack(rows)

    def coarse_first(s, c, i):
        rows = []
        for m in range(R):
            base = 32 * (i + m)
            parts = [uf[s + 1, c, pl.ds(base + t, 8, stride=2), :] for t in (0, 1, 16, 17)]
            rows.append(0.25 * ((parts[0] + parts[1]) + (parts[2] + parts[3])))
        return roll(jnp.stack(rows), 1, 2)

    def rates(s, i, level, u, mat, k, dv, dy_, xh, yh, ys, xm, ym):
        now, old = u.at[s + 1], u.at[s]
        coef = {
            m: level.load(k.at[m], i, R) for m in (GB, GZ, DM, CZU, CZD, CXP, CXM, CYU, CYD, C0)
        }
        d_mid = level.load(dv, i + 1, R)
        gradient = [
            coef[GB] * (level.load(dv, i + 2, R) - level.load(dv, i, R)),
            coef[GB]
            * (
                level.j_up(d_mid, level.row_of(dy_.at[HI], i, R))
                - level.j_down(d_mid, level.row_of(dy_.at[LO], i, R))
            ),
            coef[GZ] * (level.k_up(d_mid) - level.k_down(d_mid)),
        ]
        energy = None
        for c in range(3):
            v = level.load(now.at[c], i, R)

            def halo(side, c=c):
                return lambda: halo_row(level, xh.at[s, side, c])

            px = neighbour_rows(level, now.at[c], i, R, 1, halo(HI))
            mx = neighbour_rows(level, now.at[c], i, R, -1, halo(LO))
            py = level.j_up(v, level.row_of(yh.at[s, HI, c], i, R))
            my = level.j_down(v, level.row_of(yh.at[s, LO, c], i, R))
            if level is Fine:
                pz, mz = level.k_up(v, fine_last(c, i)), level.k_down(v)
            else:
                pz = level.k_up(v, jnp.zeros_like(v[1]))
                mz = level.k_down(v, coarse_first(s, c, i))
            rate = (
                (coef[CXP] * px + coef[CXM] * mx)
                + (coef[CYU] * py + coef[CYD] * my)
                + (coef[CZU] * pz + coef[CZD] * mz)
                - coef[C0] * v
                + gradient[c]
            )
            after = (2.0 * v - level.load(old.at[c], i, R)) + rate
            if s < STEPS - 1:
                level.store(u.at[s + 2, c], i, R, after)
            elif level is Fine:
                level.store(fine_out.at[c], i, R, after)
            else:
                for h in (0, 1):
                    coarse_out[c, pl.ds(8 * i, 8 * R), pl.ds(128 * h, 128)] = after[h].reshape(
                        8 * R, 128
                    )
            change = after - v
            part = change * change - after * rate
            energy = part if energy is None else energy + part
        return jnp.sum(coef[DM] * energy, axis=(0, 1))

    coarse_set, fine_set = levels
    for s in range(STEPS):
        last = s == STEPS - 1
        receive(s, "cy")
        if s == 0:
            receive(0, "mc")
            side_coefficients(Coarse, matc, kc, xmc, ymc)
            wait_load("coarse_prev")
        total = middle(s, *coarse_set)
        receive(s, "co", "cx")
        eacc[s, 1] = total + outer(s, *coarse_set)
        if not last:
            pack_coarse_corners(s + 1)
            send(s + 1, "co")
            send(s + 1, "cx")
            pack_y(Coarse, s + 1)
            pack_plane(s + 1)
            send(s + 1, "cy", "cq", "cp")
        receive(s, "cp", "cq", "fy")
        if s == 0:
            receive(0, "mf")
            side_coefficients(Fine, matf, kf, xmf, ymf)
            wait_load("fine_prev")
        fine_ghosts(s)
        total = middle(s, *fine_set)
        receive(s, "fo", "fx")
        eacc[s, 0] = total + outer(s, *fine_set)
        if not last:
            pack_corners(s + 1)
            send(s + 1, "fo")
            send(s + 1, "fx")
            pack_y(Fine, s + 1)
            send(s + 1, "fy")
        if s == 0:
            line_round(0)
        if s == 1:
            @pl.when(second)
            def _():
                line_wait(0)

            line_round(1)

    lane1 = lanes((1, 128))
    row = jnp.zeros((1, 128), F32)
    cells = (nx * ny * 16 * 16 * 128, nx * ny * 8 * 8 * 256)
    for s in range(STEPS):
        for m in (0, 1):
            value = jnp.sum(eacc[s, m], axis=0, keepdims=True)
            value = jnp.sum(value, axis=1, keepdims=True)
            row = jnp.where(lane1 == STEPS * m + s, value * (1.0 / cells[m]), row)
    erow[0] = row
    er1[me1] = row

    def rows(buffer, n, stage):
        part = buffer.at[pl.ds(0, n)]
        return pltpu.make_async_remote_copy(
            src_ref=part, dst_ref=part, send_sem=esend.at[stage], recv_sem=erecv.at[stage],
            device_id={"gx": line_x[0], "gy": gy}, device_id_type=MESH,
        )

    def pass_on(stage, slot, where):
        pltpu.make_async_remote_copy(
            src_ref=erow.at[stage], dst_ref=slot, send_sem=esend.at[stage],
            recv_sem=erecv.at[stage], device_id=where, device_id_type=MESH,
        ).start()

    for a in reversed(range(group_x)):
        for b in reversed(range(half)):
            if a or b:
                pass_on(0, er1.at[me1], {"gx": plane_x[a], "gy": plane_y[b] + 1})

    @pl.when(first_core)
    def _():
        pass_on(0, er1.at[me1], {"gx": gx, "gy": 2 * chip_y + 1})

    @pl.when(second)
    def _():
        rows(er1, n1 - 1, 0).wait_recv()
        plane = er1[0]
        for m in range(1, n1):
            plane = plane + er1[m]
        erow[1] = plane
        er2[gx_hi] = plane
        line_wait(1)
        for d in far_first:
            for core in (0, 1):
                pass_on(1, er2.at[gx_hi], {"gx": line_x[d], "gy": 2 * chip_y + core})
        pass_on(1, er2.at[gx_hi], {"gx": gx, "gy": 2 * chip_y})
        if n2 > 1:
            rows(er2, n2 - 1, 1).wait_recv()

    @pl.when(first_core)
    def _():
        rows(er2, n2, 1).wait_recv()

    row = er2[0]
    for m in range(1, n2):
        row = row + er2[m]
    for m in (0, 1):
        energy_out[pl.ds(m, 1), :] = roll(row, -STEPS * m, 1)[:, 0:STEPS]

    @pl.when(second)
    def _():
        rows(er1, n1 // 2 - 1, 0).wait_send()
        rows(er1, 2 * n2 - 1, 1).wait_send()

    @pl.when(first_core)
    def _():
        rows(er1, n1 // 2, 0).wait_send()

    for s in range(STEPS):
        run(s, ("co", "cp", "cq", "fo", "cx", "cy", "mc", "mf", "fx", "fy"), "wait_send")


def hand_out(*refs):
    copies = [pltpu.make_async_copy(refs[n], refs[3 + n], refs[6].at[n]) for n in range(3)]
    for c in copies:
        c.start()
    for c in copies:
        c.wait()


def per_device(nx, ny, group_x, *args):
    args = list(args)
    for m in range(4):
        shape = args[m].shape
        args[m] = args[m].reshape(shape[0], shape[1] * shape[2], shape[3])
    for m in range(4, 12):
        shape = args[m].shape
        args[m] = args[m].reshape(shape[0] * shape[1], shape[2])
    for m in range(13):
        args[m] = pltpu.with_memory_space_constraint(args[m], pltpu.HBM)
    vm, dma = pltpu.VMEM, pltpu.SemaphoreType.DMA
    n1, n2 = group_x * ny, nx // group_x
    scratch = [
        vm((STEPS + 1, 3, 256, 128), F32),
        vm((STEPS + 1, 3, 2, 64, 128), F32),
        vm((4, 256, 128), F32),
        vm((4, 2, 64, 128), F32),
        vm((NCOEF, 256, 128), F32),
        vm((NCOEF, 2, 64, 128), F32),
        vm((18 * 16, 128), F32),
        vm((2, 10 * 8, 128), F32),
        vm((2, 16, 128), F32),
        vm((2, 2, 8, 128), F32),
        vm((STEPS, 2, 4, 16, 128), F32),
        vm((STEPS, 2, 4, 2, 8, 128), F32),
        vm((STEPS, 2, 4, 16, 128), F32),
        vm((STEPS, 2, 4, 2, 8, 128), F32),
        vm((STEPS, 2, 4, 16, 128), F32),
        vm((STEPS, 2, 4, 2, 8, 128), F32),
        vm((2, 2, 16, 128), F32),
        vm((2, 2, 2, 8, 128), F32),
        vm((2, 2, 16, 128), F32),
        vm((2, 2, 2, 8, 128), F32),
        vm((2, 2, 16, 128), F32),
        vm((2, 2, 2, 8, 128), F32),
        vm((STEPS, 8, 128), F32),
        vm((STEPS, 2, 8, 128), F32),
        vm((STEPS, 2, 8, 128), F32),
        vm((STEPS, 8, 128), F32),
        vm((STEPS, 4, 4, 1, 128), F32),
        vm((STEPS, 4, 4, 1, 128), F32),
        vm((STEPS, 4, 2, 1, 128), F32),
        vm((STEPS, 4, 2, 1, 128), F32),
        vm((STEPS, 4, 2, 1, 128), F32),
        vm((STEPS, 4, 2, 1, 128), F32),
        vm((2, 16, 16), jnp.int32),
        vm((2, 8, 8, 128), F32),
        vm((2, 8, 128), F32),
        vm((STEPS, 2, 8, 128), F32),
        vm((2, 1, 128), F32),
        vm((max(n1, 2 * n2), 1, 128), F32),
        vm((max(n2, 1), 1, 128), F32),
        dma((13, 2)),
        dma((STEPS, 36)),
        dma((STEPS, 36)),
        dma((2,)),
        dma((2,)),
        pltpu.SemaphoreType.REGULAR((2, 2)),
    ]
    anywhere = pl.BlockSpec(memory_space=pltpu.HBM)
    in_vmem = pl.BlockSpec(memory_space=pltpu.VMEM)
    out_shape = (
        jax.ShapeDtypeStruct((3, 256, 128), F32),
        jax.ShapeDtypeStruct((3, 64, 256), F32),
        jax.ShapeDtypeStruct((2, STEPS), F32),
    )
    results = pl.pallas_call(
        functools.partial(kernel, nx, ny, group_x),
        out_shape=out_shape,
        in_specs=[anywhere] * 13,
        out_specs=(in_vmem, in_vmem, in_vmem),
        scratch_shapes=scratch,
        compiler_params=pltpu.CompilerParams(
            collective_id=0, has_side_effects=True, vmem_limit_bytes=32 << 20
        ),
        name="leapfrog",
    )(*args)
    fine, coarse, energy = pl.pallas_call(
        hand_out,
        out_shape=out_shape,
        in_specs=[in_vmem] * 3,
        out_specs=[anywhere] * 3,
        scratch_shapes=[dma((3,))],
        compiler_params=pltpu.CompilerParams(vmem_limit_bytes=1 << 20),
        name="hand_out",
    )(*results)
    energy = energy.T
    return fine.reshape(3, 16, 16, 128), coarse.reshape(3, 8, 8, 256), energy


def solution(mesh):
    nx, ny = mesh.shape["gx"], mesh.shape["gy"]
    group_x = next(m for m in (4, 2, 1) if nx % m == 0)
    field, cells = P(None, "gx", "gy", None), P("gx", "gy", None)
    return jax.shard_map(
        functools.partial(per_device, nx, ny, group_x),
        mesh=mesh,
        in_specs=(field,) * 4 + (cells,) * 8 + (P(None, "gx", "gy"),),
        out_specs=(field, field, P()),
        check_vma=False,
    )
```

```python
import functools

import jax
import jax.numpy as jnp
from jax import lax
from jax.experimental import pallas as pl
from jax.experimental.pallas import tpu as pltpu
from jax.sharding import PartitionSpec as P

STEPS = 3
DT = 0.15
MESH = pl.DeviceIdType.MESH
F32 = jnp.float32

R = 2
LO, HI = 0, 1
(WIDE, HALF_A, ISV, GB, GZ, DM, CZU, CZD, CXP, CXM, CYU, CYD, C0) = range(13)
NCOEF = 13


def lanes(shape):
    return lax.broadcasted_iota(jnp.int32, shape, len(shape) - 1)


def subs(shape):
    return lax.broadcasted_iota(jnp.int32, shape, len(shape) - 2)


def spread_row(row):
    return jnp.broadcast_to(row, (8, 128))


def roll(x, shift, axis):
    return pltpu.roll(x, shift % x.shape[axis], axis)


class Fine:
    n = 16
    key = "f"

    @staticmethod
    def load(ref, i, r):
        parts = [ref[pl.ds(16 * i + t, 8 * r, stride=2), :].reshape(1, r, 8, 128) for t in (0, 1)]
        return jnp.concatenate(parts, axis=0)

    @staticmethod
    def store(ref, i, r, value):
        for t in (0, 1):
            ref[pl.ds(16 * i + t, 8 * r, stride=2), :] = value[t].reshape(8 * r, 128)

    @staticmethod
    def k_up(x, last=None):
        moved = roll(x, -1, 3)
        edge = x if last is None else last
        return jnp.where(lanes(x.shape) == 127, edge, moved)

    @staticmethod
    def k_down(x, first=None):
        moved = roll(x, 1, 3)
        edge = x if first is None else first
        return jnp.where(lanes(x.shape) == 0, edge, moved)

    @staticmethod
    def edge_scale(shape):
        k = lanes(shape)
        return jnp.where((k == 0) | (k == 127), 1.0, 0.5).astype(F32)

    @staticmethod
    def row_of(ref, i, r):
        return jnp.concatenate(
            [spread_row(ref[pl.ds(i + m, 1), :]).reshape(1, 8, 128) for m in range(r)], axis=0
        )

    @staticmethod
    def j_up(x, halo):
        s = subs(x.shape[1:])
        moved = jnp.where(s == 7, halo, roll(x[0], -1, 1))
        return jnp.stack([x[1], moved])

    @staticmethod
    def j_down(x, halo):
        s = subs(x.shape[1:])
        moved = jnp.where(s == 0, halo, roll(x[1], 1, 1))
        return jnp.stack([moved, x[0]])

    @staticmethod
    def plane(ref, j):
        return jnp.concatenate([ref[pl.ds(j + 128 * h, 8, stride=16), :] for h in (0, 1)], axis=0)

    @staticmethod
    def plane_k_up(x):
        return jnp.where(lanes(x.shape) == 127, x, roll(x, -1, 1))

    @staticmethod
    def plane_k_down(x):
        return jnp.where(lanes(x.shape) == 0, x, roll(x, 1, 1))

    @staticmethod
    def corner_plane(tile_ref, comp):
        row = spread_row(tile_ref[comp])
        return jnp.concatenate([row, row], axis=0)

    @staticmethod
    def corner_row(tile_ref, comp):
        return spread_row(tile_ref[comp]).reshape(1, 8, 128)


class Coarse:
    n = 8
    key = "c"

    @staticmethod
    def load(ref, i, r):
        return ref[:, pl.ds(8 * i, 8 * r), :].reshape(2, r, 8, 128)

    @staticmethod
    def store(ref, i, r, value):
        ref[:, pl.ds(8 * i, 8 * r), :] = value.reshape(2, 8 * r, 128)

    @staticmethod
    def k_up(x, last=None):
        moved = roll(x, -1, 3)
        edge = x[1] if last is None else last
        return jnp.where(lanes(x.shape) == 127, jnp.stack([moved[1], edge]), moved)

    @staticmethod
    def k_down(x, first=None):
        moved = roll(x, 1, 3)
        edge = x[0] if first is None else first
        return jnp.where(lanes(x.shape) == 0, jnp.stack([edge, moved[0]]), moved)

    @staticmethod
    def edge_scale(shape):
        k = lanes(shape)
        half = lax.broadcasted_iota(jnp.int32, shape, 0)
        ends = ((k == 0) & (half == 0)) | ((k == 127) & (half == 1))
        return jnp.where(ends, 1.0, 0.5).astype(F32)

    @staticmethod
    def row_of(ref, i, r):
        halves = []
        for h in (0, 1):
            rows = [spread_row(ref[h, pl.ds(i + m, 1), :]).reshape(1, 8, 128) for m in range(r)]
            halves.append(jnp.concatenate(rows, axis=0))
        return jnp.stack(halves)

    @staticmethod
    def j_up(x, halo):
        return jnp.where(subs(x.shape) == 7, halo, roll(x, -1, 2))

    @staticmethod
    def j_down(x, halo):
        return jnp.where(subs(x.shape) == 0, halo, roll(x, 1, 2))

    @staticmethod
    def plane(ref, j):
        return jnp.stack([ref[h, pl.ds(j, 8, stride=8), :] for h in (0, 1)])

    @staticmethod
    def plane_k_up(x):
        return Coarse.k_up(x[:, None])[:, 0]

    @staticmethod
    def plane_k_down(x):
        return Coarse.k_down(x[:, None])[:, 0]

    @staticmethod
    def corner_plane(tile_ref, comp):
        return jnp.stack([spread_row(tile_ref[2 * comp + h]) for h in (0, 1)])

    @staticmethod
    def corner_row(tile_ref, comp):
        rows = [spread_row(tile_ref[2 * comp + h]) for h in (0, 1)]
        return jnp.stack(rows)[:, None]


def plane_roll(level, x, shift):
    return roll(x, shift, 0) if level is Fine else roll(x, shift, 1)


def plane_sub(level, x):
    return subs(x.shape)


def neighbour_rows(level, ref, i, r, step, halo):
    if step > 0:
        if i + r < level.n:
            return level.load(ref, i + 1, r)
        return halo() if r == 1 else jnp.concatenate([level.load(ref, i + 1, r - 1), halo()], axis=1)
    if i > 0:
        return level.load(ref, i - 1, r)
    return halo() if r == 1 else jnp.concatenate([halo(), level.load(ref, 0, r - 1)], axis=1)


def kernel(nx, ny, group_x, *refs):
    names_in = ["fine_disp", "fine_prev", "coarse_disp", "coarse_prev"]
    for name in ("fine", "coarse"):
        names_in += [name + part for part in ("_density", "_lame", "_rigidity", "_metric")]
    hbm = dict(zip(names_in, refs[:12]))
    offsets_hbm = refs[12]
    fine_out, coarse_out, energy_out = refs[13:16]
    (
        uf, uc, matf, matc, kf, kc, dvf, dvc, dyf, dyc,
        xhf, xhc, yhf, yhc, ysf, ysc, xmf, xmc, ymf, ymc, ysmf, ysmc,
        pls, plx, ply, pex, ccs, ccr, cps, cpr, fcs, fcr, offsets_ref, weights, ghost, eacc, erow, er1, er2,
        load_sem, send_sem, recv_sem, esend, erecv, line_sem,
    ) = refs[16:]

    gx, gy = lax.axis_index("gx"), lax.axis_index("gy")
    exists = {
        (dx, dy): functools.reduce(
            jnp.logical_and,
            ([gx > 0] if dx < 0 else [gx < nx - 1] if dx > 0 else [])
            + ([gy > 0] if dy < 0 else [gy < ny - 1] if dy > 0 else []),
        )
        for dx, dy in ((-1, 0), (1, 0), (-1, -1), (-1, 1), (1, -1), (1, 1), (0, -1), (0, 1))
    }
    directions = list(exists)
    corners = [d for d in directions if d[0] and d[1]]
    corner_id = {d: n for n, d in enumerate(corners)}

    def flag(direction):
        return jnp.where(exists[direction], 1.0, 0.0).astype(F32)

    def device(direction):
        return {"gx": gx + direction[0], "gy": gy + direction[1]}

    groups, half = nx // group_x, ny // 2
    gx_hi, gx_lo = gx // group_x, gx % group_x
    chip_y, second = gy // 2, gy % 2 == 1
    first_core = jnp.logical_not(second)
    n1, n2 = group_x * ny, groups
    me1 = gx_lo * ny + gy
    plane_x = [gx_hi * group_x + lax.rem(gx_lo + a, group_x) for a in range(group_x)]
    plane_y = [2 * lax.rem(chip_y + b, half) for b in range(half)]
    line_x = [lax.rem(gx_hi + d, n2) * group_x + gx_lo for d in range(n2)]

    loads = {}

    def start_load(name, dst, sem):
        fine = name.startswith("fine")
        src = hbm[name]
        if fine:
            copies = [pltpu.make_async_copy(src, dst, load_sem.at[sem, 0])]
        else:
            lead = (slice(None),) * (len(src.shape) - 2)
            copies = [
                pltpu.make_async_copy(
                    src.at[lead + (slice(None), pl.ds(128 * h, 128))],
                    dst.at[(slice(None), h) if lead else (h,)],
                    load_sem.at[sem, h],
                )
                for h in (0, 1)
            ]
        for c in copies:
            c.start()
        loads[name] = copies

    plan = [
        ("fine_disp", uf.at[1]), ("coarse_disp", uc.at[1]),
        ("fine_rigidity", matf.at[0]), ("coarse_rigidity", matc.at[0]),
        ("fine_metric", matf.at[1]), ("coarse_metric", matc.at[1]),
        ("fine_density", matf.at[2]), ("fine_lame", matf.at[3]),
        ("coarse_density", matc.at[2]), ("coarse_lame", matc.at[3]),
        ("fine_prev", uf.at[0]), ("coarse_prev", uc.at[0]),
    ]
    for sem, (name, dst) in enumerate(plan):
        start_load(name, dst, sem)

    loads["offsets"] = [pltpu.make_async_copy(offsets_hbm, offsets_ref, load_sem.at[12, 0])]
    loads["offsets"][0].start()

    def wait_load(*names):
        for name in names:
            for c in loads[name]:
                c.wait()

    barrier = pltpu.get_barrier_semaphore()

    def greet(where):
        pl.semaphore_signal(barrier, inc=1, device_id=where, device_id_type=MESH)

    far_first = sorted(range(1, n2), key=lambda d: -min(d, n2 - d))
    by_one = sorted({1, n2 - 1}) if n2 > 1 else []
    by_two = sorted({2, n2 - 2}) if n2 > 3 else []
    for d in by_one:
        greet({"gx": line_x[d], "gy": 2 * chip_y + 1})
    for d in directions:
        @pl.when(exists[d])
        def _(d=d):
            greet(device(d))

    @pl.when(first_core)
    def _():
        greet({"gx": gx, "gy": 2 * chip_y + 1})

    @pl.when(second)
    def _():
        for x in plane_x:
            for y in plane_y:
                if not (x is plane_x[0] and y is plane_y[0]):
                    greet({"gx": x, "gy": y})
                    greet({"gx": x, "gy": y + 1})
        greet({"gx": gx, "gy": 2 * chip_y})

    side_of = {-1: LO, 1: HI}

    def messages(s):
        out = []
        u_f, u_c = uf.at[s + 1], uc.at[s + 1]
        for dx in (-1, 1):
            own, far = side_of[dx], side_of[-dx]
            first, second = (0, 1) if dx < 0 else (15, 14)
            out.append(("fx", (dx, 0), u_f.at[:, pl.ds(16 * first, 16)], xhf.at[s, far, pl.ds(0, 3)]))
            out.append(("fx", (dx, 0), u_f.at[0, pl.ds(16 * second, 16)], xhf.at[s, far, 3]))
            first, second = (0, 1) if dx < 0 else (7, 6)
            out.append(("cx", (dx, 0), u_c.at[:, :, pl.ds(8 * first, 8)], xhc.at[s, far, pl.ds(0, 3)]))
            out.append(("cx", (dx, 0), u_c.at[0, :, pl.ds(8 * second, 8)], xhc.at[s, far, 3]))
            out.append(("cp", (dx, 0), pex.at[s], plx.at[s, far]))
            if s == 0:
                first = 0 if dx < 0 else 15
                out.append(("mf", (dx, 0), matf.at[pl.ds(0, 2), pl.ds(16 * first, 16)], xmf.at[far]))
                first = 0 if dx < 0 else 7
                out.append(("mc", (dx, 0), matc.at[pl.ds(0, 2), :, pl.ds(8 * first, 8)], xmc.at[far]))
        for dy in (-1, 1):
            own, far = side_of[dy], side_of[-dy]
            out.append(("fy", (0, dy), ysf.at[s, own], yhf.at[s, far]))
            out.append(("cy", (0, dy), ysc.at[s, own], yhc.at[s, far]))
            out.append(("cq", (0, dy), pls.at[s], ply.at[s, far]))
            if s == 0:
                out.append(("mf", (0, dy), ysmf.at[own], ymf.at[far]))
                out.append(("mc", (0, dy), ysmc.at[own], ymc.at[far]))
        for d in corners:
            back = corner_id[(-d[0], -d[1])]
            out.append(("co", d, ccs.at[s, corner_id[d]], ccr.at[s, back]))
            out.append(("cp", d, cps.at[s, corner_id[d]], cpr.at[s, back]))
            out.append(("fo", d, fcs.at[s, corner_id[d]], fcr.at[s, back]))
        return out

    copies = []
    for s in range(STEPS):
        entries = []
        for n, (group, d, src, dst) in enumerate(messages(s)):
            def copy(src=src, dst=dst, s=s, n=n, d=d):
                return pltpu.make_async_remote_copy(
                    src_ref=src, dst_ref=dst,
                    send_sem=send_sem.at[s, n], recv_sem=recv_sem.at[s, n],
                    device_id=device(d), device_id_type=MESH,
                )

            entries.append((group, d, copy))
        copies.append(entries)

    def run(s, groups_wanted, what, backwards=False, dx=None):
        for d in directions:
            mine = [c for g, e, c in copies[s] if g in groups_wanted and e == d]
            if mine and dx in (None, d[0]):
                @pl.when(exists[(-d[0], -d[1]) if backwards else d])
                def _(mine=mine):
                    for c in mine:
                        getattr(c(), what)()

    def send(s, *wanted, dx=None):
        run(s, wanted, "start", dx=dx)

    def receive(s, *wanted, side=None):
        run(s, wanted, "wait_recv", backwards=True, dx=None if side is None else -side)

    def line_round(stage):
        steps = (by_one, by_two)[stage] if n2 > 3 else []

        @pl.when(second)
        def _():
            for m, d in enumerate(steps):
                pl.semaphore_signal(
                    line_sem.at[stage, m], inc=1,
                    device_id={"gx": line_x[d], "gy": gy}, device_id_type=MESH,
                )

    def line_wait(stage):
        for m in range(len((by_one, by_two)[stage]) if n2 > 3 else 0):
            pl.semaphore_wait(line_sem.at[stage, m], 1)

    def pack_y(level, s):
        u, out = (uf, ysf) if level is Fine else (uc, ysc)
        last = 15 if level is Fine else 7
        for side, (j0, j1) in ((LO, (0, 1)), (HI, (last, last - 1))):
            for c in range(3):
                out[s, side, c] = level.plane(u.at[s + 1, c], j0)
            out[s, side, 3] = level.plane(u.at[s + 1, 1], j1)

    def plane_tile(s, tile, rows):
        lane = lanes((8, 128))
        for c in range(3):
            for i in rows:
                column = uc[s + 1, c, 0, pl.ds(8 * i, 8), 0:1]
                at = 16 * c + 2 * i
                tile = jnp.where((lane == at) | (lane == at + 1), column, tile)
        return tile

    def pack_coarse_corners(s, side):
        for (dx, dy), n in corner_id.items():
            if dx != side:
                continue
            ci, cj = (0 if dx < 0 else 7), (0 if dy < 0 else 7)
            for c in (0, 1):
                for h in (0, 1):
                    ccs[s, n, 2 * c + h] = uc[s + 1, c, h, pl.ds(8 * ci + cj, 1), :]

    def pack_plane(s):
        edge = plane_tile(s, jnp.zeros((8, 128), F32), (0, 1, 7))
        pex[s] = edge
        pls[s] = plane_tile(s, edge, range(2, 7))
        for (dx, dy), n in corner_id.items():
            for m, j in enumerate((0, 1) if dy < 0 else (7, 7)):
                cps[s, n, m] = edge[j : j + 1]

    def pack_corners(s, side):
        for (dx, dy), n in corner_id.items():
            if dx != side:
                continue
            fi, fj = (0 if dx < 0 else 15), (0 if dy < 0 else 15)
            for c in (0, 1):
                fcs[s, n, c] = uf[s + 1, c, pl.ds(16 * fi + fj, 1), :]

    for dx in (-1, 1):
        @pl.when(jnp.logical_not(exists[(dx, 0)]))
        def _(side=side_of[dx]):
            for s in range(STEPS):
                xhf[s, side] = jnp.zeros(xhf.shape[2:], F32)
                xhc[s, side] = jnp.zeros(xhc.shape[2:], F32)
                plx[s, side] = jnp.zeros((8, 128), F32)
            xmf[side, 0] = jnp.zeros(xmf.shape[2:], F32)
            xmf[side, 1] = jnp.ones(xmf.shape[2:], F32)
            xmc[side, 0] = jnp.zeros(xmc.shape[2:], F32)
            xmc[side, 1] = jnp.ones(xmc.shape[2:], F32)
    for dy in (-1, 1):
        @pl.when(jnp.logical_not(exists[(0, dy)]))
        def _(side=side_of[dy]):
            for s in range(STEPS):
                yhf[s, side] = jnp.zeros(yhf.shape[2:], F32)
                yhc[s, side] = jnp.zeros(yhc.shape[2:], F32)
                ply[s, side] = jnp.zeros((8, 128), F32)
            ymf[side, 0] = jnp.zeros(ymf.shape[2:], F32)
            ymf[side, 1] = jnp.ones(ymf.shape[2:], F32)
            ymc[side, 0] = jnp.zeros(ymc.shape[2:], F32)
            ymc[side, 1] = jnp.ones(ymc.shape[2:], F32)
    for d in corners:
        @pl.when(jnp.logical_not(exists[d]))
        def _(n=corner_id[d]):
            for s in range(STEPS):
                ccr[s, n] = jnp.zeros(ccr.shape[2:], F32)
                cpr[s, n] = jnp.zeros(cpr.shape[2:], F32)
                fcr[s, n] = jnp.zeros(fcr.shape[2:], F32)

    wait_load("fine_disp", "coarse_disp", "fine_rigidity", "coarse_rigidity", "fine_metric",
              "coarse_metric")
    for c in (0, 1):
        for side, jf, jc in ((LO, 0, 0), (HI, 15, 7)):
            ysmf[side, c] = Fine.plane(matf.at[c], jf)
            ysmc[side, c] = Coarse.plane(matc.at[c], jc)
    pack_y(Fine, 0)
    pack_y(Coarse, 0)
    for dx in (-1, 1):
        pack_coarse_corners(0, dx)
        pack_corners(0, dx)
    pack_plane(0)

    greeted = jnp.where(second, n1 // 2 + 2 * len(by_one), n1 // 2).astype(jnp.int32)
    for d in directions:
        greeted = greeted + jnp.where(exists[d], 1, 0).astype(jnp.int32)
    pl.semaphore_wait(barrier, greeted)

    send(0, "co")
    send(0, "cx", "cy", "mc")
    send(0, "fo", "fx", "fy", "mf")
    send(0, "cp", "cq")

    wait_load("fine_density", "fine_lame", "coarse_density", "coarse_lame", "offsets")
    lane8 = lanes((8, 128))
    spread = jnp.where(
        (lanes((16, 128)) % 16 == subs((16, 128))) & (lanes((16, 128)) < 48), 1.0, 0.0
    ).astype(F32)
    for t in (0, 1):
        pick = jnp.where(lanes((8, 16)) == 2 * subs((8, 16)) + t, 1.0, 0.0).astype(F32)
        for axis in (0, 1):
            table = offsets_ref[axis].astype(F32)
            turned = lax.dot_general(
                pick, table, (((1,), (1,)), ((), ())), preferred_element_type=F32
            )
            shift = jnp.dot(turned, spread, preferred_element_type=F32)
            if axis == 0:
                near = jnp.where(lane8 % 2 == 0, 0.75, 0.25).astype(F32)
            else:
                near = jnp.full((8, 128), 0.75 if t == 0 else 0.25, F32)
            for m, value in enumerate((-1.0, 0.0, 1.0, 2.0)):
                weights[t, 4 * axis + m] = jnp.where(shift == value, near, 0.0) + jnp.where(
                    shift == value - 1.0, 1.0 - near, 0.0
                )

    levels = (
        (Coarse, uc, matc, kc, dvc, dyc, xhc, yhc, ysc, xmc, ymc),
        (Fine, uf, matf, kf, dvf, dyf, xhf, yhf, ysf, xmf, ymf),
    )
    for level, u, mat, k, dv, dy_, xh, yh, ys, xm, ym in levels:
        for i in range(0, level.n, R):
            rig, met, den, lam = (level.load(mat.at[m], i, R) for m in range(4))
            scale = level.edge_scale(rig.shape)
            inverse = 1.0 / met
            light = DT / den
            a = inverse * light
            vertical = rig * inverse
            b = (lam + rig) * light
            isv = inverse * scale
            half_a = 0.5 * a
            for slot, value in (
                (WIDE, rig * met), (HALF_A, half_a), (ISV, isv), (GB, 0.5 * b), (GZ, b * isv),
                (DM, den * met), (CZU, half_a * (vertical + level.k_up(vertical))),
                (CZD, half_a * (vertical + level.k_down(vertical))),
            ):
                level.store(k.at[slot], i, R, value)

    def halo_row(level, ref):
        if level is Fine:
            return Fine.load(ref, 0, 1)
        return Coarse.load(ref, 0, 1)

    def side_coefficients(level, mat, k, xm, ym):
        for i in range(0, level.n, R):
            w = level.load(k.at[WIDE], i, R)
            ha = level.load(k.at[HALF_A], i, R)

            def outer(side):
                return halo_row(level, xm.at[side, 0]) * halo_row(level, xm.at[side, 1])

            cxp = ha * (w + neighbour_rows(level, k.at[WIDE], i, R, 1, lambda: outer(HI)))
            cxm = ha * (w + neighbour_rows(level, k.at[WIDE], i, R, -1, lambda: outer(LO)))
            up = level.row_of(ym.at[HI, 0], i, R) * level.row_of(ym.at[HI, 1], i, R)
            down = level.row_of(ym.at[LO, 0], i, R) * level.row_of(ym.at[LO, 1], i, R)
            cyu = ha * (w + level.j_up(w, up))
            cyd = ha * (w + level.j_down(w, down))
            total = cxp + cxm + cyu + cyd + level.load(k.at[CZU], i, R) + level.load(k.at[CZD], i, R)
            for slot, value in ((CXP, cxp), (CXM, cxm), (CYU, cyu), (CYD, cyd), (C0, total)):
                level.store(k.at[slot], i, R, value)

    def row_divergence(s, i, r, level, u, mat, k, dv, dy_, xh, yh, ys, xm, ym):
        now = u.at[s + 1]

        def halo(side):
            return lambda: halo_row(level, xh.at[s, side, 0])

        px = neighbour_rows(level, now.at[0], i, r, 1, halo(HI))
        mx = neighbour_rows(level, now.at[0], i, r, -1, halo(LO))
        y = level.load(now.at[1], i, r)
        z = level.load(now.at[2], i, r)
        py = level.j_up(y, level.row_of(yh.at[s, HI, 1], i, r))
        my = level.j_down(y, level.row_of(yh.at[s, LO, 1], i, r))
        isv = level.load(k.at[ISV], i, r)
        value = 0.5 * ((px - mx) + (py - my)) + isv * (level.k_up(z) - level.k_down(z))
        level.store(dv, i + 1, r, value)

    def x_side_divergence(s, dx, level, u, mat, k, dv, dy_, xh, yh, ys, xm, ym):
        cor = fcr if level is Fine else ccr
        now, n = u.at[s + 1], level.n
        side = side_of[dx]
        inside = level.load(now.at[0], 0 if dx < 0 else n - 1, 1)
        beyond = halo_row(level, xh.at[s, side, 3])
        y = halo_row(level, xh.at[s, side, 1])
        z = halo_row(level, xh.at[s, side, 2])
        py = level.j_up(y, level.corner_row(cor.at[s, corner_id[(dx, 1)]], 1))
        my = level.j_down(y, level.corner_row(cor.at[s, corner_id[(dx, -1)]], 1))
        isv = level.edge_scale(z.shape) / halo_row(level, xm.at[side, 1])
        along = (beyond - inside) if dx > 0 else (inside - beyond)
        value = 0.5 * (along + (py - my)) + isv * (level.k_up(z) - level.k_down(z))
        level.store(dv, 0 if dx < 0 else n + 1, 1, value * flag((dx, 0)))

    def y_side_divergence(s, known, level, u, mat, k, dv, dy_, xh, yh, ys, xm, ym):
        cor = fcr if level is Fine else ccr
        n = level.n
        for dy, side in side_of.items():
            x, z, beyond = yh[s, side, 0], yh[s, side, 2], yh[s, side, 3]
            inside = ys[s, side, 1]
            sub = plane_sub(level, x)
            px, mx = plane_roll(level, x, -1), plane_roll(level, x, 1)
            if 1 in known:
                px = jnp.where(sub == n - 1, level.corner_plane(cor.at[s, corner_id[(1, dy)]], 0), px)
            if -1 in known:
                mx = jnp.where(sub == 0, level.corner_plane(cor.at[s, corner_id[(-1, dy)]], 0), mx)
            isv = level.edge_scale(z.shape) / ym[side, 1]
            along = (beyond - inside) if dy > 0 else (inside - beyond)
            value = 0.5 * (along + (px - mx)) + isv * (level.plane_k_up(z) - level.plane_k_down(z))
            dy_[side] = value * flag((0, dy))

    def middle(s, level, *rest):
        n = level.n
        y_side_divergence(s, (), level, *rest)
        row_divergence(s, 1, 1, level, *rest)
        for i in range(2, n - 2, R):
            row_divergence(s, i, R, level, *rest)
        row_divergence(s, n - 2, 1, level, *rest)
        total = jnp.zeros((8, 128), F32)
        for i in range(R, first_outer(level), R):
            total = total + rates(s, i, level, *rest)
        return total

    def first_outer(level):
        return level.n - (4 if level is Fine else 2)

    def outer(s, dx, level, *rest):
        n = level.n
        x_side_divergence(s, dx, level, *rest)
        y_side_divergence(s, (-1,) if dx < 0 else (-1, 1), level, *rest)
        row_divergence(s, 0 if dx < 0 else n - 1, 1, level, *rest)
        if dx < 0:
            return rates(s, 0, level, *rest)
        total = rates(s, n - R, level, *rest)
        for i in range(first_outer(level), n - R, R):
            total = total + rates(s, i, level, *rest)
        return total

    def fine_ghosts(s, known):
        sub, lane = subs((8, 128)), lanes((8, 128)) % 16

        def shifted_rows(tile, low, high0, high1):
            return [
                jnp.where(sub == 0, low, roll(tile, 1, 0)),
                tile,
                jnp.where(sub == 7, high0, roll(tile, -1, 0)),
                jnp.where(sub == 7, high1, jnp.where(sub == 6, high0, roll(tile, -2, 0))),
            ]

        def row(ref, j):
            return spread_row(ref[pl.ds(j, 1), :])

        def corner_rows(dx):
            low, high = cpr.at[s, corner_id[(dx, -1)]], cpr.at[s, corner_id[(dx, 1)]]
            return spread_row(low[0]), spread_row(high[0]), spread_row(high[1])

        own = shifted_rows(pls[s], row(ply.at[s, LO], 7), row(ply.at[s, HI], 0), row(ply.at[s, HI], 1))
        if -1 in known:
            left = shifted_rows(plx[s, LO], *corner_rows(-1))
        if 1 in known:
            right = shifted_rows(plx[s, HI], *corner_rows(1))
        totals = [jnp.zeros((8, 128), F32) for _ in (0, 1)]
        for mx in range(4):
            inner = [jnp.zeros((8, 128), F32) for _ in (0, 1)]
            for my in range(4):
                tile = roll(own[my], 2 - 2 * mx, 1) if mx != 1 else own[my]
                if mx == 0 and -1 in known:
                    tile = jnp.where(lane < 2, roll(left[my], -14, 1), tile)
                if mx >= 2 and 1 in known:
                    edge = 18 - 2 * mx
                    tile = jnp.where(lane >= edge, roll(right[my], edge, 1), tile)
                for t in (0, 1):
                    inner[t] = inner[t] + weights[t, 4 + my] * tile
            for t in (0, 1):
                totals[t] = totals[t] + weights[t, mx] * inner[t]
        for t in (0, 1):
            ghost[t] = totals[t]

    def fine_last(c, i):
        rows = []
        for t in (0, 1):
            tile = ghost[t]
            rows.append(jnp.stack([roll(tile, 127 - (16 * c + i + m), 1) for m in range(R)]))
        return jnp.stack(rows)

    def coarse_first(s, c, i):
        rows = []
        for m in range(R):
            base = 32 * (i + m)
            parts = [uf[s + 1, c, pl.ds(base + t, 8, stride=2), :] for t in (0, 1, 16, 17)]
            rows.append(0.25 * ((parts[0] + parts[1]) + (parts[2] + parts[3])))
        return roll(jnp.stack(rows), 1, 2)

    def rates(s, i, level, u, mat, k, dv, dy_, xh, yh, ys, xm, ym):
        now, old = u.at[s + 1], u.at[s]
        coef = {
            m: level.load(k.at[m], i, R) for m in (GB, GZ, DM, CZU, CZD, CXP, CXM, CYU, CYD, C0)
        }
        d_mid = level.load(dv, i + 1, R)
        gradient = [
            coef[GB] * (level.load(dv, i + 2, R) - level.load(dv, i, R)),
            coef[GB]
            * (
                level.j_up(d_mid, level.row_of(dy_.at[HI], i, R))
                - level.j_down(d_mid, level.row_of(dy_.at[LO], i, R))
            ),
            coef[GZ] * (level.k_up(d_mid) - level.k_down(d_mid)),
        ]
        energy = None
        for c in range(3):
            v = level.load(now.at[c], i, R)

            def halo(side, c=c):
                return lambda: halo_row(level, xh.at[s, side, c])

            px = neighbour_rows(level, now.at[c], i, R, 1, halo(HI))
            mx = neighbour_rows(level, now.at[c], i, R, -1, halo(LO))
            py = level.j_up(v, level.row_of(yh.at[s, HI, c], i, R))
            my = level.j_down(v, level.row_of(yh.at[s, LO, c], i, R))
            if level is Fine:
                pz, mz = level.k_up(v, fine_last(c, i)), level.k_down(v)
            else:
                pz = level.k_up(v, jnp.zeros_like(v[1]))
                mz = level.k_down(v, coarse_first(s, c, i))
            rate = (
                (coef[CXP] * px + coef[CXM] * mx)
                + (coef[CYU] * py + coef[CYD] * my)
                + (coef[CZU] * pz + coef[CZD] * mz)
                - coef[C0] * v
                + gradient[c]
            )
            after = (2.0 * v - level.load(old.at[c], i, R)) + rate
            if s < STEPS - 1:
                level.store(u.at[s + 2, c], i, R, after)
            elif level is Fine:
                level.store(fine_out.at[c], i, R, after)
            else:
                for h in (0, 1):
                    coarse_out[c, pl.ds(8 * i, 8 * R), pl.ds(128 * h, 128)] = after[h].reshape(
                        8 * R, 128
                    )
            change = after - v
            part = change * change - after * rate
            energy = part if energy is None else energy + part
        return jnp.sum(coef[DM] * energy, axis=(0, 1))

    coarse_set, fine_set = levels
    for s in range(STEPS):
        last = s == STEPS - 1
        receive(s, "cy")
        if s == 0:
            receive(0, "mc")
            side_coefficients(Coarse, matc, kc, xmc, ymc)
            wait_load("coarse_prev")
        coarse_total = middle(s, *coarse_set)
        receive(s, "cq", "fy")
        if s == 0:
            receive(0, "mf")
            side_coefficients(Fine, matf, kf, xmf, ymf)
            wait_load("fine_prev")
        fine_ghosts(s, ())
        fine_total = middle(s, *fine_set)
        for dx in (-1, 1):
            receive(s, "co", "cx", side=dx)
            coarse_total = coarse_total + outer(s, dx, *coarse_set)
            if not last:
                pack_coarse_corners(s + 1, dx)
                send(s + 1, "co", dx=dx)
                send(s + 1, "cx", dx=dx)
        eacc[s, 1] = coarse_total
        if not last:
            pack_y(Coarse, s + 1)
            pack_plane(s + 1)
            send(s + 1, "cy", "cq", "cp")
        for dx in (-1, 1):
            receive(s, "cp", "fo", "fx", side=dx)
            fine_ghosts(s, (-1,) if dx < 0 else (-1, 1))
            fine_total = fine_total + outer(s, dx, *fine_set)
            if not last:
                pack_corners(s + 1, dx)
                send(s + 1, "fo", dx=dx)
                send(s + 1, "fx", dx=dx)
        eacc[s, 0] = fine_total
        if not last:
            pack_y(Fine, s + 1)
            send(s + 1, "fy")
        if s == 0:
            line_round(0)
        if s == 1:
            @pl.when(second)
            def _():
                line_wait(0)

            line_round(1)

    lane1 = lanes((1, 128))
    row = jnp.zeros((1, 128), F32)
    cells = (nx * ny * 16 * 16 * 128, nx * ny * 8 * 8 * 256)
    for s in range(STEPS):
        for m in (0, 1):
            value = jnp.sum(eacc[s, m], axis=0, keepdims=True)
            value = jnp.sum(value, axis=1, keepdims=True)
            row = jnp.where(lane1 == STEPS * m + s, value * (1.0 / cells[m]), row)
    erow[0] = row
    er1[me1] = row

    def rows(buffer, n, stage):
        part = buffer.at[pl.ds(0, n)]
        return pltpu.make_async_remote_copy(
            src_ref=part, dst_ref=part, send_sem=esend.at[stage], recv_sem=erecv.at[stage],
            device_id={"gx": line_x[0], "gy": gy}, device_id_type=MESH,
        )

    def pass_on(stage, slot, where):
        pltpu.make_async_remote_copy(
            src_ref=erow.at[stage], dst_ref=slot, send_sem=esend.at[stage],
            recv_sem=erecv.at[stage], device_id=where, device_id_type=MESH,
        ).start()

    for a in reversed(range(group_x)):
        for b in reversed(range(half)):
            if a or b:
                pass_on(0, er1.at[me1], {"gx": plane_x[a], "gy": plane_y[b] + 1})

    @pl.when(first_core)
    def _():
        pass_on(0, er1.at[me1], {"gx": gx, "gy": 2 * chip_y + 1})

    @pl.when(second)
    def _():
        rows(er1, n1 - 1, 0).wait_recv()
        plane = er1[0]
        for m in range(1, n1):
            plane = plane + er1[m]
        erow[1] = plane
        er2[gx_hi] = plane
        line_wait(1)
        for d in far_first:
            for core in (0, 1):
                pass_on(1, er2.at[gx_hi], {"gx": line_x[d], "gy": 2 * chip_y + core})
        pass_on(1, er2.at[gx_hi], {"gx": gx, "gy": 2 * chip_y})
        if n2 > 1:
            rows(er2, n2 - 1, 1).wait_recv()

    @pl.when(first_core)
    def _():
        rows(er2, n2, 1).wait_recv()

    row = er2[0]
    for m in range(1, n2):
        row = row + er2[m]
    for m in (0, 1):
        energy_out[pl.ds(m, 1), :] = roll(row, -STEPS * m, 1)[:, 0:STEPS]

    @pl.when(second)
    def _():
        rows(er1, n1 // 2 - 1, 0).wait_send()
        rows(er1, 2 * n2 - 1, 1).wait_send()

    @pl.when(first_core)
    def _():
        rows(er1, n1 // 2, 0).wait_send()

    for s in range(STEPS):
        run(s, ("co", "cp", "cq", "fo", "cx", "cy", "mc", "mf", "fx", "fy"), "wait_send")


def hand_out(*refs):
    copies = [pltpu.make_async_copy(refs[n], refs[3 + n], refs[6].at[n]) for n in range(3)]
    for c in copies:
        c.start()
    for c in copies:
        c.wait()


def per_device(nx, ny, group_x, *args):
    args = list(args)
    for m in range(4):
        shape = args[m].shape
        args[m] = args[m].reshape(shape[0], shape[1] * shape[2], shape[3])
    for m in range(4, 12):
        shape = args[m].shape
        args[m] = args[m].reshape(shape[0] * shape[1], shape[2])
    for m in range(13):
        args[m] = pltpu.with_memory_space_constraint(args[m], pltpu.HBM)
    vm, dma = pltpu.VMEM, pltpu.SemaphoreType.DMA
    n1, n2 = group_x * ny, nx // group_x
    scratch = [
        vm((STEPS + 1, 3, 256, 128), F32),
        vm((STEPS + 1, 3, 2, 64, 128), F32),
        vm((4, 256, 128), F32),
        vm((4, 2, 64, 128), F32),
        vm((NCOEF, 256, 128), F32),
        vm((NCOEF, 2, 64, 128), F32),
        vm((18 * 16, 128), F32),
        vm((2, 10 * 8, 128), F32),
        vm((2, 16, 128), F32),
        vm((2, 2, 8, 128), F32),
        vm((STEPS, 2, 4, 16, 128), F32),
        vm((STEPS, 2, 4, 2, 8, 128), F32),
        vm((STEPS, 2, 4, 16, 128), F32),
        vm((STEPS, 2, 4, 2, 8, 128), F32),
        vm((STEPS, 2, 4, 16, 128), F32),
        vm((STEPS, 2, 4, 2, 8, 128), F32),
        vm((2, 2, 16, 128), F32),
        vm((2, 2, 2, 8, 128), F32),
        vm((2, 2, 16, 128), F32),
        vm((2, 2, 2, 8, 128), F32),
        vm((2, 2, 16, 128), F32),
        vm((2, 2, 2, 8, 128), F32),
        vm((STEPS, 8, 128), F32),
        vm((STEPS, 2, 8, 128), F32),
        vm((STEPS, 2, 8, 128), F32),
        vm((STEPS, 8, 128), F32),
        vm((STEPS, 4, 4, 1, 128), F32),
        vm((STEPS, 4, 4, 1, 128), F32),
        vm((STEPS, 4, 2, 1, 128), F32),
        vm((STEPS, 4, 2, 1, 128), F32),
        vm((STEPS, 4, 2, 1, 128), F32),
        vm((STEPS, 4, 2, 1, 128), F32),
        vm((2, 16, 16), jnp.int32),
        vm((2, 8, 8, 128), F32),
        vm((2, 8, 128), F32),
        vm((STEPS, 2, 8, 128), F32),
        vm((2, 1, 128), F32),
        vm((max(n1, 2 * n2), 1, 128), F32),
        vm((max(n2, 1), 1, 128), F32),
        dma((13, 2)),
        dma((STEPS, 36)),
        dma((STEPS, 36)),
        dma((2,)),
        dma((2,)),
        pltpu.SemaphoreType.REGULAR((2, 2)),
    ]
    anywhere = pl.BlockSpec(memory_space=pltpu.HBM)
    in_vmem = pl.BlockSpec(memory_space=pltpu.VMEM)
    out_shape = (
        jax.ShapeDtypeStruct((3, 256, 128), F32),
        jax.ShapeDtypeStruct((3, 64, 256), F32),
        jax.ShapeDtypeStruct((2, STEPS), F32),
    )
    results = pl.pallas_call(
        functools.partial(kernel, nx, ny, group_x),
        out_shape=out_shape,
        in_specs=[anywhere] * 13,
        out_specs=(in_vmem, in_vmem, in_vmem),
        scratch_shapes=scratch,
        compiler_params=pltpu.CompilerParams(
            collective_id=0, has_side_effects=True, vmem_limit_bytes=32 << 20
        ),
        name="leapfrog",
    )(*args)
    fine, coarse, energy = pl.pallas_call(
        hand_out,
        out_shape=out_shape,
        in_specs=[in_vmem] * 3,
        out_specs=[anywhere] * 3,
        scratch_shapes=[dma((3,))],
        compiler_params=pltpu.CompilerParams(vmem_limit_bytes=1 << 20),
        name="hand_out",
    )(*results)
    energy = energy.T
    return fine.reshape(3, 16, 16, 128), coarse.reshape(3, 8, 8, 256), energy


def solution(mesh):
    nx, ny = mesh.shape["gx"], mesh.shape["gy"]
    group_x = next(m for m in (4, 2, 1) if nx % m == 0)
    field, cells = P(None, "gx", "gy", None), P("gx", "gy", None)
    return jax.shard_map(
        functools.partial(per_device, nx, ny, group_x),
        mesh=mesh,
        in_specs=(field,) * 4 + (cells,) * 8 + (P(None, "gx", "gy"),),
        out_specs=(field, field, P()),
        check_vma=False,
    )
```

```python
import functools

import jax
import jax.numpy as jnp
from jax import lax
from jax.experimental import pallas as pl
from jax.experimental.pallas import tpu as pltpu
from jax.sharding import PartitionSpec as P

STEPS = 3
DT = 0.15
MESH = pl.DeviceIdType.MESH
F32 = jnp.float32

R = 2
LO, HI = 0, 1
(WIDE, HALF_A, ISV, GB, GZ, DM, CZU, CZD, CXP, CXM, CYU, CYD, C0) = range(13)
NCOEF = 13


def lanes(shape):
    return lax.broadcasted_iota(jnp.int32, shape, len(shape) - 1)


def subs(shape):
    return lax.broadcasted_iota(jnp.int32, shape, len(shape) - 2)


def spread_row(row):
    return jnp.broadcast_to(row, (8, 128))


def roll(x, shift, axis):
    return pltpu.roll(x, shift % x.shape[axis], axis)


class Fine:
    n = 16
    key = "f"

    @staticmethod
    def load(ref, i, r):
        parts = [ref[pl.ds(16 * i + t, 8 * r, stride=2), :].reshape(1, r, 8, 128) for t in (0, 1)]
        return jnp.concatenate(parts, axis=0)

    @staticmethod
    def store(ref, i, r, value):
        for t in (0, 1):
            ref[pl.ds(16 * i + t, 8 * r, stride=2), :] = value[t].reshape(8 * r, 128)

    @staticmethod
    def k_up(x, last=None):
        moved = roll(x, -1, 3)
        edge = x if last is None else last
        return jnp.where(lanes(x.shape) == 127, edge, moved)

    @staticmethod
    def k_down(x, first=None):
        moved = roll(x, 1, 3)
        edge = x if first is None else first
        return jnp.where(lanes(x.shape) == 0, edge, moved)

    @staticmethod
    def edge_scale(shape):
        k = lanes(shape)
        return jnp.where((k == 0) | (k == 127), 1.0, 0.5).astype(F32)

    @staticmethod
    def row_of(ref, i, r):
        return jnp.concatenate(
            [spread_row(ref[pl.ds(i + m, 1), :]).reshape(1, 8, 128) for m in range(r)], axis=0
        )

    @staticmethod
    def j_up(x, halo):
        s = subs(x.shape[1:])
        moved = jnp.where(s == 7, halo, roll(x[0], -1, 1))
        return jnp.stack([x[1], moved])

    @staticmethod
    def j_down(x, halo):
        s = subs(x.shape[1:])
        moved = jnp.where(s == 0, halo, roll(x[1], 1, 1))
        return jnp.stack([moved, x[0]])

    @staticmethod
    def plane(ref, j):
        return jnp.concatenate([ref[pl.ds(j + 128 * h, 8, stride=16), :] for h in (0, 1)], axis=0)

    @staticmethod
    def plane_k_up(x):
        return jnp.where(lanes(x.shape) == 127, x, roll(x, -1, 1))

    @staticmethod
    def plane_k_down(x):
        return jnp.where(lanes(x.shape) == 0, x, roll(x, 1, 1))

    @staticmethod
    def corner_plane(tile_ref, comp):
        row = spread_row(tile_ref[comp])
        return jnp.concatenate([row, row], axis=0)

    @staticmethod
    def corner_row(tile_ref, comp):
        return spread_row(tile_ref[comp]).reshape(1, 8, 128)


class Coarse:
    n = 8
    key = "c"

    @staticmethod
    def load(ref, i, r):
        return ref[:, pl.ds(8 * i, 8 * r), :].reshape(2, r, 8, 128)

    @staticmethod
    def store(ref, i, r, value):
        ref[:, pl.ds(8 * i, 8 * r), :] = value.reshape(2, 8 * r, 128)

    @staticmethod
    def k_up(x, last=None):
        moved = roll(x, -1, 3)
        edge = x[1] if last is None else last
        return jnp.where(lanes(x.shape) == 127, jnp.stack([moved[1], edge]), moved)

    @staticmethod
    def k_down(x, first=None):
        moved = roll(x, 1, 3)
        edge = x[0] if first is None else first
        return jnp.where(lanes(x.shape) == 0, jnp.stack([edge, moved[0]]), moved)

    @staticmethod
    def edge_scale(shape):
        k = lanes(shape)
        half = lax.broadcasted_iota(jnp.int32, shape, 0)
        ends = ((k == 0) & (half == 0)) | ((k == 127) & (half == 1))
        return jnp.where(ends, 1.0, 0.5).astype(F32)

    @staticmethod
    def row_of(ref, i, r):
        halves = []
        for h in (0, 1):
            rows = [spread_row(ref[h, pl.ds(i + m, 1), :]).reshape(1, 8, 128) for m in range(r)]
            halves.append(jnp.concatenate(rows, axis=0))
        return jnp.stack(halves)

    @staticmethod
    def j_up(x, halo):
        return jnp.where(subs(x.shape) == 7, halo, roll(x, -1, 2))

    @staticmethod
    def j_down(x, halo):
        return jnp.where(subs(x.shape) == 0, halo, roll(x, 1, 2))

    @staticmethod
    def plane(ref, j):
        return jnp.stack([ref[h, pl.ds(j, 8, stride=8), :] for h in (0, 1)])

    @staticmethod
    def plane_k_up(x):
        return Coarse.k_up(x[:, None])[:, 0]

    @staticmethod
    def plane_k_down(x):
        return Coarse.k_down(x[:, None])[:, 0]

    @staticmethod
    def corner_plane(tile_ref, comp):
        return jnp.stack([spread_row(tile_ref[2 * comp + h]) for h in (0, 1)])

    @staticmethod
    def corner_row(tile_ref, comp):
        rows = [spread_row(tile_ref[2 * comp + h]) for h in (0, 1)]
        return jnp.stack(rows)[:, None]


def plane_roll(level, x, shift):
    return roll(x, shift, 0) if level is Fine else roll(x, shift, 1)


def plane_sub(level, x):
    return subs(x.shape)


def neighbour_rows(level, ref, i, r, step, halo):
    if step > 0:
        if i + r < level.n:
            return level.load(ref, i + 1, r)
        return halo() if r == 1 else jnp.concatenate([level.load(ref, i + 1, r - 1), halo()], axis=1)
    if i > 0:
        return level.load(ref, i - 1, r)
    return halo() if r == 1 else jnp.concatenate([halo(), level.load(ref, 0, r - 1)], axis=1)


def kernel(nx, ny, group_x, *refs):
    names_in = ["fine_disp", "fine_prev", "coarse_disp", "coarse_prev"]
    for name in ("fine", "coarse"):
        names_in += [name + part for part in ("_density", "_lame", "_rigidity", "_metric")]
    hbm = dict(zip(names_in, refs[:12]))
    offsets_hbm = refs[12]
    fine_out, coarse_out, energy_out = refs[13:16]
    (
        uf, uc, matf, matc, kf, kc, dvf, dvc, dyf, dyc,
        xhf, xhc, yhf, yhc, ysf, ysc, xmf, xmc, ymf, ymc, ysmf, ysmc,
        pls, plx, ply, pex, ccs, ccr, cps, cpr, fcs, fcr, offsets_ref, weights, ghost, eacc, erow, er1, er2,
        load_sem, send_sem, recv_sem, esend, erecv, line_sem, plane_sem,
    ) = refs[16:]

    gx, gy = lax.axis_index("gx"), lax.axis_index("gy")
    exists = {
        (dx, dy): functools.reduce(
            jnp.logical_and,
            ([gx > 0] if dx < 0 else [gx < nx - 1] if dx > 0 else [])
            + ([gy > 0] if dy < 0 else [gy < ny - 1] if dy > 0 else []),
        )
        for dx, dy in ((-1, 0), (1, 0), (-1, -1), (-1, 1), (1, -1), (1, 1), (0, -1), (0, 1))
    }
    directions = list(exists)
    corners = [d for d in directions if d[0] and d[1]]
    corner_id = {d: n for n, d in enumerate(corners)}

    def flag(direction):
        return jnp.where(exists[direction], 1.0, 0.0).astype(F32)

    def device(direction):
        return {"gx": gx + direction[0], "gy": gy + direction[1]}

    groups, half = nx // group_x, ny // 2
    gx_hi, gx_lo = gx // group_x, gx % group_x
    chip_y, second = gy // 2, gy % 2 == 1
    first_core = jnp.logical_not(second)
    n1, n2 = group_x * ny, groups
    me1 = gx_lo * ny + gy
    plane_x = [gx_hi * group_x + lax.rem(gx_lo + a, group_x) for a in range(group_x)]
    plane_y = [2 * lax.rem(chip_y + b, half) for b in range(half)]
    line_x = [lax.rem(gx_hi + d, n2) * group_x + gx_lo for d in range(n2)]

    loads = {}

    def start_load(name, dst, sem):
        fine = name.startswith("fine")
        src = hbm[name]
        if fine:
            copies = [pltpu.make_async_copy(src, dst, load_sem.at[sem, 0])]
        else:
            lead = (slice(None),) * (len(src.shape) - 2)
            copies = [
                pltpu.make_async_copy(
                    src.at[lead + (slice(None), pl.ds(128 * h, 128))],
                    dst.at[(slice(None), h) if lead else (h,)],
                    load_sem.at[sem, h],
                )
                for h in (0, 1)
            ]
        for c in copies:
            c.start()
        loads[name] = copies

    plan = [
        ("fine_disp", uf.at[1]), ("coarse_disp", uc.at[1]),
        ("fine_rigidity", matf.at[0]), ("coarse_rigidity", matc.at[0]),
        ("fine_metric", matf.at[1]), ("coarse_metric", matc.at[1]),
        ("fine_density", matf.at[2]), ("fine_lame", matf.at[3]),
        ("coarse_density", matc.at[2]), ("coarse_lame", matc.at[3]),
        ("fine_prev", uf.at[0]), ("coarse_prev", uc.at[0]),
    ]
    for sem, (name, dst) in enumerate(plan):
        start_load(name, dst, sem)

    loads["offsets"] = [pltpu.make_async_copy(offsets_hbm, offsets_ref, load_sem.at[12, 0])]
    loads["offsets"][0].start()

    def wait_load(*names):
        for name in names:
            for c in loads[name]:
                c.wait()

    barrier = pltpu.get_barrier_semaphore()

    def greet(where):
        pl.semaphore_signal(barrier, inc=1, device_id=where, device_id_type=MESH)

    far_first = sorted(range(1, n2), key=lambda d: -min(d, n2 - d))
    by_one = sorted({1, n2 - 1}) if n2 > 1 else []
    by_two = sorted({2, n2 - 2}) if n2 > 3 else []
    for d in by_one:
        greet({"gx": line_x[d], "gy": 2 * chip_y + 1})
    for d in directions:
        @pl.when(exists[d])
        def _(d=d):
            greet(device(d))

    side_of = {-1: LO, 1: HI}

    def messages(s):
        out = []
        u_f, u_c = uf.at[s + 1], uc.at[s + 1]
        for dx in (-1, 1):
            own, far = side_of[dx], side_of[-dx]
            first, second = (0, 1) if dx < 0 else (15, 14)
            out.append(("fx", (dx, 0), u_f.at[:, pl.ds(16 * first, 16)], xhf.at[s, far, pl.ds(0, 3)]))
            out.append(("fx", (dx, 0), u_f.at[0, pl.ds(16 * second, 16)], xhf.at[s, far, 3]))
            first, second = (0, 1) if dx < 0 else (7, 6)
            out.append(("cx", (dx, 0), u_c.at[:, :, pl.ds(8 * first, 8)], xhc.at[s, far, pl.ds(0, 3)]))
            out.append(("cx", (dx, 0), u_c.at[0, :, pl.ds(8 * second, 8)], xhc.at[s, far, 3]))
            out.append(("cp", (dx, 0), pex.at[s], plx.at[s, far]))
            if s == 0:
                first = 0 if dx < 0 else 15
                out.append(("mfx", (dx, 0), matf.at[pl.ds(0, 2), pl.ds(16 * first, 16)], xmf.at[far]))
                first = 0 if dx < 0 else 7
                out.append(("mcx", (dx, 0), matc.at[pl.ds(0, 2), :, pl.ds(8 * first, 8)], xmc.at[far]))
        for dy in (-1, 1):
            own, far = side_of[dy], side_of[-dy]
            out.append(("fy", (0, dy), ysf.at[s, own], yhf.at[s, far]))
            out.append(("cy", (0, dy), ysc.at[s, own], yhc.at[s, far]))
            out.append(("cq", (0, dy), pls.at[s], ply.at[s, far]))
            if s == 0:
                out.append(("mfy", (0, dy), ysmf.at[own], ymf.at[far]))
                out.append(("mcy", (0, dy), ysmc.at[own], ymc.at[far]))
        for d in corners:
            back = corner_id[(-d[0], -d[1])]
            out.append(("co", d, ccs.at[s, corner_id[d]], ccr.at[s, back]))
            out.append(("cp", d, cps.at[s, corner_id[d]], cpr.at[s, back]))
            out.append(("fo", d, fcs.at[s, corner_id[d]], fcr.at[s, back]))
        return out

    copies = []
    for s in range(STEPS):
        entries = []
        for n, (group, d, src, dst) in enumerate(messages(s)):
            def copy(src=src, dst=dst, s=s, n=n, d=d):
                return pltpu.make_async_remote_copy(
                    src_ref=src, dst_ref=dst,
                    send_sem=send_sem.at[s, n], recv_sem=recv_sem.at[s, n],
                    device_id=device(d), device_id_type=MESH,
                )

            entries.append((group, d, copy))
        copies.append(entries)

    def run(s, groups_wanted, what, backwards=False, dx=None):
        for d in directions:
            mine = [c for g, e, c in copies[s] if g in groups_wanted and e == d]
            if mine and dx in (None, d[0]):
                @pl.when(exists[(-d[0], -d[1]) if backwards else d])
                def _(mine=mine):
                    for c in mine:
                        getattr(c(), what)()

    def send(s, *wanted, dx=None):
        run(s, wanted, "start", dx=dx)

    def receive(s, *wanted, side=None):
        run(s, wanted, "wait_recv", backwards=True, dx=None if side is None else -side)

    def round_signals(stage):
        away = 2 << stage
        for side, ok, to in ((LO, gy + away < ny, gy + away), (HI, gy >= away, gy - away)):
            if ny > 5:
                @pl.when(ok)
                def _(side=side, to=to):
                    pl.semaphore_signal(
                        plane_sem.at[stage, side], inc=1,
                        device_id={"gx": gx, "gy": to}, device_id_type=MESH,
                    )
        if n2 > 3:
            @pl.when(second)
            def _():
                for m, d in enumerate((by_one, by_two)[stage]):
                    pl.semaphore_signal(
                        line_sem.at[stage, m], inc=1,
                        device_id={"gx": line_x[d], "gy": gy}, device_id_type=MESH,
                    )

    def round_wait(stage):
        away = 2 << stage
        for side, ok in ((LO, gy >= away), (HI, gy + away < ny)):
            if ny > 5:
                @pl.when(ok)
                def _(side=side):
                    pl.semaphore_wait(plane_sem.at[stage, side], 1)
        if n2 > 3:
            @pl.when(second)
            def _():
                for m in range(len((by_one, by_two)[stage])):
                    pl.semaphore_wait(line_sem.at[stage, m], 1)

    def pack_y(level, s):
        u, out = (uf, ysf) if level is Fine else (uc, ysc)
        last = 15 if level is Fine else 7
        for side, (j0, j1) in ((LO, (0, 1)), (HI, (last, last - 1))):
            for c in range(3):
                out[s, side, c] = level.plane(u.at[s + 1, c], j0)
            out[s, side, 3] = level.plane(u.at[s + 1, 1], j1)

    def plane_tile(s, tile, rows):
        lane = lanes((8, 128))
        for c in range(3):
            for i in rows:
                column = uc[s + 1, c, 0, pl.ds(8 * i, 8), 0:1]
                at = 16 * c + 2 * i
                tile = jnp.where((lane == at) | (lane == at + 1), column, tile)
        return tile

    def pack_coarse_corners(s, side):
        for (dx, dy), n in corner_id.items():
            if dx != side:
                continue
            ci, cj = (0 if dx < 0 else 7), (0 if dy < 0 else 7)
            for c in (0, 1):
                for h in (0, 1):
                    ccs[s, n, 2 * c + h] = uc[s + 1, c, h, pl.ds(8 * ci + cj, 1), :]

    def pack_plane(s):
        edge = plane_tile(s, jnp.zeros((8, 128), F32), (0, 1, 7))
        pex[s] = edge
        pls[s] = plane_tile(s, edge, range(2, 7))
        for (dx, dy), n in corner_id.items():
            for m, j in enumerate((0, 1) if dy < 0 else (7, 7)):
                cps[s, n, m] = edge[j : j + 1]

    def pack_corners(s, side):
        for (dx, dy), n in corner_id.items():
            if dx != side:
                continue
            fi, fj = (0 if dx < 0 else 15), (0 if dy < 0 else 15)
            for c in (0, 1):
                fcs[s, n, c] = uf[s + 1, c, pl.ds(16 * fi + fj, 1), :]

    for dx in (-1, 1):
        @pl.when(jnp.logical_not(exists[(dx, 0)]))
        def _(side=side_of[dx]):
            for s in range(STEPS):
                xhf[s, side] = jnp.zeros(xhf.shape[2:], F32)
                xhc[s, side] = jnp.zeros(xhc.shape[2:], F32)
                plx[s, side] = jnp.zeros((8, 128), F32)
            xmf[side, 0] = jnp.zeros(xmf.shape[2:], F32)
            xmf[side, 1] = jnp.ones(xmf.shape[2:], F32)
            xmc[side, 0] = jnp.zeros(xmc.shape[2:], F32)
            xmc[side, 1] = jnp.ones(xmc.shape[2:], F32)
    for dy in (-1, 1):
        @pl.when(jnp.logical_not(exists[(0, dy)]))
        def _(side=side_of[dy]):
            for s in range(STEPS):
                yhf[s, side] = jnp.zeros(yhf.shape[2:], F32)
                yhc[s, side] = jnp.zeros(yhc.shape[2:], F32)
                ply[s, side] = jnp.zeros((8, 128), F32)
            ymf[side, 0] = jnp.zeros(ymf.shape[2:], F32)
            ymf[side, 1] = jnp.ones(ymf.shape[2:], F32)
            ymc[side, 0] = jnp.zeros(ymc.shape[2:], F32)
            ymc[side, 1] = jnp.ones(ymc.shape[2:], F32)
    for d in corners:
        @pl.when(jnp.logical_not(exists[d]))
        def _(n=corner_id[d]):
            for s in range(STEPS):
                ccr[s, n] = jnp.zeros(ccr.shape[2:], F32)
                cpr[s, n] = jnp.zeros(cpr.shape[2:], F32)
                fcr[s, n] = jnp.zeros(fcr.shape[2:], F32)

    wait_load("fine_disp", "coarse_disp", "fine_rigidity", "coarse_rigidity", "fine_metric",
              "coarse_metric")
    for c in (0, 1):
        for side, jf, jc in ((LO, 0, 0), (HI, 15, 7)):
            ysmf[side, c] = Fine.plane(matf.at[c], jf)
            ysmc[side, c] = Coarse.plane(matc.at[c], jc)
    pack_y(Fine, 0)
    pack_y(Coarse, 0)
    for dx in (-1, 1):
        pack_coarse_corners(0, dx)
        pack_corners(0, dx)
    pack_plane(0)

    greeted = jnp.where(second, 2 * len(by_one), 0).astype(jnp.int32)
    for d in directions:
        greeted = greeted + jnp.where(exists[d], 1, 0).astype(jnp.int32)
    pl.semaphore_wait(barrier, greeted)

    send(0, "co")
    send(0, "cx", "mcx")
    send(0, "cy", "mcy", "cq", "fy", "mfy")
    send(0, "fo", "fx", "mfx")
    send(0, "cp")

    wait_load("fine_density", "fine_lame", "coarse_density", "coarse_lame", "offsets")
    lane8 = lanes((8, 128))
    spread = jnp.where(
        (lanes((16, 128)) % 16 == subs((16, 128))) & (lanes((16, 128)) < 48), 1.0, 0.0
    ).astype(F32)
    for t in (0, 1):
        pick = jnp.where(lanes((8, 16)) == 2 * subs((8, 16)) + t, 1.0, 0.0).astype(F32)
        for axis in (0, 1):
            table = offsets_ref[axis].astype(F32)
            turned = lax.dot_general(
                pick, table, (((1,), (1,)), ((), ())), preferred_element_type=F32
            )
            shift = jnp.dot(turned, spread, preferred_element_type=F32)
            if axis == 0:
                near = jnp.where(lane8 % 2 == 0, 0.75, 0.25).astype(F32)
            else:
                near = jnp.full((8, 128), 0.75 if t == 0 else 0.25, F32)
            for m, value in enumerate((-1.0, 0.0, 1.0, 2.0)):
                weights[t, 4 * axis + m] = jnp.where(shift == value, near, 0.0) + jnp.where(
                    shift == value - 1.0, 1.0 - near, 0.0
                )

    levels = (
        (Coarse, uc, matc, kc, dvc, dyc, xhc, yhc, ysc, xmc, ymc),
        (Fine, uf, matf, kf, dvf, dyf, xhf, yhf, ysf, xmf, ymf),
    )
    for level, u, mat, k, dv, dy_, xh, yh, ys, xm, ym in levels:
        for i in range(0, level.n, R):
            rig, met, den, lam = (level.load(mat.at[m], i, R) for m in range(4))
            scale = level.edge_scale(rig.shape)
            inverse = 1.0 / met
            light = DT / den
            a = inverse * light
            vertical = rig * inverse
            b = (lam + rig) * light
            isv = inverse * scale
            half_a = 0.5 * a
            for slot, value in (
                (WIDE, rig * met), (HALF_A, half_a), (ISV, isv), (GB, 0.5 * b), (GZ, b * isv),
                (DM, den * met), (CZU, half_a * (vertical + level.k_up(vertical))),
                (CZD, half_a * (vertical + level.k_down(vertical))),
            ):
                level.store(k.at[slot], i, R, value)

    def halo_row(level, ref):
        if level is Fine:
            return Fine.load(ref, 0, 1)
        return Coarse.load(ref, 0, 1)

    def side_coefficients(level, i, r, u, mat, k, dv, dy_, xh, yh, ys, xm, ym):
        w = level.load(k.at[WIDE], i, r)
        ha = level.load(k.at[HALF_A], i, r)

        def outer(side):
            return halo_row(level, xm.at[side, 0]) * halo_row(level, xm.at[side, 1])

        cxp = ha * (w + neighbour_rows(level, k.at[WIDE], i, r, 1, lambda: outer(HI)))
        cxm = ha * (w + neighbour_rows(level, k.at[WIDE], i, r, -1, lambda: outer(LO)))
        up = level.row_of(ym.at[HI, 0], i, r) * level.row_of(ym.at[HI, 1], i, r)
        down = level.row_of(ym.at[LO, 0], i, r) * level.row_of(ym.at[LO, 1], i, r)
        cyu = ha * (w + level.j_up(w, up))
        cyd = ha * (w + level.j_down(w, down))
        total = cxp + cxm + cyu + cyd + level.load(k.at[CZU], i, r) + level.load(k.at[CZD], i, r)
        for slot, value in ((CXP, cxp), (CXM, cxm), (CYU, cyu), (CYD, cyd), (C0, total)):
            level.store(k.at[slot], i, r, value)

    def inner_coefficients(level, *rest):
        for i, r in [(1, 1)] + [(i, R) for i in range(2, level.n - 2, R)] + [(level.n - 2, 1)]:
            side_coefficients(level, i, r, *rest)

    def row_divergence(s, i, r, level, u, mat, k, dv, dy_, xh, yh, ys, xm, ym):
        now = u.at[s + 1]

        def halo(side):
            return lambda: halo_row(level, xh.at[s, side, 0])

        px = neighbour_rows(level, now.at[0], i, r, 1, halo(HI))
        mx = neighbour_rows(level, now.at[0], i, r, -1, halo(LO))
        y = level.load(now.at[1], i, r)
        z = level.load(now.at[2], i, r)
        py = level.j_up(y, level.row_of(yh.at[s, HI, 1], i, r))
        my = level.j_down(y, level.row_of(yh.at[s, LO, 1], i, r))
        isv = level.load(k.at[ISV], i, r)
        value = 0.5 * ((px - mx) + (py - my)) + isv * (level.k_up(z) - level.k_down(z))
        level.store(dv, i + 1, r, value)

    def x_side_divergence(s, dx, level, u, mat, k, dv, dy_, xh, yh, ys, xm, ym):
        cor = fcr if level is Fine else ccr
        now, n = u.at[s + 1], level.n
        side = side_of[dx]
        inside = level.load(now.at[0], 0 if dx < 0 else n - 1, 1)
        beyond = halo_row(level, xh.at[s, side, 3])
        y = halo_row(level, xh.at[s, side, 1])
        z = halo_row(level, xh.at[s, side, 2])
        py = level.j_up(y, level.corner_row(cor.at[s, corner_id[(dx, 1)]], 1))
        my = level.j_down(y, level.corner_row(cor.at[s, corner_id[(dx, -1)]], 1))
        isv = level.edge_scale(z.shape) / halo_row(level, xm.at[side, 1])
        along = (beyond - inside) if dx > 0 else (inside - beyond)
        value = 0.5 * (along + (py - my)) + isv * (level.k_up(z) - level.k_down(z))
        level.store(dv, 0 if dx < 0 else n + 1, 1, value * flag((dx, 0)))

    def y_side_divergence(s, known, level, u, mat, k, dv, dy_, xh, yh, ys, xm, ym):
        cor = fcr if level is Fine else ccr
        n = level.n
        for dy, side in side_of.items():
            x, z, beyond = yh[s, side, 0], yh[s, side, 2], yh[s, side, 3]
            inside = ys[s, side, 1]
            sub = plane_sub(level, x)
            px, mx = plane_roll(level, x, -1), plane_roll(level, x, 1)
            if 1 in known:
                px = jnp.where(sub == n - 1, level.corner_plane(cor.at[s, corner_id[(1, dy)]], 0), px)
            if -1 in known:
                mx = jnp.where(sub == 0, level.corner_plane(cor.at[s, corner_id[(-1, dy)]], 0), mx)
            isv = level.edge_scale(z.shape) / ym[side, 1]
            along = (beyond - inside) if dy > 0 else (inside - beyond)
            value = 0.5 * (along + (px - mx)) + isv * (level.plane_k_up(z) - level.plane_k_down(z))
            dy_[side] = value * flag((0, dy))

    def middle(s, level, *rest):
        n = level.n
        y_side_divergence(s, (), level, *rest)
        row_divergence(s, 1, 1, level, *rest)
        for i in range(2, n - 2, R):
            row_divergence(s, i, R, level, *rest)
        row_divergence(s, n - 2, 1, level, *rest)
        total = jnp.zeros((8, 128), F32)
        for i in range(R, first_outer(level), R):
            total = total + rates(s, i, level, *rest)
        return total

    def first_outer(level):
        return level.n - (4 if level is Fine else 2)

    def outer(s, dx, level, *rest):
        n = level.n
        x_side_divergence(s, dx, level, *rest)
        y_side_divergence(s, (-1,) if dx < 0 else (-1, 1), level, *rest)
        row_divergence(s, 0 if dx < 0 else n - 1, 1, level, *rest)
        if dx < 0:
            return rates(s, 0, level, *rest)
        total = rates(s, n - R, level, *rest)
        for i in range(first_outer(level), n - R, R):
            total = total + rates(s, i, level, *rest)
        return total

    def fine_ghosts(s, known):
        sub, lane = subs((8, 128)), lanes((8, 128)) % 16

        def shifted_rows(tile, low, high0, high1):
            return [
                jnp.where(sub == 0, low, roll(tile, 1, 0)),
                tile,
                jnp.where(sub == 7, high0, roll(tile, -1, 0)),
                jnp.where(sub == 7, high1, jnp.where(sub == 6, high0, roll(tile, -2, 0))),
            ]

        def row(ref, j):
            return spread_row(ref[pl.ds(j, 1), :])

        def corner_rows(dx):
            low, high = cpr.at[s, corner_id[(dx, -1)]], cpr.at[s, corner_id[(dx, 1)]]
            return spread_row(low[0]), spread_row(high[0]), spread_row(high[1])

        own = shifted_rows(pls[s], row(ply.at[s, LO], 7), row(ply.at[s, HI], 0), row(ply.at[s, HI], 1))
        if -1 in known:
            left = shifted_rows(plx[s, LO], *corner_rows(-1))
        if 1 in known:
            right = shifted_rows(plx[s, HI], *corner_rows(1))
        totals = [jnp.zeros((8, 128), F32) for _ in (0, 1)]
        for mx in range(4):
            inner = [jnp.zeros((8, 128), F32) for _ in (0, 1)]
            for my in range(4):
                tile = roll(own[my], 2 - 2 * mx, 1) if mx != 1 else own[my]
                if mx == 0 and -1 in known:
                    tile = jnp.where(lane < 2, roll(left[my], -14, 1), tile)
                if mx >= 2 and 1 in known:
                    edge = 18 - 2 * mx
                    tile = jnp.where(lane >= edge, roll(right[my], edge, 1), tile)
                for t in (0, 1):
                    inner[t] = inner[t] + weights[t, 4 + my] * tile
            for t in (0, 1):
                totals[t] = totals[t] + weights[t, mx] * inner[t]
        for t in (0, 1):
            ghost[t] = totals[t]

    def fine_last(c, i):
        rows = []
        for t in (0, 1):
            tile = ghost[t]
            rows.append(jnp.stack([roll(tile, 127 - (16 * c + i + m), 1) for m in range(R)]))
        return jnp.stack(rows)

    def coarse_first(s, c, i):
        rows = []
        for m in range(R):
            base = 32 * (i + m)
            parts = [uf[s + 1, c, pl.ds(base + t, 8, stride=2), :] for t in (0, 1, 16, 17)]
            rows.append(0.25 * ((parts[0] + parts[1]) + (parts[2] + parts[3])))
        return roll(jnp.stack(rows), 1, 2)

    def rates(s, i, level, u, mat, k, dv, dy_, xh, yh, ys, xm, ym):
        now, old = u.at[s + 1], u.at[s]
        coef = {
            m: level.load(k.at[m], i, R) for m in (GB, GZ, DM, CZU, CZD, CXP, CXM, CYU, CYD, C0)
        }
        d_mid = level.load(dv, i + 1, R)
        gradient = [
            coef[GB] * (level.load(dv, i + 2, R) - level.load(dv, i, R)),
            coef[GB]
            * (
                level.j_up(d_mid, level.row_of(dy_.at[HI], i, R))
                - level.j_down(d_mid, level.row_of(dy_.at[LO], i, R))
            ),
            coef[GZ] * (level.k_up(d_mid) - level.k_down(d_mid)),
        ]
        energy = None
        for c in range(3):
            v = level.load(now.at[c], i, R)

            def halo(side, c=c):
                return lambda: halo_row(level, xh.at[s, side, c])

            px = neighbour_rows(level, now.at[c], i, R, 1, halo(HI))
            mx = neighbour_rows(level, now.at[c], i, R, -1, halo(LO))
            py = level.j_up(v, level.row_of(yh.at[s, HI, c], i, R))
            my = level.j_down(v, level.row_of(yh.at[s, LO, c], i, R))
            if level is Fine:
                pz, mz = level.k_up(v, fine_last(c, i)), level.k_down(v)
            else:
                pz = level.k_up(v, jnp.zeros_like(v[1]))
                mz = level.k_down(v, coarse_first(s, c, i))
            rate = (
                (coef[CXP] * px + coef[CXM] * mx)
                + (coef[CYU] * py + coef[CYD] * my)
                + (coef[CZU] * pz + coef[CZD] * mz)
                - coef[C0] * v
                + gradient[c]
            )
            after = (2.0 * v - level.load(old.at[c], i, R)) + rate
            if s < STEPS - 1:
                level.store(u.at[s + 2, c], i, R, after)
            elif level is Fine:
                level.store(fine_out.at[c], i, R, after)
            else:
                for h in (0, 1):
                    coarse_out[c, pl.ds(8 * i, 8 * R), pl.ds(128 * h, 128)] = after[h].reshape(
                        8 * R, 128
                    )
            change = after - v
            part = change * change - after * rate
            energy = part if energy is None else energy + part
        return jnp.sum(coef[DM] * energy, axis=(0, 1))

    coarse_set, fine_set = levels
    for s in range(STEPS):
        last = s == STEPS - 1
        receive(s, "cy")
        if s == 0:
            receive(0, "mcy")
            inner_coefficients(*coarse_set)
            wait_load("coarse_prev")
        coarse_total = middle(s, *coarse_set)
        receive(s, "cq", "fy")
        if s == 0:
            receive(0, "mfy")
            inner_coefficients(*fine_set)
            wait_load("fine_prev")
        fine_ghosts(s, ())
        fine_total = middle(s, *fine_set)
        for dx in (-1, 1):
            receive(s, "co", "cx", side=dx)
            if s == 0:
                receive(0, "mcx", side=dx)
                side_coefficients(Coarse, 0 if dx < 0 else 7, 1, *coarse_set[1:])
            coarse_total = coarse_total + outer(s, dx, *coarse_set)
            if not last:
                pack_coarse_corners(s + 1, dx)
                send(s + 1, "co", dx=dx)
                send(s + 1, "cx", dx=dx)
        eacc[s, 1] = coarse_total
        if not last:
            pack_y(Coarse, s + 1)
            pack_plane(s + 1)
            send(s + 1, "cy", "cq", "cp")
        for dx in (-1, 1):
            receive(s, "cp", "fo", "fx", side=dx)
            if s == 0:
                receive(0, "mfx", side=dx)
                side_coefficients(Fine, 0 if dx < 0 else 15, 1, *fine_set[1:])
            fine_ghosts(s, (-1,) if dx < 0 else (-1, 1))
            fine_total = fine_total + outer(s, dx, *fine_set)
            if not last:
                pack_corners(s + 1, dx)
                send(s + 1, "fo", dx=dx)
                send(s + 1, "fx", dx=dx)
        eacc[s, 0] = fine_total
        if not last:
            pack_y(Fine, s + 1)
            send(s + 1, "fy")
        if s == 0:
            round_signals(0)
        elif s == 1:
            round_wait(0)
            round_signals(1)
        else:
            round_wait(1)

    lane1 = lanes((1, 128))
    row = jnp.zeros((1, 128), F32)
    cells = (nx * ny * 16 * 16 * 128, nx * ny * 8 * 8 * 256)
    for s in range(STEPS):
        for m in (0, 1):
            value = jnp.sum(eacc[s, m], axis=0, keepdims=True)
            value = jnp.sum(value, axis=1, keepdims=True)
            row = jnp.where(lane1 == STEPS * m + s, value * (1.0 / cells[m]), row)
    erow[0] = row
    er1[me1] = row

    def rows(buffer, n, stage):
        part = buffer.at[pl.ds(0, n)]
        return pltpu.make_async_remote_copy(
            src_ref=part, dst_ref=part, send_sem=esend.at[stage], recv_sem=erecv.at[stage],
            device_id={"gx": line_x[0], "gy": gy}, device_id_type=MESH,
        )

    def pass_on(stage, slot, where):
        pltpu.make_async_remote_copy(
            src_ref=erow.at[stage], dst_ref=slot, send_sem=esend.at[stage],
            recv_sem=erecv.at[stage], device_id=where, device_id_type=MESH,
        ).start()

    for a in reversed(range(group_x)):
        for b in reversed(range(half)):
            if a or b:
                pass_on(0, er1.at[me1], {"gx": plane_x[a], "gy": plane_y[b] + 1})

    @pl.when(first_core)
    def _():
        pass_on(0, er1.at[me1], {"gx": gx, "gy": 2 * chip_y + 1})

    @pl.when(second)
    def _():
        rows(er1, n1 - 1, 0).wait_recv()
        plane = er1[0]
        for m in range(1, n1):
            plane = plane + er1[m]
        erow[1] = plane
        er2[gx_hi] = plane
        for d in far_first:
            for core in (0, 1):
                pass_on(1, er2.at[gx_hi], {"gx": line_x[d], "gy": 2 * chip_y + core})
        pass_on(1, er2.at[gx_hi], {"gx": gx, "gy": 2 * chip_y})
        if n2 > 1:
            rows(er2, n2 - 1, 1).wait_recv()

    @pl.when(first_core)
    def _():
        rows(er2, n2, 1).wait_recv()

    row = er2[0]
    for m in range(1, n2):
        row = row + er2[m]
    for m in (0, 1):
        energy_out[pl.ds(m, 1), :] = roll(row, -STEPS * m, 1)[:, 0:STEPS]

    @pl.when(second)
    def _():
        rows(er1, n1 // 2 - 1, 0).wait_send()
        rows(er1, 2 * n2 - 1, 1).wait_send()

    @pl.when(first_core)
    def _():
        rows(er1, n1 // 2, 0).wait_send()

    for s in range(STEPS):
        run(s, ("co", "cp", "cq", "fo", "cx", "cy", "mcx", "mcy", "mfx", "mfy", "fx", "fy"), "wait_send")


def hand_out(*refs):
    copies = [pltpu.make_async_copy(refs[n], refs[3 + n], refs[6].at[n]) for n in range(3)]
    for c in copies:
        c.start()
    for c in copies:
        c.wait()


def per_device(nx, ny, group_x, *args):
    args = list(args)
    for m in range(4):
        shape = args[m].shape
        args[m] = args[m].reshape(shape[0], shape[1] * shape[2], shape[3])
    for m in range(4, 12):
        shape = args[m].shape
        args[m] = args[m].reshape(shape[0] * shape[1], shape[2])
    for m in range(13):
        args[m] = pltpu.with_memory_space_constraint(args[m], pltpu.HBM)
    vm, dma = pltpu.VMEM, pltpu.SemaphoreType.DMA
    n1, n2 = group_x * ny, nx // group_x
    scratch = [
        vm((STEPS + 1, 3, 256, 128), F32),
        vm((STEPS + 1, 3, 2, 64, 128), F32),
        vm((4, 256, 128), F32),
        vm((4, 2, 64, 128), F32),
        vm((NCOEF, 256, 128), F32),
        vm((NCOEF, 2, 64, 128), F32),
        vm((18 * 16, 128), F32),
        vm((2, 10 * 8, 128), F32),
        vm((2, 16, 128), F32),
        vm((2, 2, 8, 128), F32),
        vm((STEPS, 2, 4, 16, 128), F32),
        vm((STEPS, 2, 4, 2, 8, 128), F32),
        vm((STEPS, 2, 4, 16, 128), F32),
        vm((STEPS, 2, 4, 2, 8, 128), F32),
        vm((STEPS, 2, 4, 16, 128), F32),
        vm((STEPS, 2, 4, 2, 8, 128), F32),
        vm((2, 2, 16, 128), F32),
        vm((2, 2, 2, 8, 128), F32),
        vm((2, 2, 16, 128), F32),
        vm((2, 2, 2, 8, 128), F32),
        vm((2, 2, 16, 128), F32),
        vm((2, 2, 2, 8, 128), F32),
        vm((STEPS, 8, 128), F32),
        vm((STEPS, 2, 8, 128), F32),
        vm((STEPS, 2, 8, 128), F32),
        vm((STEPS, 8, 128), F32),
        vm((STEPS, 4, 4, 1, 128), F32),
        vm((STEPS, 4, 4, 1, 128), F32),
        vm((STEPS, 4, 2, 1, 128), F32),
        vm((STEPS, 4, 2, 1, 128), F32),
        vm((STEPS, 4, 2, 1, 128), F32),
        vm((STEPS, 4, 2, 1, 128), F32),
        vm((2, 16, 16), jnp.int32),
        vm((2, 8, 8, 128), F32),
        vm((2, 8, 128), F32),
        vm((STEPS, 2, 8, 128), F32),
        vm((2, 1, 128), F32),
        vm((max(n1, 2 * n2), 1, 128), F32),
        vm((max(n2, 1), 1, 128), F32),
        dma((13, 2)),
        dma((STEPS, 36)),
        dma((STEPS, 36)),
        dma((2,)),
        dma((2,)),
        pltpu.SemaphoreType.REGULAR((2, 2)),
        pltpu.SemaphoreType.REGULAR((2, 2)),
    ]
    anywhere = pl.BlockSpec(memory_space=pltpu.HBM)
    in_vmem = pl.BlockSpec(memory_space=pltpu.VMEM)
    out_shape = (
        jax.ShapeDtypeStruct((3, 256, 128), F32),
        jax.ShapeDtypeStruct((3, 64, 256), F32),
        jax.ShapeDtypeStruct((2, STEPS), F32),
    )
    results = pl.pallas_call(
        functools.partial(kernel, nx, ny, group_x),
        out_shape=out_shape,
        in_specs=[anywhere] * 13,
        out_specs=(in_vmem, in_vmem, in_vmem),
        scratch_shapes=scratch,
        compiler_params=pltpu.CompilerParams(
            collective_id=0, has_side_effects=True, vmem_limit_bytes=32 << 20
        ),
        name="leapfrog",
    )(*args)
    fine, coarse, energy = pl.pallas_call(
        hand_out,
        out_shape=out_shape,
        in_specs=[in_vmem] * 3,
        out_specs=[anywhere] * 3,
        scratch_shapes=[dma((3,))],
        compiler_params=pltpu.CompilerParams(vmem_limit_bytes=1 << 20),
        name="hand_out",
    )(*results)
    energy = energy.T
    return fine.reshape(3, 16, 16, 128), coarse.reshape(3, 8, 8, 256), energy


def solution(mesh):
    nx, ny = mesh.shape["gx"], mesh.shape["gy"]
    group_x = next(m for m in (4, 2, 1) if nx % m == 0)
    field, cells = P(None, "gx", "gy", None), P("gx", "gy", None)
    return jax.shard_map(
        functools.partial(per_device, nx, ny, group_x),
        mesh=mesh,
        in_specs=(field,) * 4 + (cells,) * 8 + (P(None, "gx", "gy"),),
        out_specs=(field, field, P()),
        check_vma=False,
    )
```

```python
import functools
import math

import jax
import jax.numpy as jnp
from jax import lax
from jax.experimental import pallas as pl
from jax.experimental.pallas import tpu as pltpu
from jax.sharding import PartitionSpec as P

STEPS = 3
DT = 0.15
MESH = pl.DeviceIdType.MESH
F32 = jnp.float32

R = 2
LO, HI = 0, 1
(WIDE, HALF_A, ISV, GB, GZ, DM, CZU, CZD, CXP, CXM, CYU, CYD, C0) = range(13)
NCOEF = 13


def lanes(shape):
    return lax.broadcasted_iota(jnp.int32, shape, len(shape) - 1)


def subs(shape):
    return lax.broadcasted_iota(jnp.int32, shape, len(shape) - 2)


def spread_row(row):
    return jnp.broadcast_to(row, (8, 128))


def roll(x, shift, axis):
    return pltpu.roll(x, shift % x.shape[axis], axis)


class Fine:
    n = 16
    key = "f"

    @staticmethod
    def load(ref, i, r):
        parts = [ref[pl.ds(16 * i + t, 8 * r, stride=2), :].reshape(1, r, 8, 128) for t in (0, 1)]
        return jnp.concatenate(parts, axis=0)

    @staticmethod
    def store(ref, i, r, value):
        for t in (0, 1):
            ref[pl.ds(16 * i + t, 8 * r, stride=2), :] = value[t].reshape(8 * r, 128)

    @staticmethod
    def k_up(x, last=None):
        moved = roll(x, -1, 3)
        edge = x if last is None else last
        return jnp.where(lanes(x.shape) == 127, edge, moved)

    @staticmethod
    def k_down(x, first=None):
        moved = roll(x, 1, 3)
        edge = x if first is None else first
        return jnp.where(lanes(x.shape) == 0, edge, moved)

    @staticmethod
    def edge_scale(shape):
        k = lanes(shape)
        return jnp.where((k == 0) | (k == 127), 1.0, 0.5).astype(F32)

    @staticmethod
    def row_of(ref, i, r):
        return jnp.concatenate(
            [spread_row(ref[pl.ds(i + m, 1), :]).reshape(1, 8, 128) for m in range(r)], axis=0
        )

    @staticmethod
    def j_up(x, halo):
        s = subs(x.shape[1:])
        moved = jnp.where(s == 7, halo, roll(x[0], -1, 1))
        return jnp.stack([x[1], moved])

    @staticmethod
    def j_down(x, halo):
        s = subs(x.shape[1:])
        moved = jnp.where(s == 0, halo, roll(x[1], 1, 1))
        return jnp.stack([moved, x[0]])

    @staticmethod
    def plane(ref, j):
        return jnp.concatenate([ref[pl.ds(j + 128 * h, 8, stride=16), :] for h in (0, 1)], axis=0)

    @staticmethod
    def plane_k_up(x):
        return jnp.where(lanes(x.shape) == 127, x, roll(x, -1, 1))

    @staticmethod
    def plane_k_down(x):
        return jnp.where(lanes(x.shape) == 0, x, roll(x, 1, 1))

    @staticmethod
    def corner_plane(tile_ref, comp):
        row = spread_row(tile_ref[comp])
        return jnp.concatenate([row, row], axis=0)

    @staticmethod
    def corner_row(tile_ref, comp):
        return spread_row(tile_ref[comp]).reshape(1, 8, 128)


class Coarse:
    n = 8
    key = "c"

    @staticmethod
    def load(ref, i, r):
        return ref[:, pl.ds(8 * i, 8 * r), :].reshape(2, r, 8, 128)

    @staticmethod
    def store(ref, i, r, value):
        ref[:, pl.ds(8 * i, 8 * r), :] = value.reshape(2, 8 * r, 128)

    @staticmethod
    def k_up(x, last=None):
        moved = roll(x, -1, 3)
        edge = x[1] if last is None else last
        return jnp.where(lanes(x.shape) == 127, jnp.stack([moved[1], edge]), moved)

    @staticmethod
    def k_down(x, first=None):
        moved = roll(x, 1, 3)
        edge = x[0] if first is None else first
        return jnp.where(lanes(x.shape) == 0, jnp.stack([edge, moved[0]]), moved)

    @staticmethod
    def edge_scale(shape):
        k = lanes(shape)
        half = lax.broadcasted_iota(jnp.int32, shape, 0)
        ends = ((k == 0) & (half == 0)) | ((k == 127) & (half == 1))
        return jnp.where(ends, 1.0, 0.5).astype(F32)

    @staticmethod
    def row_of(ref, i, r):
        halves = []
        for h in (0, 1):
            rows = [spread_row(ref[h, pl.ds(i + m, 1), :]).reshape(1, 8, 128) for m in range(r)]
            halves.append(jnp.concatenate(rows, axis=0))
        return jnp.stack(halves)

    @staticmethod
    def j_up(x, halo):
        return jnp.where(subs(x.shape) == 7, halo, roll(x, -1, 2))

    @staticmethod
    def j_down(x, halo):
        return jnp.where(subs(x.shape) == 0, halo, roll(x, 1, 2))

    @staticmethod
    def plane(ref, j):
        return jnp.stack([ref[h, pl.ds(j, 8, stride=8), :] for h in (0, 1)])

    @staticmethod
    def plane_k_up(x):
        return Coarse.k_up(x[:, None])[:, 0]

    @staticmethod
    def plane_k_down(x):
        return Coarse.k_down(x[:, None])[:, 0]

    @staticmethod
    def corner_plane(tile_ref, comp):
        return jnp.stack([spread_row(tile_ref[2 * comp + h]) for h in (0, 1)])

    @staticmethod
    def corner_row(tile_ref, comp):
        rows = [spread_row(tile_ref[2 * comp + h]) for h in (0, 1)]
        return jnp.stack(rows)[:, None]


def plane_roll(level, x, shift):
    return roll(x, shift, 0) if level is Fine else roll(x, shift, 1)


def plane_sub(level, x):
    return subs(x.shape)


def neighbour_rows(level, ref, i, r, step, halo):
    if step > 0:
        if i + r < level.n:
            return level.load(ref, i + 1, r)
        return halo() if r == 1 else jnp.concatenate([level.load(ref, i + 1, r - 1), halo()], axis=1)
    if i > 0:
        return level.load(ref, i - 1, r)
    return halo() if r == 1 else jnp.concatenate([halo(), level.load(ref, 0, r - 1)], axis=1)


def kernel(nx, ny, group_x, *refs):
    names_in = ["fine_disp", "fine_prev", "coarse_disp", "coarse_prev"]
    for name in ("fine", "coarse"):
        names_in += [name + part for part in ("_density", "_lame", "_rigidity", "_metric")]
    hbm = dict(zip(names_in, refs[:12]))
    offsets_hbm = refs[12]
    fine_out, coarse_out, energy_out = refs[13:16]
    (
        uf, uc, matf, matc, kf, kc, dvf, dvc, dyf, dyc,
        xhf, xhc, yhf, yhc, ysf, ysc, xmf, xmc, ymf, ymc, ysmf, ysmc,
        pls, plx, ply, pex, ccs, ccr, fcs, fcr, sized, offsets_ref, weights, ghost, eacc, erow, er1, er2,
        load_sem, send_sem, recv_sem, esend, erecv, line_sem, plane_sem,
    ) = refs[16:]

    gx, gy = lax.axis_index("gx"), lax.axis_index("gy")
    exists = {
        (dx, dy): functools.reduce(
            jnp.logical_and,
            ([gx > 0] if dx < 0 else [gx < nx - 1] if dx > 0 else [])
            + ([gy > 0] if dy < 0 else [gy < ny - 1] if dy > 0 else []),
        )
        for dx, dy in ((-1, 0), (1, 0), (-1, -1), (-1, 1), (1, -1), (1, 1), (0, -1), (0, 1))
    }
    directions = list(exists)
    corners = [d for d in directions if d[0] and d[1]]
    corner_id = {d: n for n, d in enumerate(corners)}

    def flag(direction):
        return jnp.where(exists[direction], 1.0, 0.0).astype(F32)

    def device(direction):
        return {"gx": gx + direction[0], "gy": gy + direction[1]}

    groups, half = nx // group_x, ny // 2
    gx_hi, gx_lo = gx // group_x, gx % group_x
    chip_y, second = gy // 2, gy % 2 == 1
    first_core = jnp.logical_not(second)
    n1, n2 = group_x * ny, groups
    me1 = gx_lo * ny + gy
    plane_x = [gx_hi * group_x + lax.rem(gx_lo + a, group_x) for a in range(group_x)]
    plane_y = [2 * lax.rem(chip_y + b, half) for b in range(half)]
    line_x = [lax.rem(gx_hi + d, n2) * group_x + gx_lo for d in range(n2)]

    def start_load(name, dst, sem):
        src = hbm[name]
        if name.startswith("fine"):
            pltpu.make_async_copy(src, dst, load_sem.at[sem]).start()
            return
        lead = (slice(None),) * (len(src.shape) - 2)
        for h in (0, 1):
            pltpu.make_async_copy(
                src.at[lead + (slice(None), pl.ds(128 * h, 128))],
                dst.at[(slice(None), h) if lead else (h,)],
                load_sem.at[sem],
            ).start()

    plan = [
        ("fine_disp", uf.at[1], 0), ("coarse_disp", uc.at[1], 1),
        ("fine_rigidity", matf.at[0], 0), ("coarse_rigidity", matc.at[0], 1),
        ("fine_metric", matf.at[1], 0), ("coarse_metric", matc.at[1], 1),
        ("fine_density", matf.at[2], 2), ("fine_lame", matf.at[3], 2),
        ("coarse_density", matc.at[2], 3), ("coarse_lame", matc.at[3], 3),
        ("fine_prev", uf.at[0], 4), ("coarse_prev", uc.at[0], 5),
    ]
    for entry in plan:
        start_load(*entry)
    offsets_load = pltpu.make_async_copy(offsets_hbm, offsets_ref, load_sem.at[6])
    offsets_load.start()
    load_sizes = (kf.at[pl.ds(0, 5)], kc.at[pl.ds(0, 5)], kf.at[pl.ds(0, 2)], kc.at[pl.ds(0, 2)],
                  kf.at[pl.ds(0, 3)], kc.at[pl.ds(0, 3)])

    def wait_load(*sems):
        for sem in sems:
            pltpu.make_async_copy(load_sizes[sem], load_sizes[sem], load_sem.at[sem]).wait()

    barrier = pltpu.get_barrier_semaphore()

    def greet(where):
        pl.semaphore_signal(barrier, inc=1, device_id=where, device_id_type=MESH)

    far_first = sorted(range(1, n2), key=lambda d: -min(d, n2 - d))
    by_one = sorted({1, n2 - 1}) if n2 > 1 else []
    by_two = sorted({2, n2 - 2}) if n2 > 3 else []
    for d in by_one:
        greet({"gx": line_x[d], "gy": 2 * chip_y + 1})
    for d in directions:
        @pl.when(exists[d])
        def _(d=d):
            greet(device(d))

    side_of = {-1: LO, 1: HI}

    def messages(s):
        out = []
        u_f, u_c = uf.at[s + 1], uc.at[s + 1]
        for dx in (-1, 1):
            own, far = side_of[dx], side_of[-dx]
            first, second = (0, 1) if dx < 0 else (15, 14)
            out.append(("fx", (dx, 0), u_f.at[:, pl.ds(16 * first, 16)], xhf.at[s, far, pl.ds(0, 3)]))
            out.append(("fx", (dx, 0), u_f.at[0, pl.ds(16 * second, 16)], xhf.at[s, far, 3]))
            first, second = (0, 1) if dx < 0 else (7, 6)
            out.append(("cx", (dx, 0), u_c.at[:, :, pl.ds(8 * first, 8)], xhc.at[s, far, pl.ds(0, 3)]))
            out.append(("cx", (dx, 0), u_c.at[0, :, pl.ds(8 * second, 8)], xhc.at[s, far, 3]))
            out.append(("cp", (dx, 0), pex.at[s], plx.at[s, far]))
            if s == 0:
                first = 0 if dx < 0 else 15
                out.append(("mfx", (dx, 0), matf.at[pl.ds(0, 2), pl.ds(16 * first, 16)], xmf.at[far]))
                first = 0 if dx < 0 else 7
                out.append(("mcx", (dx, 0), matc.at[pl.ds(0, 2), :, pl.ds(8 * first, 8)], xmc.at[far]))
        for dy in (-1, 1):
            own, far = side_of[dy], side_of[-dy]
            out.append(("fy", (0, dy), ysf.at[s, own], yhf.at[s, far]))
            out.append(("cy", (0, dy), ysc.at[s, own], yhc.at[s, far]))
            out.append(("cq", (0, dy), pls.at[s], ply.at[s, far]))
            if s == 0:
                out.append(("mfy", (0, dy), ysmf.at[own], ymf.at[far]))
                out.append(("mcy", (0, dy), ysmc.at[own], ymc.at[far]))
        for d in corners:
            back = corner_id[(-d[0], -d[1])]
            out.append(("co", d, ccs.at[s, corner_id[d]], ccr.at[s, back]))
            out.append(("fo", d, fcs.at[s, corner_id[d]], fcr.at[s, back]))
        return out

    wait_with = {"cp": "fx", "mfx": "fx", "mcx": "cx", "cq": "fy", "mfy": "fy", "mcy": "cy"}
    slots, copies, arriving, leaving = {}, [], [], dict.fromkeys(directions, 0)
    for s in range(STEPS):
        entries, rows_of = [], {}
        for group, d, src, dst in messages(s):
            name = wait_with.get(group, group)
            key = (s if name == "fx" else s % 2, name, d)
            slot = slots.setdefault(key, len(slots))
            rows = math.prod(src.shape) // 128
            rows_of[key] = rows_of.get(key, 0) + rows
            leaving[d] += rows

            def copy(src=src, dst=dst, slot=slot, d=d):
                return pltpu.make_async_remote_copy(
                    src_ref=src, dst_ref=dst,
                    send_sem=send_sem.at[directions.index(d)], recv_sem=recv_sem.at[slot],
                    device_id=device(d), device_id_type=MESH,
                )

            entries.append((group, d, copy))
        copies.append(entries)
        arriving.append(rows_of)

    def bytes_of(rows, d, slot):
        part = sized.at[pl.ds(0, rows)]
        return pltpu.make_async_remote_copy(
            src_ref=part, dst_ref=part,
            send_sem=send_sem.at[directions.index(d)], recv_sem=recv_sem.at[slot],
            device_id=device(d), device_id_type=MESH,
        )

    def send(s, *wanted, dx=None):
        for d in directions:
            mine = [c for g, e, c in copies[s] if g in wanted and e == d]
            if mine and dx in (None, d[0]):
                @pl.when(exists[d])
                def _(mine=mine):
                    for c in mine:
                        c().start()

    def receive(s, *wanted, side=None):
        for d in directions:
            mine = [k for k in arriving[s] if k[1] in wanted and k[2] == d]
            if mine and (side is None or d[0] == -side):
                @pl.when(exists[(-d[0], -d[1])])
                def _(mine=mine, d=d):
                    for k in mine:
                        bytes_of(arriving[s][k], d, slots[k]).wait_recv()

    def round_signals(stage):
        away = 2 << stage
        for side, ok, to in ((LO, gy + away < ny, gy + away), (HI, gy >= away, gy - away)):
            if ny > 5:
                @pl.when(ok)
                def _(side=side, to=to):
                    pl.semaphore_signal(
                        plane_sem.at[stage, side], inc=1,
                        device_id={"gx": gx, "gy": to}, device_id_type=MESH,
                    )
        if n2 > 3:
            @pl.when(second)
            def _():
                for m, d in enumerate((by_one, by_two)[stage]):
                    pl.semaphore_signal(
                        line_sem.at[stage, m], inc=1,
                        device_id={"gx": line_x[d], "gy": gy}, device_id_type=MESH,
                    )

    def round_wait(stage):
        away = 2 << stage
        for side, ok in ((LO, gy >= away), (HI, gy + away < ny)):
            if ny > 5:
                @pl.when(ok)
                def _(side=side):
                    pl.semaphore_wait(plane_sem.at[stage, side], 1)
        if n2 > 3:
            @pl.when(second)
            def _():
                for m in range(len((by_one, by_two)[stage])):
                    pl.semaphore_wait(line_sem.at[stage, m], 1)

    def pack_y(level, s):
        u, out = (uf, ysf) if level is Fine else (uc, ysc)
        last = 15 if level is Fine else 7
        for side, (j0, j1) in ((LO, (0, 1)), (HI, (last, last - 1))):
            for c in range(3):
                out[s, side, c] = level.plane(u.at[s + 1, c], j0)
            out[s, side, 3] = level.plane(u.at[s + 1, 1], j1)

    def plane_tile(s, tile, rows):
        lane = lanes((8, 128))
        for c in range(3):
            for i in rows:
                column = uc[s + 1, c, 0, pl.ds(8 * i, 8), 0:1]
                at = 16 * c + 2 * i
                tile = jnp.where((lane == at) | (lane == at + 1), column, tile)
        return tile

    def pack_coarse_corners(s, side):
        for (dx, dy), n in corner_id.items():
            if dx != side:
                continue
            ci, cj = (0 if dx < 0 else 7), (0 if dy < 0 else 7)
            for c in (0, 1):
                for h in (0, 1):
                    ccs[s, n, 2 * c + h] = uc[s + 1, c, h, pl.ds(8 * ci + cj, 1), :]

    def pack_plane(s):
        edge = plane_tile(s, jnp.zeros((8, 128), F32), (0, 1, 7))
        pex[s] = edge
        pls[s] = plane_tile(s, edge, range(2, 7))
        for (dx, dy), n in corner_id.items():
            for m, j in enumerate((0, 1) if dy < 0 else (7, 7)):
                fcs[s, n, 2 + m] = edge[j : j + 1]

    def pack_corners(s, side):
        for (dx, dy), n in corner_id.items():
            if dx != side:
                continue
            fi, fj = (0 if dx < 0 else 15), (0 if dy < 0 else 15)
            for c in (0, 1):
                fcs[s, n, c] = uf[s + 1, c, pl.ds(16 * fi + fj, 1), :]

    for dx in (-1, 1):
        @pl.when(jnp.logical_not(exists[(dx, 0)]))
        def _(side=side_of[dx]):
            for s in range(STEPS):
                xhf[s, side] = jnp.zeros(xhf.shape[2:], F32)
                xhc[s, side] = jnp.zeros(xhc.shape[2:], F32)
                plx[s, side] = jnp.zeros((8, 128), F32)
            xmf[side, 0] = jnp.zeros(xmf.shape[2:], F32)
            xmf[side, 1] = jnp.ones(xmf.shape[2:], F32)
            xmc[side, 0] = jnp.zeros(xmc.shape[2:], F32)
            xmc[side, 1] = jnp.ones(xmc.shape[2:], F32)
    for dy in (-1, 1):
        @pl.when(jnp.logical_not(exists[(0, dy)]))
        def _(side=side_of[dy]):
            for s in range(STEPS):
                yhf[s, side] = jnp.zeros(yhf.shape[2:], F32)
                yhc[s, side] = jnp.zeros(yhc.shape[2:], F32)
                ply[s, side] = jnp.zeros((8, 128), F32)
            ymf[side, 0] = jnp.zeros(ymf.shape[2:], F32)
            ymf[side, 1] = jnp.ones(ymf.shape[2:], F32)
            ymc[side, 0] = jnp.zeros(ymc.shape[2:], F32)
            ymc[side, 1] = jnp.ones(ymc.shape[2:], F32)
    for d in corners:
        @pl.when(jnp.logical_not(exists[d]))
        def _(n=corner_id[d]):
            for s in range(STEPS):
                ccr[s, n] = jnp.zeros(ccr.shape[2:], F32)
                fcr[s, n] = jnp.zeros(fcr.shape[2:], F32)

    wait_load(0, 1)
    for c in (0, 1):
        for side, jf, jc in ((LO, 0, 0), (HI, 15, 7)):
            ysmf[side, c] = Fine.plane(matf.at[c], jf)
            ysmc[side, c] = Coarse.plane(matc.at[c], jc)
    pack_y(Fine, 0)
    pack_y(Coarse, 0)
    for dx in (-1, 1):
        pack_coarse_corners(0, dx)
        pack_corners(0, dx)
    pack_plane(0)

    greeted = jnp.where(second, 2 * len(by_one), 0).astype(jnp.int32)
    for d in directions:
        greeted = greeted + jnp.where(exists[d], 1, 0).astype(jnp.int32)
    pl.semaphore_wait(barrier, greeted)

    send(0, "co")
    send(0, "cx", "mcx")
    send(0, "cy", "mcy", "cq", "fy", "mfy")
    send(0, "fo", "fx", "mfx")
    send(0, "cp")

    wait_load(2, 3)
    offsets_load.wait()
    lane8 = lanes((8, 128))
    spread = jnp.where(
        (lanes((16, 128)) % 16 == subs((16, 128))) & (lanes((16, 128)) < 48), 1.0, 0.0
    ).astype(F32)
    for t in (0, 1):
        pick = jnp.where(lanes((8, 16)) == 2 * subs((8, 16)) + t, 1.0, 0.0).astype(F32)
        for axis in (0, 1):
            table = offsets_ref[axis].astype(F32)
            turned = lax.dot_general(
                pick, table, (((1,), (1,)), ((), ())), preferred_element_type=F32
            )
            shift = jnp.dot(turned, spread, preferred_element_type=F32)
            if axis == 0:
                near = jnp.where(lane8 % 2 == 0, 0.75, 0.25).astype(F32)
            else:
                near = jnp.full((8, 128), 0.75 if t == 0 else 0.25, F32)
            for m, value in enumerate((-1.0, 0.0, 1.0, 2.0)):
                weights[t, 4 * axis + m] = jnp.where(shift == value, near, 0.0) + jnp.where(
                    shift == value - 1.0, 1.0 - near, 0.0
                )

    levels = (
        (Coarse, uc, matc, kc, dvc, dyc, xhc, yhc, ysc, xmc, ymc),
        (Fine, uf, matf, kf, dvf, dyf, xhf, yhf, ysf, xmf, ymf),
    )
    for level, u, mat, k, dv, dy_, xh, yh, ys, xm, ym in levels:
        for i in range(0, level.n, R):
            rig, met, den, lam = (level.load(mat.at[m], i, R) for m in range(4))
            scale = level.edge_scale(rig.shape)
            inverse = 1.0 / met
            light = DT / den
            a = inverse * light
            vertical = rig * inverse
            b = (lam + rig) * light
            isv = inverse * scale
            half_a = 0.5 * a
            for slot, value in (
                (WIDE, rig * met), (HALF_A, half_a), (ISV, isv), (GB, 0.5 * b), (GZ, b * isv),
                (DM, den * met), (CZU, half_a * (vertical + level.k_up(vertical))),
                (CZD, half_a * (vertical + level.k_down(vertical))),
            ):
                level.store(k.at[slot], i, R, value)

    def halo_row(level, ref):
        if level is Fine:
            return Fine.load(ref, 0, 1)
        return Coarse.load(ref, 0, 1)

    def side_coefficients(level, i, r, u, mat, k, dv, dy_, xh, yh, ys, xm, ym):
        w = level.load(k.at[WIDE], i, r)
        ha = level.load(k.at[HALF_A], i, r)

        def outer(side):
            return halo_row(level, xm.at[side, 0]) * halo_row(level, xm.at[side, 1])

        cxp = ha * (w + neighbour_rows(level, k.at[WIDE], i, r, 1, lambda: outer(HI)))
        cxm = ha * (w + neighbour_rows(level, k.at[WIDE], i, r, -1, lambda: outer(LO)))
        up = level.row_of(ym.at[HI, 0], i, r) * level.row_of(ym.at[HI, 1], i, r)
        down = level.row_of(ym.at[LO, 0], i, r) * level.row_of(ym.at[LO, 1], i, r)
        cyu = ha * (w + level.j_up(w, up))
        cyd = ha * (w + level.j_down(w, down))
        total = cxp + cxm + cyu + cyd + level.load(k.at[CZU], i, r) + level.load(k.at[CZD], i, r)
        for slot, value in ((CXP, cxp), (CXM, cxm), (CYU, cyu), (CYD, cyd), (C0, total)):
            level.store(k.at[slot], i, r, value)

    def inner_coefficients(level, *rest):
        for i, r in [(1, 1)] + [(i, R) for i in range(2, level.n - 2, R)] + [(level.n - 2, 1)]:
            side_coefficients(level, i, r, *rest)

    def row_divergence(s, i, r, level, u, mat, k, dv, dy_, xh, yh, ys, xm, ym):
        now = u.at[s + 1]

        def halo(side):
            return lambda: halo_row(level, xh.at[s, side, 0])

        px = neighbour_rows(level, now.at[0], i, r, 1, halo(HI))
        mx = neighbour_rows(level, now.at[0], i, r, -1, halo(LO))
        y = level.load(now.at[1], i, r)
        z = level.load(now.at[2], i, r)
        py = level.j_up(y, level.row_of(yh.at[s, HI, 1], i, r))
        my = level.j_down(y, level.row_of(yh.at[s, LO, 1], i, r))
        isv = level.load(k.at[ISV], i, r)
        value = 0.5 * ((px - mx) + (py - my)) + isv * (level.k_up(z) - level.k_down(z))
        level.store(dv, i + 1, r, value)

    def x_side_divergence(s, dx, level, u, mat, k, dv, dy_, xh, yh, ys, xm, ym):
        cor = fcr if level is Fine else ccr
        now, n = u.at[s + 1], level.n
        side = side_of[dx]
        inside = level.load(now.at[0], 0 if dx < 0 else n - 1, 1)
        beyond = halo_row(level, xh.at[s, side, 3])
        y = halo_row(level, xh.at[s, side, 1])
        z = halo_row(level, xh.at[s, side, 2])
        py = level.j_up(y, level.corner_row(cor.at[s, corner_id[(dx, 1)]], 1))
        my = level.j_down(y, level.corner_row(cor.at[s, corner_id[(dx, -1)]], 1))
        isv = level.edge_scale(z.shape) / halo_row(level, xm.at[side, 1])
        along = (beyond - inside) if dx > 0 else (inside - beyond)
        value = 0.5 * (along + (py - my)) + isv * (level.k_up(z) - level.k_down(z))
        level.store(dv, 0 if dx < 0 else n + 1, 1, value * flag((dx, 0)))

    def y_side_divergence(s, known, level, u, mat, k, dv, dy_, xh, yh, ys, xm, ym):
        cor = fcr if level is Fine else ccr
        n = level.n
        for dy, side in side_of.items():
            x, z, beyond = yh[s, side, 0], yh[s, side, 2], yh[s, side, 3]
            inside = ys[s, side, 1]
            sub = plane_sub(level, x)
            px, mx = plane_roll(level, x, -1), plane_roll(level, x, 1)
            if 1 in known:
                px = jnp.where(sub == n - 1, level.corner_plane(cor.at[s, corner_id[(1, dy)]], 0), px)
            if -1 in known:
                mx = jnp.where(sub == 0, level.corner_plane(cor.at[s, corner_id[(-1, dy)]], 0), mx)
            isv = level.edge_scale(z.shape) / ym[side, 1]
            along = (beyond - inside) if dy > 0 else (inside - beyond)
            value = 0.5 * (along + (px - mx)) + isv * (level.plane_k_up(z) - level.plane_k_down(z))
            dy_[side] = value * flag((0, dy))

    def middle(s, level, *rest):
        n = level.n
        y_side_divergence(s, (), level, *rest)
        row_divergence(s, 1, 1, level, *rest)
        for i in range(2, n - 2, R):
            row_divergence(s, i, R, level, *rest)
        row_divergence(s, n - 2, 1, level, *rest)
        total = jnp.zeros((8, 128), F32)
        for i in range(R, first_outer(level), R):
            total = total + rates(s, i, level, *rest)
        return total

    def first_outer(level):
        return level.n - (4 if level is Fine else 2)

    def outer(s, dx, level, *rest):
        n = level.n
        x_side_divergence(s, dx, level, *rest)
        y_side_divergence(s, (-1,) if dx < 0 else (-1, 1), level, *rest)
        row_divergence(s, 0 if dx < 0 else n - 1, 1, level, *rest)
        if dx < 0:
            return rates(s, 0, level, *rest)
        total = rates(s, n - R, level, *rest)
        for i in range(first_outer(level), n - R, R):
            total = total + rates(s, i, level, *rest)
        return total

    def fine_ghosts(s, known):
        sub, lane = subs((8, 128)), lanes((8, 128)) % 16

        def shifted_rows(tile, low, high0, high1):
            return [
                jnp.where(sub == 0, low, roll(tile, 1, 0)),
                tile,
                jnp.where(sub == 7, high0, roll(tile, -1, 0)),
                jnp.where(sub == 7, high1, jnp.where(sub == 6, high0, roll(tile, -2, 0))),
            ]

        def row(ref, j):
            return spread_row(ref[pl.ds(j, 1), :])

        def corner_rows(dx):
            low, high = fcr.at[s, corner_id[(dx, -1)]], fcr.at[s, corner_id[(dx, 1)]]
            return spread_row(low[2]), spread_row(high[2]), spread_row(high[3])

        own = shifted_rows(pls[s], row(ply.at[s, LO], 7), row(ply.at[s, HI], 0), row(ply.at[s, HI], 1))
        if -1 in known:
            left = shifted_rows(plx[s, LO], *corner_rows(-1))
        if 1 in known:
            right = shifted_rows(plx[s, HI], *corner_rows(1))
        totals = [jnp.zeros((8, 128), F32) for _ in (0, 1)]
        for mx in range(4):
            inner = [jnp.zeros((8, 128), F32) for _ in (0, 1)]
            for my in range(4):
                tile = roll(own[my], 2 - 2 * mx, 1) if mx != 1 else own[my]
                if mx == 0 and -1 in known:
                    tile = jnp.where(lane < 2, roll(left[my], -14, 1), tile)
                if mx >= 2 and 1 in known:
                    edge = 18 - 2 * mx
                    tile = jnp.where(lane >= edge, roll(right[my], edge, 1), tile)
                for t in (0, 1):
                    inner[t] = inner[t] + weights[t, 4 + my] * tile
            for t in (0, 1):
                totals[t] = totals[t] + weights[t, mx] * inner[t]
        for t in (0, 1):
            ghost[t] = totals[t]

    def fine_last(c, i):
        rows = []
        for t in (0, 1):
            tile = ghost[t]
            rows.append(jnp.stack([roll(tile, 127 - (16 * c + i + m), 1) for m in range(R)]))
        return jnp.stack(rows)

    def coarse_first(s, c, i):
        rows = []
        for m in range(R):
            base = 32 * (i + m)
            parts = [uf[s + 1, c, pl.ds(base + t, 8, stride=2), :] for t in (0, 1, 16, 17)]
            rows.append(0.25 * ((parts[0] + parts[1]) + (parts[2] + parts[3])))
        return roll(jnp.stack(rows), 1, 2)

    def rates(s, i, level, u, mat, k, dv, dy_, xh, yh, ys, xm, ym):
        now, old = u.at[s + 1], u.at[s]
        coef = {
            m: level.load(k.at[m], i, R) for m in (GB, GZ, DM, CZU, CZD, CXP, CXM, CYU, CYD, C0)
        }
        d_mid = level.load(dv, i + 1, R)
        gradient = [
            coef[GB] * (level.load(dv, i + 2, R) - level.load(dv, i, R)),
            coef[GB]
            * (
                level.j_up(d_mid, level.row_of(dy_.at[HI], i, R))
                - level.j_down(d_mid, level.row_of(dy_.at[LO], i, R))
            ),
            coef[GZ] * (level.k_up(d_mid) - level.k_down(d_mid)),
        ]
        energy = None
        for c in range(3):
            v = level.load(now.at[c], i, R)

            def halo(side, c=c):
                return lambda: halo_row(level, xh.at[s, side, c])

            px = neighbour_rows(level, now.at[c], i, R, 1, halo(HI))
            mx = neighbour_rows(level, now.at[c], i, R, -1, halo(LO))
            py = level.j_up(v, level.row_of(yh.at[s, HI, c], i, R))
            my = level.j_down(v, level.row_of(yh.at[s, LO, c], i, R))
            if level is Fine:
                pz, mz = level.k_up(v, fine_last(c, i)), level.k_down(v)
            else:
                pz = level.k_up(v, jnp.zeros_like(v[1]))
                mz = level.k_down(v, coarse_first(s, c, i))
            rate = (
                (coef[CXP] * px + coef[CXM] * mx)
                + (coef[CYU] * py + coef[CYD] * my)
                + (coef[CZU] * pz + coef[CZD] * mz)
                - coef[C0] * v
                + gradient[c]
            )
            after = (2.0 * v - level.load(old.at[c], i, R)) + rate
            if s < STEPS - 1:
                level.store(u.at[s + 2, c], i, R, after)
            elif level is Fine:
                level.store(fine_out.at[c], i, R, after)
            else:
                for h in (0, 1):
                    coarse_out[c, pl.ds(8 * i, 8 * R), pl.ds(128 * h, 128)] = after[h].reshape(
                        8 * R, 128
                    )
            change = after - v
            part = change * change - after * rate
            energy = part if energy is None else energy + part
        return jnp.sum(coef[DM] * energy, axis=(0, 1))

    coarse_set, fine_set = levels
    for s in range(STEPS):
        last = s == STEPS - 1
        receive(s, "cy")
        if s == 0:
            inner_coefficients(*coarse_set)
            wait_load(5)
        coarse_total = middle(s, *coarse_set)
        receive(s, "fy")
        if s == 0:
            inner_coefficients(*fine_set)
            wait_load(4)
        fine_ghosts(s, ())
        fine_total = middle(s, *fine_set)
        for dx in (-1, 1):
            receive(s, "co", "cx", side=dx)
            if s == 0:
                side_coefficients(Coarse, 0 if dx < 0 else 7, 1, *coarse_set[1:])
            coarse_total = coarse_total + outer(s, dx, *coarse_set)
            if not last:
                pack_coarse_corners(s + 1, dx)
                send(s + 1, "co", dx=dx)
                send(s + 1, "cx", dx=dx)
        eacc[s, 1] = coarse_total
        if not last:
            pack_y(Coarse, s + 1)
            pack_plane(s + 1)
            send(s + 1, "cy", "cq", "cp")
        for dx in (-1, 1):
            receive(s, "fo", "fx", side=dx)
            if s == 0:
                side_coefficients(Fine, 0 if dx < 0 else 15, 1, *fine_set[1:])
            fine_ghosts(s, (-1,) if dx < 0 else (-1, 1))
            fine_total = fine_total + outer(s, dx, *fine_set)
            if not last:
                pack_corners(s + 1, dx)
                send(s + 1, "fo", dx=dx)
                send(s + 1, "fx", dx=dx)
        eacc[s, 0] = fine_total
        if not last:
            pack_y(Fine, s + 1)
            send(s + 1, "fy")
        if s == 0:
            round_signals(0)
        elif s == 1:
            round_wait(0)
            round_signals(1)
        else:
            round_wait(1)

    lane1 = lanes((1, 128))
    row = jnp.zeros((1, 128), F32)
    cells = (nx * ny * 16 * 16 * 128, nx * ny * 8 * 8 * 256)
    for s in range(STEPS):
        for m in (0, 1):
            value = jnp.sum(eacc[s, m], axis=0, keepdims=True)
            value = jnp.sum(value, axis=1, keepdims=True)
            row = jnp.where(lane1 == STEPS * m + s, value * (1.0 / cells[m]), row)
    erow[0] = row
    er1[me1] = row

    def rows(buffer, n, stage):
        part = buffer.at[pl.ds(0, n)]
        return pltpu.make_async_remote_copy(
            src_ref=part, dst_ref=part, send_sem=esend.at[stage], recv_sem=erecv.at[stage],
            device_id={"gx": line_x[0], "gy": gy}, device_id_type=MESH,
        )

    def pass_on(stage, slot, where):
        pltpu.make_async_remote_copy(
            src_ref=erow.at[stage], dst_ref=slot, send_sem=esend.at[stage],
            recv_sem=erecv.at[stage], device_id=where, device_id_type=MESH,
        ).start()

    for a in reversed(range(group_x)):
        for b in reversed(range(half)):
            if a or b:
                pass_on(0, er1.at[me1], {"gx": plane_x[a], "gy": plane_y[b] + 1})

    @pl.when(first_core)
    def _():
        pass_on(0, er1.at[me1], {"gx": gx, "gy": 2 * chip_y + 1})

    @pl.when(second)
    def _():
        rows(er1, n1 - 1, 0).wait_recv()
        plane = er1[0]
        for m in range(1, n1):
            plane = plane + er1[m]
        erow[1] = plane
        er2[gx_hi] = plane
        for d in far_first:
            for core in (0, 1):
                pass_on(1, er2.at[gx_hi], {"gx": line_x[d], "gy": 2 * chip_y + core})
        pass_on(1, er2.at[gx_hi], {"gx": gx, "gy": 2 * chip_y})
        if n2 > 1:
            rows(er2, n2 - 1, 1).wait_recv()

    @pl.when(first_core)
    def _():
        rows(er2, n2, 1).wait_recv()

    row = er2[0]
    for m in range(1, n2):
        row = row + er2[m]
    for m in (0, 1):
        energy_out[pl.ds(m, 1), :] = roll(row, -STEPS * m, 1)[:, 0:STEPS]

    @pl.when(second)
    def _():
        rows(er1, n1 // 2 - 1, 0).wait_send()
        rows(er1, 2 * n2 - 1, 1).wait_send()

    @pl.when(first_core)
    def _():
        rows(er1, n1 // 2, 0).wait_send()

    for d in directions:
        @pl.when(exists[d])
        def _(d=d):
            bytes_of(leaving[d], d, 0).wait_send()


def hand_out(*refs):
    copies = [pltpu.make_async_copy(refs[n], refs[3 + n], refs[6].at[n]) for n in range(3)]
    for c in copies:
        c.start()
    for c in copies:
        c.wait()


def per_device(nx, ny, group_x, *args):
    args = list(args)
    for m in range(4):
        shape = args[m].shape
        args[m] = args[m].reshape(shape[0], shape[1] * shape[2], shape[3])
    for m in range(4, 12):
        shape = args[m].shape
        args[m] = args[m].reshape(shape[0] * shape[1], shape[2])
    for m in range(13):
        args[m] = pltpu.with_memory_space_constraint(args[m], pltpu.HBM)
    vm, dma = pltpu.VMEM, pltpu.SemaphoreType.DMA
    n1, n2 = group_x * ny, nx // group_x
    scratch = [
        vm((STEPS + 1, 3, 256, 128), F32),
        vm((STEPS + 1, 3, 2, 64, 128), F32),
        vm((4, 256, 128), F32),
        vm((4, 2, 64, 128), F32),
        vm((NCOEF, 256, 128), F32),
        vm((NCOEF, 2, 64, 128), F32),
        vm((18 * 16, 128), F32),
        vm((2, 10 * 8, 128), F32),
        vm((2, 16, 128), F32),
        vm((2, 2, 8, 128), F32),
        vm((STEPS, 2, 4, 16, 128), F32),
        vm((STEPS, 2, 4, 2, 8, 128), F32),
        vm((STEPS, 2, 4, 16, 128), F32),
        vm((STEPS, 2, 4, 2, 8, 128), F32),
        vm((STEPS, 2, 4, 16, 128), F32),
        vm((STEPS, 2, 4, 2, 8, 128), F32),
        vm((2, 2, 16, 128), F32),
        vm((2, 2, 2, 8, 128), F32),
        vm((2, 2, 16, 128), F32),
        vm((2, 2, 2, 8, 128), F32),
        vm((2, 2, 16, 128), F32),
        vm((2, 2, 2, 8, 128), F32),
        vm((STEPS, 8, 128), F32),
        vm((STEPS, 2, 8, 128), F32),
        vm((STEPS, 2, 8, 128), F32),
        vm((STEPS, 8, 128), F32),
        vm((STEPS, 4, 4, 1, 128), F32),
        vm((STEPS, 4, 4, 1, 128), F32),
        vm((STEPS, 4, 4, 1, 128), F32),
        vm((STEPS, 4, 4, 1, 128), F32),
        vm((480, 128), F32),
        vm((2, 16, 16), jnp.int32),
        vm((2, 8, 8, 128), F32),
        vm((2, 8, 128), F32),
        vm((STEPS, 2, 8, 128), F32),
        vm((2, 1, 128), F32),
        vm((max(n1, 2 * n2), 1, 128), F32),
        vm((max(n2, 1), 1, 128), F32),
        dma((7,)),
        dma((8,)),
        dma((34,)),
        dma((2,)),
        dma((2,)),
        pltpu.SemaphoreType.REGULAR((2, 2)),
        pltpu.SemaphoreType.REGULAR((2, 2)),
    ]
    anywhere = pl.BlockSpec(memory_space=pltpu.HBM)
    in_vmem = pl.BlockSpec(memory_space=pltpu.VMEM)
    out_shape = (
        jax.ShapeDtypeStruct((3, 256, 128), F32),
        jax.ShapeDtypeStruct((3, 64, 256), F32),
        jax.ShapeDtypeStruct((2, STEPS), F32),
    )
    results = pl.pallas_call(
        functools.partial(kernel, nx, ny, group_x),
        out_shape=out_shape,
        in_specs=[anywhere] * 13,
        out_specs=(in_vmem, in_vmem, in_vmem),
        scratch_shapes=scratch,
        compiler_params=pltpu.CompilerParams(
            collective_id=0, has_side_effects=True, vmem_limit_bytes=32 << 20
        ),
        name="leapfrog",
    )(*args)
    fine, coarse, energy = pl.pallas_call(
        hand_out,
        out_shape=out_shape,
        in_specs=[in_vmem] * 3,
        out_specs=[anywhere] * 3,
        scratch_shapes=[dma((3,))],
        compiler_params=pltpu.CompilerParams(vmem_limit_bytes=1 << 20),
        name="hand_out",
    )(*results)
    energy = energy.T
    return fine.reshape(3, 16, 16, 128), coarse.reshape(3, 8, 8, 256), energy


def solution(mesh):
    nx, ny = mesh.shape["gx"], mesh.shape["gy"]
    group_x = next(m for m in (4, 2, 1) if nx % m == 0)
    field, cells = P(None, "gx", "gy", None), P("gx", "gy", None)
    return jax.shard_map(
        functools.partial(per_device, nx, ny, group_x),
        mesh=mesh,
        in_specs=(field,) * 4 + (cells,) * 8 + (P(None, "gx", "gy"),),
        out_specs=(field, field, P()),
        check_vma=False,
    )
```

```python
import functools
import math

import jax
import jax.numpy as jnp
from jax import lax
from jax.experimental import pallas as pl
from jax.experimental.pallas import tpu as pltpu
from jax.sharding import PartitionSpec as P

STEPS = 3
DT = 0.15
MESH = pl.DeviceIdType.MESH
F32 = jnp.float32

R = 2
LO, HI = 0, 1
(WIDE, HALF_A, ISV, GB, GZ, DM, CZU, CZD, CXP, CXM, CYU, CYD, C0) = range(13)
NCOEF = 13


def lanes(shape):
    return lax.broadcasted_iota(jnp.int32, shape, len(shape) - 1)


def subs(shape):
    return lax.broadcasted_iota(jnp.int32, shape, len(shape) - 2)


def spread_row(row):
    return jnp.broadcast_to(row, (8, 128))


def roll(x, shift, axis):
    return pltpu.roll(x, shift % x.shape[axis], axis)


class Fine:
    n = 16
    key = "f"

    @staticmethod
    def load(ref, i, r):
        parts = [ref[pl.ds(16 * i + t, 8 * r, stride=2), :].reshape(1, r, 8, 128) for t in (0, 1)]
        return jnp.concatenate(parts, axis=0)

    @staticmethod
    def store(ref, i, r, value):
        for t in (0, 1):
            ref[pl.ds(16 * i + t, 8 * r, stride=2), :] = value[t].reshape(8 * r, 128)

    @staticmethod
    def k_up(x, last=None):
        moved = roll(x, -1, 3)
        edge = x if last is None else last
        return jnp.where(lanes(x.shape) == 127, edge, moved)

    @staticmethod
    def k_down(x, first=None):
        moved = roll(x, 1, 3)
        edge = x if first is None else first
        return jnp.where(lanes(x.shape) == 0, edge, moved)

    @staticmethod
    def edge_scale(shape):
        k = lanes(shape)
        return jnp.where((k == 0) | (k == 127), 1.0, 0.5).astype(F32)

    @staticmethod
    def row_of(ref, i, r):
        return jnp.concatenate(
            [spread_row(ref[pl.ds(i + m, 1), :]).reshape(1, 8, 128) for m in range(r)], axis=0
        )

    @staticmethod
    def j_up(x, halo):
        s = subs(x.shape[1:])
        moved = jnp.where(s == 7, halo, roll(x[0], -1, 1))
        return jnp.stack([x[1], moved])

    @staticmethod
    def j_down(x, halo):
        s = subs(x.shape[1:])
        moved = jnp.where(s == 0, halo, roll(x[1], 1, 1))
        return jnp.stack([moved, x[0]])

    @staticmethod
    def plane(ref, j):
        return jnp.concatenate([ref[pl.ds(j + 128 * h, 8, stride=16), :] for h in (0, 1)], axis=0)

    @staticmethod
    def plane_k_up(x):
        return jnp.where(lanes(x.shape) == 127, x, roll(x, -1, 1))

    @staticmethod
    def plane_k_down(x):
        return jnp.where(lanes(x.shape) == 0, x, roll(x, 1, 1))

    @staticmethod
    def corner_plane(tile_ref, comp):
        row = spread_row(tile_ref[comp])
        return jnp.concatenate([row, row], axis=0)

    @staticmethod
    def corner_row(tile_ref, comp):
        return spread_row(tile_ref[comp]).reshape(1, 8, 128)


class Coarse:
    n = 8
    key = "c"

    @staticmethod
    def load(ref, i, r):
        return ref[:, pl.ds(8 * i, 8 * r), :].reshape(2, r, 8, 128)

    @staticmethod
    def store(ref, i, r, value):
        ref[:, pl.ds(8 * i, 8 * r), :] = value.reshape(2, 8 * r, 128)

    @staticmethod
    def k_up(x, last=None):
        moved = roll(x, -1, 3)
        edge = x[1] if last is None else last
        return jnp.where(lanes(x.shape) == 127, jnp.stack([moved[1], edge]), moved)

    @staticmethod
    def k_down(x, first=None):
        moved = roll(x, 1, 3)
        edge = x[0] if first is None else first
        return jnp.where(lanes(x.shape) == 0, jnp.stack([edge, moved[0]]), moved)

    @staticmethod
    def edge_scale(shape):
        k = lanes(shape)
        half = lax.broadcasted_iota(jnp.int32, shape, 0)
        ends = ((k == 0) & (half == 0)) | ((k == 127) & (half == 1))
        return jnp.where(ends, 1.0, 0.5).astype(F32)

    @staticmethod
    def row_of(ref, i, r):
        halves = []
        for h in (0, 1):
            rows = [spread_row(ref[h, pl.ds(i + m, 1), :]).reshape(1, 8, 128) for m in range(r)]
            halves.append(jnp.concatenate(rows, axis=0))
        return jnp.stack(halves)

    @staticmethod
    def j_up(x, halo):
        return jnp.where(subs(x.shape) == 7, halo, roll(x, -1, 2))

    @staticmethod
    def j_down(x, halo):
        return jnp.where(subs(x.shape) == 0, halo, roll(x, 1, 2))

    @staticmethod
    def plane(ref, j):
        return jnp.stack([ref[h, pl.ds(j, 8, stride=8), :] for h in (0, 1)])

    @staticmethod
    def plane_k_up(x):
        return Coarse.k_up(x[:, None])[:, 0]

    @staticmethod
    def plane_k_down(x):
        return Coarse.k_down(x[:, None])[:, 0]

    @staticmethod
    def corner_plane(tile_ref, comp):
        return jnp.stack([spread_row(tile_ref[2 * comp + h]) for h in (0, 1)])

    @staticmethod
    def corner_row(tile_ref, comp):
        rows = [spread_row(tile_ref[2 * comp + h]) for h in (0, 1)]
        return jnp.stack(rows)[:, None]


def plane_roll(level, x, shift):
    return roll(x, shift, 0) if level is Fine else roll(x, shift, 1)


def plane_sub(level, x):
    return subs(x.shape)


def neighbour_rows(level, ref, i, r, step, halo):
    if step > 0:
        if i + r < level.n:
            return level.load(ref, i + 1, r)
        return halo() if r == 1 else jnp.concatenate([level.load(ref, i + 1, r - 1), halo()], axis=1)
    if i > 0:
        return level.load(ref, i - 1, r)
    return halo() if r == 1 else jnp.concatenate([halo(), level.load(ref, 0, r - 1)], axis=1)


def kernel(nx, ny, group_x, *refs):
    names_in = ["fine_disp", "fine_prev", "coarse_disp", "coarse_prev"]
    for name in ("fine", "coarse"):
        names_in += [name + part for part in ("_density", "_lame", "_rigidity", "_metric")]
    hbm = dict(zip(names_in, refs[:12]))
    offsets_hbm = refs[12]
    fine_out, coarse_out, energy_out = refs[13:16]
    (
        uf, uc, matf, matc, kf, kc, dvf, dvc, dyf, dyc,
        xhf, xhc, yhf, yhc, ysf, ysc, xmf, xmc, ymf, ymc, ysmf, ysmc,
        pls, plx, ply, pex, ccs, ccr, fcs, fcr, sized, offsets_ref, weights, ghost, eacc, erow, er1, er2,
        load_sem, send_sem, recv_sem, esend, erecv, line_sem, plane_sem,
    ) = refs[16:]

    gx, gy = lax.axis_index("gx"), lax.axis_index("gy")
    exists = {
        (dx, dy): functools.reduce(
            jnp.logical_and,
            ([gx > 0] if dx < 0 else [gx < nx - 1] if dx > 0 else [])
            + ([gy > 0] if dy < 0 else [gy < ny - 1] if dy > 0 else []),
        )
        for dx, dy in ((-1, 0), (1, 0), (-1, -1), (-1, 1), (1, -1), (1, 1), (0, -1), (0, 1))
    }
    directions = list(exists)
    corners = [d for d in directions if d[0] and d[1]]
    corner_id = {d: n for n, d in enumerate(corners)}

    def flag(direction):
        return jnp.where(exists[direction], 1.0, 0.0).astype(F32)

    def device(direction):
        return {"gx": gx + direction[0], "gy": gy + direction[1]}

    groups, half = nx // group_x, ny // 2
    gx_hi, gx_lo = gx // group_x, gx % group_x
    chip_y, second = gy // 2, gy % 2 == 1
    first_core = jnp.logical_not(second)
    n1, n2 = group_x * ny, groups
    me1 = gx_lo * ny + gy
    plane_x = [gx_hi * group_x + lax.rem(gx_lo + a, group_x) for a in range(group_x)]
    plane_y = [2 * lax.rem(chip_y + b, half) for b in range(half)]
    line_x = [lax.rem(gx_hi + d, n2) * group_x + gx_lo for d in range(n2)]

    def start_load(name, dst, sem):
        src = hbm[name]
        if name.startswith("fine"):
            pltpu.make_async_copy(src, dst, load_sem.at[sem]).start()
            return
        lead = (slice(None),) * (len(src.shape) - 2)
        for h in (0, 1):
            pltpu.make_async_copy(
                src.at[lead + (slice(None), pl.ds(128 * h, 128))],
                dst.at[(slice(None), h) if lead else (h,)],
                load_sem.at[sem],
            ).start()

    plan = [
        ("fine_disp", uf.at[1], 0), ("coarse_disp", uc.at[1], 1),
        ("fine_rigidity", matf.at[0], 0), ("coarse_rigidity", matc.at[0], 1),
        ("fine_metric", matf.at[1], 0), ("coarse_metric", matc.at[1], 1),
        ("fine_density", matf.at[2], 2), ("fine_lame", matf.at[3], 2),
        ("coarse_density", matc.at[2], 3), ("coarse_lame", matc.at[3], 3),
        ("fine_prev", uf.at[0], 4), ("coarse_prev", uc.at[0], 5),
    ]
    for entry in plan:
        start_load(*entry)
    offsets_load = pltpu.make_async_copy(offsets_hbm, offsets_ref, load_sem.at[6])
    offsets_load.start()
    load_sizes = (kf.at[pl.ds(0, 5)], kc.at[pl.ds(0, 5)], kf.at[pl.ds(0, 2)], kc.at[pl.ds(0, 2)],
                  kf.at[pl.ds(0, 3)], kc.at[pl.ds(0, 3)])

    def wait_load(*sems):
        for sem in sems:
            pltpu.make_async_copy(load_sizes[sem], load_sizes[sem], load_sem.at[sem]).wait()

    barrier = pltpu.get_barrier_semaphore()

    def greet(where):
        pl.semaphore_signal(barrier, inc=1, device_id=where, device_id_type=MESH)

    far_first = sorted(range(1, n2), key=lambda d: -min(d, n2 - d))
    by_one = sorted({1, n2 - 1}) if n2 > 1 else []
    by_two = sorted({2, n2 - 2}) if n2 > 3 else []
    for d in by_one:
        greet({"gx": line_x[d], "gy": 2 * chip_y + 1})
    for d in directions:
        @pl.when(exists[d])
        def _(d=d):
            greet(device(d))

    side_of = {-1: LO, 1: HI}

    def messages(s):
        out = []
        u_f, u_c = uf.at[s + 1], uc.at[s + 1]
        for dx in (-1, 1):
            own, far = side_of[dx], side_of[-dx]
            first, second = (0, 1) if dx < 0 else (15, 14)
            out.append(("fx", (dx, 0), u_f.at[:, pl.ds(16 * first, 16)], xhf.at[s, far, pl.ds(0, 3)]))
            out.append(("fx", (dx, 0), u_f.at[0, pl.ds(16 * second, 16)], xhf.at[s, far, 3]))
            first, second = (0, 1) if dx < 0 else (7, 6)
            out.append(("cx", (dx, 0), u_c.at[:, :, pl.ds(8 * first, 8)], xhc.at[s, far, pl.ds(0, 3)]))
            out.append(("cx", (dx, 0), u_c.at[0, :, pl.ds(8 * second, 8)], xhc.at[s, far, 3]))
            out.append(("cp", (dx, 0), pex.at[s], plx.at[s, far]))
            if s == 0:
                first = 0 if dx < 0 else 15
                out.append(("mfx", (dx, 0), matf.at[pl.ds(0, 2), pl.ds(16 * first, 16)], xmf.at[far]))
                first = 0 if dx < 0 else 7
                out.append(("mcx", (dx, 0), matc.at[pl.ds(0, 2), :, pl.ds(8 * first, 8)], xmc.at[far]))
        for dy in (-1, 1):
            own, far = side_of[dy], side_of[-dy]
            out.append(("fy", (0, dy), ysf.at[s, own], yhf.at[s, far]))
            out.append(("cy", (0, dy), ysc.at[s, own], yhc.at[s, far]))
            out.append(("cq", (0, dy), pls.at[s], ply.at[s, far]))
            if s == 0:
                out.append(("mfy", (0, dy), ysmf.at[own], ymf.at[far]))
                out.append(("mcy", (0, dy), ysmc.at[own], ymc.at[far]))
        for d in corners:
            back = corner_id[(-d[0], -d[1])]
            out.append(("co", d, ccs.at[s, corner_id[d]], ccr.at[s, back]))
            out.append(("fo", d, fcs.at[s, corner_id[d]], fcr.at[s, back]))
        return out

    wait_with = {"mfx": "fx", "mcx": "cx", "cq": "fy", "mfy": "fy", "mcy": "cy"}
    slots, copies, arriving, leaving = {}, [], [], dict.fromkeys(directions, 0)
    for s in range(STEPS):
        entries, rows_of = [], {}
        for group, d, src, dst in messages(s):
            name = wait_with.get(group, group)
            key = (s if name == "cp" else s % 2, name, d)
            slot = slots.setdefault(key, len(slots))
            rows = math.prod(src.shape) // 128
            rows_of[key] = rows_of.get(key, 0) + rows
            leaving[d] += rows

            def copy(src=src, dst=dst, slot=slot, d=d):
                return pltpu.make_async_remote_copy(
                    src_ref=src, dst_ref=dst,
                    send_sem=send_sem.at[directions.index(d)], recv_sem=recv_sem.at[slot],
                    device_id=device(d), device_id_type=MESH,
                )

            entries.append((group, d, copy))
        copies.append(entries)
        arriving.append(rows_of)

    def bytes_of(rows, d, slot):
        part = sized.at[pl.ds(0, rows)]
        return pltpu.make_async_remote_copy(
            src_ref=part, dst_ref=part,
            send_sem=send_sem.at[directions.index(d)], recv_sem=recv_sem.at[slot],
            device_id=device(d), device_id_type=MESH,
        )

    def send(s, *wanted, dx=None):
        for d in directions:
            mine = [c for g, e, c in copies[s] if g in wanted and e == d]
            if mine and dx in (None, d[0]):
                @pl.when(exists[d])
                def _(mine=mine):
                    for c in mine:
                        c().start()

    def receive(s, *wanted, side=None):
        for d in directions:
            mine = [k for k in arriving[s] if k[1] in wanted and k[2] == d]
            if mine and (side is None or d[0] == -side):
                @pl.when(exists[(-d[0], -d[1])])
                def _(mine=mine, d=d):
                    for k in mine:
                        bytes_of(arriving[s][k], d, slots[k]).wait_recv()

    def round_signals(stage):
        away = 2 << stage
        for side, ok, to in ((LO, gy + away < ny, gy + away), (HI, gy >= away, gy - away)):
            if ny > 5:
                @pl.when(ok)
                def _(side=side, to=to):
                    pl.semaphore_signal(
                        plane_sem.at[stage, side], inc=1,
                        device_id={"gx": gx, "gy": to}, device_id_type=MESH,
                    )
        if n2 > 3:
            @pl.when(second)
            def _():
                for m, d in enumerate((by_one, by_two)[stage]):
                    pl.semaphore_signal(
                        line_sem.at[stage, m], inc=1,
                        device_id={"gx": line_x[d], "gy": gy}, device_id_type=MESH,
                    )

    def round_wait(stage):
        away = 2 << stage
        for side, ok in ((LO, gy >= away), (HI, gy + away < ny)):
            if ny > 5:
                @pl.when(ok)
                def _(side=side):
                    pl.semaphore_wait(plane_sem.at[stage, side], 1)
        if n2 > 3:
            @pl.when(second)
            def _():
                for m in range(len((by_one, by_two)[stage])):
                    pl.semaphore_wait(line_sem.at[stage, m], 1)

    def pack_y(level, s):
        u, out = (uf, ysf) if level is Fine else (uc, ysc)
        last = 15 if level is Fine else 7
        for side, (j0, j1) in ((LO, (0, 1)), (HI, (last, last - 1))):
            for c in range(3):
                out[s, side, c] = level.plane(u.at[s + 1, c], j0)
            out[s, side, 3] = level.plane(u.at[s + 1, 1], j1)

    def plane_tile(s, tile, rows):
        lane = lanes((8, 128))
        for c in range(3):
            for i in rows:
                column = uc[s + 1, c, 0, pl.ds(8 * i, 8), 0:1]
                at = 16 * c + 2 * i
                tile = jnp.where((lane == at) | (lane == at + 1), column, tile)
        return tile

    def pack_coarse_corners(s, side):
        for (dx, dy), n in corner_id.items():
            if dx != side:
                continue
            ci, cj = (0 if dx < 0 else 7), (0 if dy < 0 else 7)
            for c in (0, 1):
                for h in (0, 1):
                    ccs[s, n, 2 * c + h] = uc[s + 1, c, h, pl.ds(8 * ci + cj, 1), :]

    def pack_plane(s):
        edge = plane_tile(s, jnp.zeros((8, 128), F32), (0, 1, 7))
        pex[s] = edge
        pls[s] = plane_tile(s, edge, range(2, 7))
        for (dx, dy), n in corner_id.items():
            for m, j in enumerate((0, 1) if dy < 0 else (7, 7)):
                fcs[s, n, 2 + m] = edge[j : j + 1]

    def pack_corners(s, side):
        for (dx, dy), n in corner_id.items():
            if dx != side:
                continue
            fi, fj = (0 if dx < 0 else 15), (0 if dy < 0 else 15)
            for c in (0, 1):
                fcs[s, n, c] = uf[s + 1, c, pl.ds(16 * fi + fj, 1), :]

    for dx in (-1, 1):
        @pl.when(jnp.logical_not(exists[(dx, 0)]))
        def _(side=side_of[dx]):
            for s in range(STEPS):
                xhf[s, side] = jnp.zeros(xhf.shape[2:], F32)
                xhc[s, side] = jnp.zeros(xhc.shape[2:], F32)
                plx[s, side] = jnp.zeros((8, 128), F32)
            xmf[side, 0] = jnp.zeros(xmf.shape[2:], F32)
            xmf[side, 1] = jnp.ones(xmf.shape[2:], F32)
            xmc[side, 0] = jnp.zeros(xmc.shape[2:], F32)
            xmc[side, 1] = jnp.ones(xmc.shape[2:], F32)
    for dy in (-1, 1):
        @pl.when(jnp.logical_not(exists[(0, dy)]))
        def _(side=side_of[dy]):
            for s in range(STEPS):
                yhf[s, side] = jnp.zeros(yhf.shape[2:], F32)
                yhc[s, side] = jnp.zeros(yhc.shape[2:], F32)
                ply[s, side] = jnp.zeros((8, 128), F32)
            ymf[side, 0] = jnp.zeros(ymf.shape[2:], F32)
            ymf[side, 1] = jnp.ones(ymf.shape[2:], F32)
            ymc[side, 0] = jnp.zeros(ymc.shape[2:], F32)
            ymc[side, 1] = jnp.ones(ymc.shape[2:], F32)
    for d in corners:
        @pl.when(jnp.logical_not(exists[d]))
        def _(n=corner_id[d]):
            for s in range(STEPS):
                ccr[s, n] = jnp.zeros(ccr.shape[2:], F32)
                fcr[s, n] = jnp.zeros(fcr.shape[2:], F32)

    wait_load(0, 1)
    for c in (0, 1):
        for side, jf, jc in ((LO, 0, 0), (HI, 15, 7)):
            ysmf[side, c] = Fine.plane(matf.at[c], jf)
            ysmc[side, c] = Coarse.plane(matc.at[c], jc)
    pack_y(Fine, 0)
    pack_y(Coarse, 0)
    for dx in (-1, 1):
        pack_coarse_corners(0, dx)
        pack_corners(0, dx)
    pack_plane(0)

    greeted = jnp.where(second, 2 * len(by_one), 0).astype(jnp.int32)
    for d in directions:
        greeted = greeted + jnp.where(exists[d], 1, 0).astype(jnp.int32)
    pl.semaphore_wait(barrier, greeted)

    def send_first_x():
        send(0, "cx", "mcx")
        send(0, "cp", "fx", "mfx")

    send(0, "co", "fo")

    @pl.when(first_core)
    def _():
        send_first_x()

    send(0, "cy", "mcy", "cq", "fy", "mfy")

    wait_load(2, 3)
    offsets_load.wait()
    lane8 = lanes((8, 128))
    spread = jnp.where(
        (lanes((16, 128)) % 16 == subs((16, 128))) & (lanes((16, 128)) < 48), 1.0, 0.0
    ).astype(F32)
    for t in (0, 1):
        pick = jnp.where(lanes((8, 16)) == 2 * subs((8, 16)) + t, 1.0, 0.0).astype(F32)
        for axis in (0, 1):
            table = offsets_ref[axis].astype(F32)
            turned = lax.dot_general(
                pick, table, (((1,), (1,)), ((), ())), preferred_element_type=F32
            )
            shift = jnp.dot(turned, spread, preferred_element_type=F32)
            if axis == 0:
                near = jnp.where(lane8 % 2 == 0, 0.75, 0.25).astype(F32)
            else:
                near = jnp.full((8, 128), 0.75 if t == 0 else 0.25, F32)
            for m, value in enumerate((-1.0, 0.0, 1.0, 2.0)):
                weights[t, 4 * axis + m] = jnp.where(shift == value, near, 0.0) + jnp.where(
                    shift == value - 1.0, 1.0 - near, 0.0
                )

    levels = (
        (Coarse, uc, matc, kc, dvc, dyc, xhc, yhc, ysc, xmc, ymc),
        (Fine, uf, matf, kf, dvf, dyf, xhf, yhf, ysf, xmf, ymf),
    )
    for level, u, mat, k, dv, dy_, xh, yh, ys, xm, ym in levels:
        for i in range(0, level.n, R):
            rig, met, den, lam = (level.load(mat.at[m], i, R) for m in range(4))
            scale = level.edge_scale(rig.shape)
            inverse = 1.0 / met
            light = DT / den
            a = inverse * light
            vertical = rig * inverse
            b = (lam + rig) * light
            isv = inverse * scale
            half_a = 0.5 * a
            for slot, value in (
                (WIDE, rig * met), (HALF_A, half_a), (ISV, isv), (GB, 0.5 * b), (GZ, b * isv),
                (DM, den * met), (CZU, half_a * (vertical + level.k_up(vertical))),
                (CZD, half_a * (vertical + level.k_down(vertical))),
            ):
                level.store(k.at[slot], i, R, value)

    @pl.when(second)
    def _():
        send_first_x()

    def halo_row(level, ref):
        if level is Fine:
            return Fine.load(ref, 0, 1)
        return Coarse.load(ref, 0, 1)

    def side_coefficients(level, i, r, u, mat, k, dv, dy_, xh, yh, ys, xm, ym):
        w = level.load(k.at[WIDE], i, r)
        ha = level.load(k.at[HALF_A], i, r)

        def outer(side):
            return halo_row(level, xm.at[side, 0]) * halo_row(level, xm.at[side, 1])

        cxp = ha * (w + neighbour_rows(level, k.at[WIDE], i, r, 1, lambda: outer(HI)))
        cxm = ha * (w + neighbour_rows(level, k.at[WIDE], i, r, -1, lambda: outer(LO)))
        up = level.row_of(ym.at[HI, 0], i, r) * level.row_of(ym.at[HI, 1], i, r)
        down = level.row_of(ym.at[LO, 0], i, r) * level.row_of(ym.at[LO, 1], i, r)
        cyu = ha * (w + level.j_up(w, up))
        cyd = ha * (w + level.j_down(w, down))
        total = cxp + cxm + cyu + cyd + level.load(k.at[CZU], i, r) + level.load(k.at[CZD], i, r)
        for slot, value in ((CXP, cxp), (CXM, cxm), (CYU, cyu), (CYD, cyd), (C0, total)):
            level.store(k.at[slot], i, r, value)

    def inner_coefficients(level, *rest):
        for i, r in [(1, 1)] + [(i, R) for i in range(2, level.n - 2, R)] + [(level.n - 2, 1)]:
            side_coefficients(level, i, r, *rest)

    def row_divergence(s, i, r, level, u, mat, k, dv, dy_, xh, yh, ys, xm, ym):
        now = u.at[s + 1]

        def halo(side):
            return lambda: halo_row(level, xh.at[s, side, 0])

        px = neighbour_rows(level, now.at[0], i, r, 1, halo(HI))
        mx = neighbour_rows(level, now.at[0], i, r, -1, halo(LO))
        y = level.load(now.at[1], i, r)
        z = level.load(now.at[2], i, r)
        py = level.j_up(y, level.row_of(yh.at[s, HI, 1], i, r))
        my = level.j_down(y, level.row_of(yh.at[s, LO, 1], i, r))
        isv = level.load(k.at[ISV], i, r)
        value = 0.5 * ((px - mx) + (py - my)) + isv * (level.k_up(z) - level.k_down(z))
        level.store(dv, i + 1, r, value)

    def x_side_divergence(s, dx, level, u, mat, k, dv, dy_, xh, yh, ys, xm, ym):
        cor = fcr if level is Fine else ccr
        now, n = u.at[s + 1], level.n
        side = side_of[dx]
        inside = level.load(now.at[0], 0 if dx < 0 else n - 1, 1)
        beyond = halo_row(level, xh.at[s, side, 3])
        y = halo_row(level, xh.at[s, side, 1])
        z = halo_row(level, xh.at[s, side, 2])
        py = level.j_up(y, level.corner_row(cor.at[s, corner_id[(dx, 1)]], 1))
        my = level.j_down(y, level.corner_row(cor.at[s, corner_id[(dx, -1)]], 1))
        isv = level.edge_scale(z.shape) / halo_row(level, xm.at[side, 1])
        along = (beyond - inside) if dx > 0 else (inside - beyond)
        value = 0.5 * (along + (py - my)) + isv * (level.k_up(z) - level.k_down(z))
        level.store(dv, 0 if dx < 0 else n + 1, 1, value * flag((dx, 0)))

    def y_side_divergence(s, known, level, u, mat, k, dv, dy_, xh, yh, ys, xm, ym):
        cor = fcr if level is Fine else ccr
        n = level.n
        for dy, side in side_of.items():
            x, z, beyond = yh[s, side, 0], yh[s, side, 2], yh[s, side, 3]
            inside = ys[s, side, 1]
            sub = plane_sub(level, x)
            px, mx = plane_roll(level, x, -1), plane_roll(level, x, 1)
            if 1 in known:
                px = jnp.where(sub == n - 1, level.corner_plane(cor.at[s, corner_id[(1, dy)]], 0), px)
            if -1 in known:
                mx = jnp.where(sub == 0, level.corner_plane(cor.at[s, corner_id[(-1, dy)]], 0), mx)
            isv = level.edge_scale(z.shape) / ym[side, 1]
            along = (beyond - inside) if dy > 0 else (inside - beyond)
            value = 0.5 * (along + (px - mx)) + isv * (level.plane_k_up(z) - level.plane_k_down(z))
            dy_[side] = value * flag((0, dy))

    def middle(s, level, *rest):
        n = level.n
        y_side_divergence(s, (), level, *rest)
        row_divergence(s, 1, 1, level, *rest)
        for i in range(2, n - 2, R):
            row_divergence(s, i, R, level, *rest)
        row_divergence(s, n - 2, 1, level, *rest)
        total = jnp.zeros((8, 128), F32)
        for i in range(R, first_outer(level), R):
            total = total + rates(s, i, level, *rest)
        return total

    def first_outer(level):
        return level.n - (4 if level is Fine else 2)

    def outer(s, dx, level, *rest):
        n = level.n
        x_side_divergence(s, dx, level, *rest)
        y_side_divergence(s, (-1,) if dx < 0 else (-1, 1), level, *rest)
        row_divergence(s, 0 if dx < 0 else n - 1, 1, level, *rest)
        return rates(s, 0 if dx < 0 else n - R, level, *rest)

    def fine_ghosts(s, known):
        sub, lane = subs((8, 128)), lanes((8, 128)) % 16

        def shifted_rows(tile, low, high0, high1):
            return [
                jnp.where(sub == 0, low, roll(tile, 1, 0)),
                tile,
                jnp.where(sub == 7, high0, roll(tile, -1, 0)),
                jnp.where(sub == 7, high1, jnp.where(sub == 6, high0, roll(tile, -2, 0))),
            ]

        def row(ref, j):
            return spread_row(ref[pl.ds(j, 1), :])

        def corner_rows(dx):
            low, high = fcr.at[s, corner_id[(dx, -1)]], fcr.at[s, corner_id[(dx, 1)]]
            return spread_row(low[2]), spread_row(high[2]), spread_row(high[3])

        own = shifted_rows(pls[s], row(ply.at[s, LO], 7), row(ply.at[s, HI], 0), row(ply.at[s, HI], 1))
        if -1 in known:
            left = shifted_rows(plx[s, LO], *corner_rows(-1))
        if 1 in known:
            right = shifted_rows(plx[s, HI], *corner_rows(1))
        totals = [jnp.zeros((8, 128), F32) for _ in (0, 1)]
        for mx in range(4):
            inner = [jnp.zeros((8, 128), F32) for _ in (0, 1)]
            for my in range(4):
                tile = roll(own[my], 2 - 2 * mx, 1) if mx != 1 else own[my]
                if mx == 0 and -1 in known:
                    tile = jnp.where(lane < 2, roll(left[my], -14, 1), tile)
                if mx >= 2 and 1 in known:
                    edge = 18 - 2 * mx
                    tile = jnp.where(lane >= edge, roll(right[my], edge, 1), tile)
                for t in (0, 1):
                    inner[t] = inner[t] + weights[t, 4 + my] * tile
            for t in (0, 1):
                totals[t] = totals[t] + weights[t, mx] * inner[t]
        for t in (0, 1):
            ghost[t] = totals[t]

    def fine_last(c, i):
        rows = []
        for t in (0, 1):
            tile = ghost[t]
            rows.append(jnp.stack([roll(tile, 127 - (16 * c + i + m), 1) for m in range(R)]))
        return jnp.stack(rows)

    def coarse_first(s, c, i):
        rows = []
        for m in range(R):
            base = 32 * (i + m)
            parts = [uf[s + 1, c, pl.ds(base + t, 8, stride=2), :] for t in (0, 1, 16, 17)]
            rows.append(0.25 * ((parts[0] + parts[1]) + (parts[2] + parts[3])))
        return roll(jnp.stack(rows), 1, 2)

    def rates(s, i, level, u, mat, k, dv, dy_, xh, yh, ys, xm, ym):
        now, old = u.at[s + 1], u.at[s]
        coef = {
            m: level.load(k.at[m], i, R) for m in (GB, GZ, DM, CZU, CZD, CXP, CXM, CYU, CYD, C0)
        }
        d_mid = level.load(dv, i + 1, R)
        gradient = [
            coef[GB] * (level.load(dv, i + 2, R) - level.load(dv, i, R)),
            coef[GB]
            * (
                level.j_up(d_mid, level.row_of(dy_.at[HI], i, R))
                - level.j_down(d_mid, level.row_of(dy_.at[LO], i, R))
            ),
            coef[GZ] * (level.k_up(d_mid) - level.k_down(d_mid)),
        ]
        energy = None
        for c in range(3):
            v = level.load(now.at[c], i, R)

            def halo(side, c=c):
                return lambda: halo_row(level, xh.at[s, side, c])

            px = neighbour_rows(level, now.at[c], i, R, 1, halo(HI))
            mx = neighbour_rows(level, now.at[c], i, R, -1, halo(LO))
            py = level.j_up(v, level.row_of(yh.at[s, HI, c], i, R))
            my = level.j_down(v, level.row_of(yh.at[s, LO, c], i, R))
            if level is Fine:
                pz, mz = level.k_up(v, fine_last(c, i)), level.k_down(v)
            else:
                pz = level.k_up(v, jnp.zeros_like(v[1]))
                mz = level.k_down(v, coarse_first(s, c, i))
            rate = (
                (coef[CXP] * px + coef[CXM] * mx)
                + (coef[CYU] * py + coef[CYD] * my)
                + (coef[CZU] * pz + coef[CZD] * mz)
                - coef[C0] * v
                + gradient[c]
            )
            after = (2.0 * v - level.load(old.at[c], i, R)) + rate
            if s < STEPS - 1:
                level.store(u.at[s + 2, c], i, R, after)
            elif level is Fine:
                level.store(fine_out.at[c], i, R, after)
            else:
                for h in (0, 1):
                    coarse_out[c, pl.ds(8 * i, 8 * R), pl.ds(128 * h, 128)] = after[h].reshape(
                        8 * R, 128
                    )
            change = after - v
            part = change * change - after * rate
            energy = part if energy is None else energy + part
        return jnp.sum(coef[DM] * energy, axis=(0, 1))

    coarse_set, fine_set = levels
    for s in range(STEPS):
        last = s == STEPS - 1
        receive(s, "cy")
        if s == 0:
            inner_coefficients(*coarse_set)
            wait_load(5)
        coarse_total = middle(s, *coarse_set)
        receive(s, "fy")
        if s == 0:
            inner_coefficients(*fine_set)
            wait_load(4)
        fine_ghosts(s, ())
        fine_total = middle(s, *fine_set)
        for dx in (-1, 1):
            receive(s, "co", "cx", side=dx)
            if s == 0:
                side_coefficients(Coarse, 0 if dx < 0 else 7, 1, *coarse_set[1:])
            coarse_total = coarse_total + outer(s, dx, *coarse_set)
            if not last:
                pack_coarse_corners(s + 1, dx)
                send(s + 1, "co", dx=dx)
                send(s + 1, "cx", dx=dx)
        eacc[s, 1] = coarse_total
        if not last:
            pack_y(Coarse, s + 1)
            pack_plane(s + 1)
            send(s + 1, "cy", "cq", "cp")
        receive(s, "cp", "fo")
        fine_ghosts(s, (-1, 1))
        fine_total = fine_total + rates(s, first_outer(Fine), *fine_set)
        for dx in (-1, 1):
            receive(s, "fx", side=dx)
            if s == 0:
                side_coefficients(Fine, 0 if dx < 0 else 15, 1, *fine_set[1:])
            fine_total = fine_total + outer(s, dx, *fine_set)
            if not last:
                pack_corners(s + 1, dx)
                send(s + 1, "fo", dx=dx)
                send(s + 1, "fx", dx=dx)
        eacc[s, 0] = fine_total
        if not last:
            pack_y(Fine, s + 1)
            send(s + 1, "fy")
        if s == 0:
            round_signals(0)
        elif s == 1:
            round_wait(0)
            round_signals(1)
        else:
            round_wait(1)

    lane1 = lanes((1, 128))
    row = jnp.zeros((1, 128), F32)
    cells = (nx * ny * 16 * 16 * 128, nx * ny * 8 * 8 * 256)
    for s in range(STEPS):
        for m in (0, 1):
            value = jnp.sum(eacc[s, m], axis=0, keepdims=True)
            value = jnp.sum(value, axis=1, keepdims=True)
            row = jnp.where(lane1 == STEPS * m + s, value * (1.0 / cells[m]), row)
    erow[0] = row
    er1[me1] = row

    def rows(buffer, n, stage):
        part = buffer.at[pl.ds(0, n)]
        return pltpu.make_async_remote_copy(
            src_ref=part, dst_ref=part, send_sem=esend.at[stage], recv_sem=erecv.at[stage],
            device_id={"gx": line_x[0], "gy": gy}, device_id_type=MESH,
        )

    def pass_on(stage, slot, where):
        pltpu.make_async_remote_copy(
            src_ref=erow.at[stage], dst_ref=slot, send_sem=esend.at[stage],
            recv_sem=erecv.at[stage], device_id=where, device_id_type=MESH,
        ).start()

    for a in reversed(range(group_x)):
        for b in reversed(range(half)):
            if a or b:
                pass_on(0, er1.at[me1], {"gx": plane_x[a], "gy": plane_y[b] + 1})

    @pl.when(first_core)
    def _():
        pass_on(0, er1.at[me1], {"gx": gx, "gy": 2 * chip_y + 1})

    @pl.when(second)
    def _():
        rows(er1, n1 - 1, 0).wait_recv()
        plane = er1[0]
        for m in range(1, n1):
            plane = plane + er1[m]
        erow[1] = plane
        er2[gx_hi] = plane
        for d in far_first:
            for core in (0, 1):
                pass_on(1, er2.at[gx_hi], {"gx": line_x[d], "gy": 2 * chip_y + core})
        pass_on(1, er2.at[gx_hi], {"gx": gx, "gy": 2 * chip_y})
        if n2 > 1:
            rows(er2, n2 - 1, 1).wait_recv()

    @pl.when(first_core)
    def _():
        rows(er2, n2, 1).wait_recv()

    row = er2[0]
    for m in range(1, n2):
        row = row + er2[m]
    for m in (0, 1):
        energy_out[pl.ds(m, 1), :] = roll(row, -STEPS * m, 1)[:, 0:STEPS]

    @pl.when(second)
    def _():
        rows(er1, n1 // 2 - 1, 0).wait_send()
        rows(er1, 2 * n2 - 1, 1).wait_send()

    @pl.when(first_core)
    def _():
        rows(er1, n1 // 2, 0).wait_send()

    for d in directions:
        @pl.when(exists[d])
        def _(d=d):
            bytes_of(leaving[d], d, 0).wait_send()


def hand_out(*refs):
    copies = [pltpu.make_async_copy(refs[n], refs[3 + n], refs[6].at[n]) for n in range(3)]
    for c in copies:
        c.start()
    for c in copies:
        c.wait()


def per_device(nx, ny, group_x, *args):
    args = list(args)
    for m in range(4):
        shape = args[m].shape
        args[m] = args[m].reshape(shape[0], shape[1] * shape[2], shape[3])
    for m in range(4, 12):
        shape = args[m].shape
        args[m] = args[m].reshape(shape[0] * shape[1], shape[2])
    for m in range(13):
        args[m] = pltpu.with_memory_space_constraint(args[m], pltpu.HBM)
    vm, dma = pltpu.VMEM, pltpu.SemaphoreType.DMA
    n1, n2 = group_x * ny, nx // group_x
    scratch = [
        vm((STEPS + 1, 3, 256, 128), F32),
        vm((STEPS + 1, 3, 2, 64, 128), F32),
        vm((4, 256, 128), F32),
        vm((4, 2, 64, 128), F32),
        vm((NCOEF, 256, 128), F32),
        vm((NCOEF, 2, 64, 128), F32),
        vm((18 * 16, 128), F32),
        vm((2, 10 * 8, 128), F32),
        vm((2, 16, 128), F32),
        vm((2, 2, 8, 128), F32),
        vm((STEPS, 2, 4, 16, 128), F32),
        vm((STEPS, 2, 4, 2, 8, 128), F32),
        vm((STEPS, 2, 4, 16, 128), F32),
        vm((STEPS, 2, 4, 2, 8, 128), F32),
        vm((STEPS, 2, 4, 16, 128), F32),
        vm((STEPS, 2, 4, 2, 8, 128), F32),
        vm((2, 2, 16, 128), F32),
        vm((2, 2, 2, 8, 128), F32),
        vm((2, 2, 16, 128), F32),
        vm((2, 2, 2, 8, 128), F32),
        vm((2, 2, 16, 128), F32),
        vm((2, 2, 2, 8, 128), F32),
        vm((STEPS, 8, 128), F32),
        vm((STEPS, 2, 8, 128), F32),
        vm((STEPS, 2, 8, 128), F32),
        vm((STEPS, 8, 128), F32),
        vm((STEPS, 4, 4, 1, 128), F32),
        vm((STEPS, 4, 4, 1, 128), F32),
        vm((STEPS, 4, 4, 1, 128), F32),
        vm((STEPS, 4, 4, 1, 128), F32),
        vm((480, 128), F32),
        vm((2, 16, 16), jnp.int32),
        vm((2, 8, 8, 128), F32),
        vm((2, 8, 128), F32),
        vm((STEPS, 2, 8, 128), F32),
        vm((2, 1, 128), F32),
        vm((max(n1, 2 * n2), 1, 128), F32),
        vm((max(n2, 1), 1, 128), F32),
        dma((7,)),
        dma((8,)),
        dma((38,)),
        dma((2,)),
        dma((2,)),
        pltpu.SemaphoreType.REGULAR((2, 2)),
        pltpu.SemaphoreType.REGULAR((2, 2)),
    ]
    anywhere = pl.BlockSpec(memory_space=pltpu.HBM)
    in_vmem = pl.BlockSpec(memory_space=pltpu.VMEM)
    out_shape = (
        jax.ShapeDtypeStruct((3, 256, 128), F32),
        jax.ShapeDtypeStruct((3, 64, 256), F32),
        jax.ShapeDtypeStruct((2, STEPS), F32),
    )
    results = pl.pallas_call(
        functools.partial(kernel, nx, ny, group_x),
        out_shape=out_shape,
        in_specs=[anywhere] * 13,
        out_specs=(in_vmem, in_vmem, in_vmem),
        scratch_shapes=scratch,
        compiler_params=pltpu.CompilerParams(
            collective_id=0, has_side_effects=True, vmem_limit_bytes=32 << 20
        ),
        name="leapfrog",
    )(*args)
    fine, coarse, energy = pl.pallas_call(
        hand_out,
        out_shape=out_shape,
        in_specs=[in_vmem] * 3,
        out_specs=[anywhere] * 3,
        scratch_shapes=[dma((3,))],
        compiler_params=pltpu.CompilerParams(vmem_limit_bytes=1 << 20),
        name="hand_out",
    )(*results)
    energy = energy.T
    return fine.reshape(3, 16, 16, 128), coarse.reshape(3, 8, 8, 256), energy


def solution(mesh):
    nx, ny = mesh.shape["gx"], mesh.shape["gy"]
    group_x = next(m for m in (4, 2, 1) if nx % m == 0)
    field, cells = P(None, "gx", "gy", None), P("gx", "gy", None)
    return jax.shard_map(
        functools.partial(per_device, nx, ny, group_x),
        mesh=mesh,
        in_specs=(field,) * 4 + (cells,) * 8 + (P(None, "gx", "gy"),),
        out_specs=(field, field, P()),
        check_vma=False,
    )
```

```python
import functools
import math

import jax
import jax.numpy as jnp
from jax import lax
from jax.experimental import pallas as pl
from jax.experimental.pallas import tpu as pltpu
from jax.sharding import PartitionSpec as P

STEPS = 3
DT = 0.15
MESH = pl.DeviceIdType.MESH
F32 = jnp.float32

R = 2
LO, HI = 0, 1
(WIDE, HALF_A, ISV, GB, GZ, DM, CZU, CZD, CXP, CXM, CYU, CYD, C0) = range(13)
NCOEF = 13


def lanes(shape):
    return lax.broadcasted_iota(jnp.int32, shape, len(shape) - 1)


def subs(shape):
    return lax.broadcasted_iota(jnp.int32, shape, len(shape) - 2)


def spread_row(row):
    return jnp.broadcast_to(row, (8, 128))


def roll(x, shift, axis):
    return pltpu.roll(x, shift % x.shape[axis], axis)


class Fine:
    n = 16
    key = "f"

    @staticmethod
    def load(ref, i, r):
        parts = [ref[pl.ds(16 * i + t, 8 * r, stride=2), :].reshape(1, r, 8, 128) for t in (0, 1)]
        return jnp.concatenate(parts, axis=0)

    @staticmethod
    def store(ref, i, r, value):
        for t in (0, 1):
            ref[pl.ds(16 * i + t, 8 * r, stride=2), :] = value[t].reshape(8 * r, 128)

    @staticmethod
    def k_up(x, last=None):
        moved = roll(x, -1, 3)
        edge = x if last is None else last
        return jnp.where(lanes(x.shape) == 127, edge, moved)

    @staticmethod
    def k_down(x, first=None):
        moved = roll(x, 1, 3)
        edge = x if first is None else first
        return jnp.where(lanes(x.shape) == 0, edge, moved)

    @staticmethod
    def edge_scale(shape):
        k = lanes(shape)
        return jnp.where((k == 0) | (k == 127), 1.0, 0.5).astype(F32)

    @staticmethod
    def row_of(ref, i, r):
        return jnp.concatenate(
            [spread_row(ref[pl.ds(i + m, 1), :]).reshape(1, 8, 128) for m in range(r)], axis=0
        )

    @staticmethod
    def j_up(x, halo):
        s = subs(x.shape[1:])
        moved = jnp.where(s == 7, halo, roll(x[0], -1, 1))
        return jnp.stack([x[1], moved])

    @staticmethod
    def j_down(x, halo):
        s = subs(x.shape[1:])
        moved = jnp.where(s == 0, halo, roll(x[1], 1, 1))
        return jnp.stack([moved, x[0]])

    @staticmethod
    def plane(ref, j):
        return jnp.concatenate([ref[pl.ds(j + 128 * h, 8, stride=16), :] for h in (0, 1)], axis=0)

    @staticmethod
    def plane_k_up(x):
        return jnp.where(lanes(x.shape) == 127, x, roll(x, -1, 1))

    @staticmethod
    def plane_k_down(x):
        return jnp.where(lanes(x.shape) == 0, x, roll(x, 1, 1))

    @staticmethod
    def corner_plane(tile_ref, comp):
        row = spread_row(tile_ref[comp])
        return jnp.concatenate([row, row], axis=0)

    @staticmethod
    def corner_row(tile_ref, comp):
        return spread_row(tile_ref[comp]).reshape(1, 8, 128)


class Coarse:
    n = 8
    key = "c"

    @staticmethod
    def load(ref, i, r):
        return ref[:, pl.ds(8 * i, 8 * r), :].reshape(2, r, 8, 128)

    @staticmethod
    def store(ref, i, r, value):
        ref[:, pl.ds(8 * i, 8 * r), :] = value.reshape(2, 8 * r, 128)

    @staticmethod
    def k_up(x, last=None):
        moved = roll(x, -1, 3)
        edge = x[1] if last is None else last
        return jnp.where(lanes(x.shape) == 127, jnp.stack([moved[1], edge]), moved)

    @staticmethod
    def k_down(x, first=None):
        moved = roll(x, 1, 3)
        edge = x[0] if first is None else first
        return jnp.where(lanes(x.shape) == 0, jnp.stack([edge, moved[0]]), moved)

    @staticmethod
    def edge_scale(shape):
        k = lanes(shape)
        half = lax.broadcasted_iota(jnp.int32, shape, 0)
        ends = ((k == 0) & (half == 0)) | ((k == 127) & (half == 1))
        return jnp.where(ends, 1.0, 0.5).astype(F32)

    @staticmethod
    def row_of(ref, i, r):
        halves = []
        for h in (0, 1):
            rows = [spread_row(ref[h, pl.ds(i + m, 1), :]).reshape(1, 8, 128) for m in range(r)]
            halves.append(jnp.concatenate(rows, axis=0))
        return jnp.stack(halves)

    @staticmethod
    def j_up(x, halo):
        return jnp.where(subs(x.shape) == 7, halo, roll(x, -1, 2))

    @staticmethod
    def j_down(x, halo):
        return jnp.where(subs(x.shape) == 0, halo, roll(x, 1, 2))

    @staticmethod
    def plane(ref, j):
        return jnp.stack([ref[h, pl.ds(j, 8, stride=8), :] for h in (0, 1)])

    @staticmethod
    def plane_k_up(x):
        return Coarse.k_up(x[:, None])[:, 0]

    @staticmethod
    def plane_k_down(x):
        return Coarse.k_down(x[:, None])[:, 0]

    @staticmethod
    def corner_plane(tile_ref, comp):
        return jnp.stack([spread_row(tile_ref[2 * comp + h]) for h in (0, 1)])

    @staticmethod
    def corner_row(tile_ref, comp):
        rows = [spread_row(tile_ref[2 * comp + h]) for h in (0, 1)]
        return jnp.stack(rows)[:, None]


def plane_roll(level, x, shift):
    return roll(x, shift, 0) if level is Fine else roll(x, shift, 1)


def plane_sub(level, x):
    return subs(x.shape)


def neighbour_rows(level, ref, i, r, step, halo):
    if step > 0:
        if i + r < level.n:
            return level.load(ref, i + 1, r)
        return halo() if r == 1 else jnp.concatenate([level.load(ref, i + 1, r - 1), halo()], axis=1)
    if i > 0:
        return level.load(ref, i - 1, r)
    return halo() if r == 1 else jnp.concatenate([halo(), level.load(ref, 0, r - 1)], axis=1)


def kernel(nx, ny, group_x, *refs):
    names_in = ["fine_disp", "fine_prev", "coarse_disp", "coarse_prev"]
    for name in ("fine", "coarse"):
        names_in += [name + part for part in ("_density", "_lame", "_rigidity", "_metric")]
    hbm = dict(zip(names_in, refs[:12]))
    offsets_hbm = refs[12]
    fine_out, coarse_out, energy_out = refs[13:16]
    (
        uf, uc, matf, matc, kf, kc, dvf, dvc, dyf, dyc,
        xhf, xhc, yhf, yhc, ysf, ysc, xmf, xmc, ymf, ymc, ysmf, ysmc,
        pls, plx, ply, pex, ccs, ccr, fcs, fcr, sized, offsets_ref, weights, ghost, eacc, erow, er1, er2,
        load_sem, send_sem, recv_sem, esend, erecv, line_sem, plane_sem,
    ) = refs[16:]

    gx, gy = lax.axis_index("gx"), lax.axis_index("gy")
    exists = {
        (dx, dy): functools.reduce(
            jnp.logical_and,
            ([gx > 0] if dx < 0 else [gx < nx - 1] if dx > 0 else [])
            + ([gy > 0] if dy < 0 else [gy < ny - 1] if dy > 0 else []),
        )
        for dx, dy in ((-1, 0), (1, 0), (-1, -1), (-1, 1), (1, -1), (1, 1), (0, -1), (0, 1))
    }
    directions = list(exists)
    corners = [d for d in directions if d[0] and d[1]]
    corner_id = {d: n for n, d in enumerate(corners)}

    def flag(direction):
        return jnp.where(exists[direction], 1.0, 0.0).astype(F32)

    def device(direction):
        return {"gx": gx + direction[0], "gy": gy + direction[1]}

    groups, half = nx // group_x, ny // 2
    gx_hi, gx_lo = gx // group_x, gx % group_x
    chip_y, second = gy // 2, gy % 2 == 1
    first_core = jnp.logical_not(second)
    n1, n2 = group_x * ny, groups
    me1 = gx_lo * ny + gy
    plane_x = [gx_hi * group_x + lax.rem(gx_lo + a, group_x) for a in range(group_x)]
    plane_y = [2 * lax.rem(chip_y + b, half) for b in range(half)]
    line_x = [lax.rem(gx_hi + d, n2) * group_x + gx_lo for d in range(n2)]

    def start_load(name, dst, sem):
        src = hbm[name]
        if name.startswith("fine"):
            pltpu.make_async_copy(src, dst, load_sem.at[sem]).start()
            return
        lead = (slice(None),) * (len(src.shape) - 2)
        for h in (0, 1):
            pltpu.make_async_copy(
                src.at[lead + (slice(None), pl.ds(128 * h, 128))],
                dst.at[(slice(None), h) if lead else (h,)],
                load_sem.at[sem],
            ).start()

    plan = [
        ("fine_disp", uf.at[1], 0), ("coarse_disp", uc.at[1], 1),
        ("fine_rigidity", matf.at[0], 0), ("coarse_rigidity", matc.at[0], 1),
        ("fine_metric", matf.at[1], 0), ("coarse_metric", matc.at[1], 1),
        ("fine_density", matf.at[2], 2), ("fine_lame", matf.at[3], 2),
        ("coarse_density", matc.at[2], 3), ("coarse_lame", matc.at[3], 3),
        ("fine_prev", uf.at[0], 4), ("coarse_prev", uc.at[0], 5),
    ]
    for entry in plan:
        start_load(*entry)
    offsets_load = pltpu.make_async_copy(offsets_hbm, offsets_ref, load_sem.at[6])
    offsets_load.start()
    load_sizes = (kf.at[pl.ds(0, 5)], kc.at[pl.ds(0, 5)], kf.at[pl.ds(0, 2)], kc.at[pl.ds(0, 2)],
                  kf.at[pl.ds(0, 3)], kc.at[pl.ds(0, 3)])

    def wait_load(*sems):
        for sem in sems:
            pltpu.make_async_copy(load_sizes[sem], load_sizes[sem], load_sem.at[sem]).wait()

    barrier = pltpu.get_barrier_semaphore()

    def greet(where):
        pl.semaphore_signal(barrier, inc=1, device_id=where, device_id_type=MESH)

    far_first = sorted(range(1, n2), key=lambda d: -min(d, n2 - d))
    by_one = sorted({1, n2 - 1}) if n2 > 1 else []
    by_two = sorted({2, n2 - 2}) if n2 > 3 else []
    for d in by_one:
        greet({"gx": line_x[d], "gy": 2 * chip_y + 1})
    for d in directions:
        @pl.when(exists[d])
        def _(d=d):
            greet(device(d))

    side_of = {-1: LO, 1: HI}

    def messages(s):
        out = []
        u_f, u_c = uf.at[s + 1], uc.at[s + 1]
        for dx in (-1, 1):
            own, far = side_of[dx], side_of[-dx]
            first, second = (0, 1) if dx < 0 else (15, 14)
            out.append(("fx", (dx, 0), u_f.at[:, pl.ds(16 * first, 16)], xhf.at[s, far, pl.ds(0, 3)]))
            out.append(("fx", (dx, 0), u_f.at[0, pl.ds(16 * second, 16)], xhf.at[s, far, 3]))
            first, second = (0, 1) if dx < 0 else (7, 6)
            out.append(("cx", (dx, 0), u_c.at[:, :, pl.ds(8 * first, 8)], xhc.at[s, far, pl.ds(0, 3)]))
            out.append(("cx", (dx, 0), u_c.at[0, :, pl.ds(8 * second, 8)], xhc.at[s, far, 3]))
            out.append(("cp", (dx, 0), pex.at[s], plx.at[s, far]))
            if s == 0:
                first = 0 if dx < 0 else 15
                out.append(("mfx", (dx, 0), matf.at[pl.ds(0, 2), pl.ds(16 * first, 16)], xmf.at[far]))
                first = 0 if dx < 0 else 7
                out.append(("mcx", (dx, 0), matc.at[pl.ds(0, 2), :, pl.ds(8 * first, 8)], xmc.at[far]))
        for dy in (-1, 1):
            own, far = side_of[dy], side_of[-dy]
            out.append(("fy", (0, dy), ysf.at[s, own], yhf.at[s, far]))
            out.append(("cy", (0, dy), ysc.at[s, own], yhc.at[s, far]))
            out.append(("cq", (0, dy), pls.at[s], ply.at[s, far]))
            if s == 0:
                out.append(("mfy", (0, dy), ysmf.at[own], ymf.at[far]))
                out.append(("mcy", (0, dy), ysmc.at[own], ymc.at[far]))
        for d in corners:
            back = corner_id[(-d[0], -d[1])]
            out.append(("co", d, ccs.at[s, corner_id[d]], ccr.at[s, back]))
            out.append(("fo", d, fcs.at[s, corner_id[d]], fcr.at[s, back]))
        return out

    wait_with = {"mfx": "fx", "mcx": "cx", "cq": "fy", "mfy": "fy", "mcy": "cy"}
    slots, copies, arriving, leaving = {}, [], [], dict.fromkeys(directions, 0)
    for s in range(STEPS):
        entries, rows_of = [], {}
        for group, d, src, dst in messages(s):
            name = wait_with.get(group, group)
            key = (s if name == "cp" else s % 2, name, d)
            slot = slots.setdefault(key, len(slots))
            rows = math.prod(src.shape) // 128
            rows_of[key] = rows_of.get(key, 0) + rows
            leaving[d] += rows

            def copy(src=src, dst=dst, slot=slot, d=d):
                return pltpu.make_async_remote_copy(
                    src_ref=src, dst_ref=dst,
                    send_sem=send_sem.at[directions.index(d)], recv_sem=recv_sem.at[slot],
                    device_id=device(d), device_id_type=MESH,
                )

            entries.append((group, d, copy))
        copies.append(entries)
        arriving.append(rows_of)

    def bytes_of(rows, d, slot):
        part = sized.at[pl.ds(0, rows)]
        return pltpu.make_async_remote_copy(
            src_ref=part, dst_ref=part,
            send_sem=send_sem.at[directions.index(d)], recv_sem=recv_sem.at[slot],
            device_id=device(d), device_id_type=MESH,
        )

    def send(s, *wanted, dx=None):
        for d in directions:
            mine = [c for g, e, c in copies[s] if g in wanted and e == d]
            if mine and dx in (None, d[0]):
                @pl.when(exists[d])
                def _(mine=mine):
                    for c in mine:
                        c().start()

    def receive(s, *wanted, side=None):
        for d in directions:
            mine = [k for k in arriving[s] if k[1] in wanted and k[2] == d]
            if mine and (side is None or d[0] == -side):
                @pl.when(exists[(-d[0], -d[1])])
                def _(mine=mine, d=d):
                    for k in mine:
                        bytes_of(arriving[s][k], d, slots[k]).wait_recv()

    def round_signals(stage):
        away = 2 << stage
        for side, ok, to in ((LO, gy + away < ny, gy + away), (HI, gy >= away, gy - away)):
            if ny > 5:
                @pl.when(ok)
                def _(side=side, to=to):
                    pl.semaphore_signal(
                        plane_sem.at[stage, side], inc=1,
                        device_id={"gx": gx, "gy": to}, device_id_type=MESH,
                    )
        if n2 > 3:
            @pl.when(second)
            def _():
                for m, d in enumerate((by_one, by_two)[stage]):
                    pl.semaphore_signal(
                        line_sem.at[stage, m], inc=1,
                        device_id={"gx": line_x[d], "gy": gy}, device_id_type=MESH,
                    )

    def round_wait(stage):
        away = 2 << stage
        for side, ok in ((LO, gy >= away), (HI, gy + away < ny)):
            if ny > 5:
                @pl.when(ok)
                def _(side=side):
                    pl.semaphore_wait(plane_sem.at[stage, side], 1)
        if n2 > 3:
            @pl.when(second)
            def _():
                for m in range(len((by_one, by_two)[stage])):
                    pl.semaphore_wait(line_sem.at[stage, m], 1)

    def pack_y(level, s):
        u, out = (uf, ysf) if level is Fine else (uc, ysc)
        last = 15 if level is Fine else 7
        for side, (j0, j1) in ((LO, (0, 1)), (HI, (last, last - 1))):
            for c in range(3):
                out[s, side, c] = level.plane(u.at[s + 1, c], j0)
            out[s, side, 3] = level.plane(u.at[s + 1, 1], j1)

    def plane_tile(s, tile, rows):
        lane = lanes((8, 128))
        for c in range(3):
            for i in rows:
                column = uc[s + 1, c, 0, pl.ds(8 * i, 8), 0:1]
                at = 16 * c + 2 * i
                tile = jnp.where((lane == at) | (lane == at + 1), column, tile)
        return tile

    def pack_coarse_corners(s, side):
        for (dx, dy), n in corner_id.items():
            if dx != side:
                continue
            ci, cj = (0 if dx < 0 else 7), (0 if dy < 0 else 7)
            for c in (0, 1):
                for h in (0, 1):
                    ccs[s, n, 2 * c + h] = uc[s + 1, c, h, pl.ds(8 * ci + cj, 1), :]

    def pack_plane(s):
        edge = plane_tile(s, jnp.zeros((8, 128), F32), (0, 1, 7))
        pex[s] = edge
        pls[s] = plane_tile(s, edge, range(2, 7))
        for (dx, dy), n in corner_id.items():
            for m, j in enumerate((0, 1) if dy < 0 else (7, 7)):
                fcs[s, n, 2 + m] = edge[j : j + 1]

    def pack_corners(s, side):
        for (dx, dy), n in corner_id.items():
            if dx != side:
                continue
            fi, fj = (0 if dx < 0 else 15), (0 if dy < 0 else 15)
            for c in (0, 1):
                fcs[s, n, c] = uf[s + 1, c, pl.ds(16 * fi + fj, 1), :]

    for dx in (-1, 1):
        @pl.when(jnp.logical_not(exists[(dx, 0)]))
        def _(side=side_of[dx]):
            for s in range(STEPS):
                xhf[s, side] = jnp.zeros(xhf.shape[2:], F32)
                xhc[s, side] = jnp.zeros(xhc.shape[2:], F32)
                plx[s, side] = jnp.zeros((8, 128), F32)
            xmf[side, 0] = jnp.zeros(xmf.shape[2:], F32)
            xmf[side, 1] = jnp.ones(xmf.shape[2:], F32)
            xmc[side, 0] = jnp.zeros(xmc.shape[2:], F32)
            xmc[side, 1] = jnp.ones(xmc.shape[2:], F32)
    for dy in (-1, 1):
        @pl.when(jnp.logical_not(exists[(0, dy)]))
        def _(side=side_of[dy]):
            for s in range(STEPS):
                yhf[s, side] = jnp.zeros(yhf.shape[2:], F32)
                yhc[s, side] = jnp.zeros(yhc.shape[2:], F32)
                ply[s, side] = jnp.zeros((8, 128), F32)
            ymf[side, 0] = jnp.zeros(ymf.shape[2:], F32)
            ymf[side, 1] = jnp.ones(ymf.shape[2:], F32)
            ymc[side, 0] = jnp.zeros(ymc.shape[2:], F32)
            ymc[side, 1] = jnp.ones(ymc.shape[2:], F32)
    for d in corners:
        @pl.when(jnp.logical_not(exists[d]))
        def _(n=corner_id[d]):
            for s in range(STEPS):
                ccr[s, n] = jnp.zeros(ccr.shape[2:], F32)
                fcr[s, n] = jnp.zeros(fcr.shape[2:], F32)

    wait_load(0, 1)
    for c in (0, 1):
        for side, jf, jc in ((LO, 0, 0), (HI, 15, 7)):
            ysmf[side, c] = Fine.plane(matf.at[c], jf)
            ysmc[side, c] = Coarse.plane(matc.at[c], jc)
    pack_y(Fine, 0)
    pack_y(Coarse, 0)
    for dx in (-1, 1):
        pack_coarse_corners(0, dx)
        pack_corners(0, dx)
    pack_plane(0)

    greeted = jnp.where(second, 2 * len(by_one), 0).astype(jnp.int32)
    for d in directions:
        greeted = greeted + jnp.where(exists[d], 1, 0).astype(jnp.int32)
    pl.semaphore_wait(barrier, greeted)

    def send_first_x():
        send(0, "cx", "mcx")
        send(0, "cp", "fx", "mfx")

    send(0, "co", "fo")

    @pl.when(first_core)
    def _():
        send_first_x()

    send(0, "cy", "mcy", "cq", "fy", "mfy")

    wait_load(2, 3)
    offsets_load.wait()
    lane8 = lanes((8, 128))
    spread = jnp.where(
        (lanes((16, 128)) % 16 == subs((16, 128))) & (lanes((16, 128)) < 48), 1.0, 0.0
    ).astype(F32)
    for t in (0, 1):
        pick = jnp.where(lanes((8, 16)) == 2 * subs((8, 16)) + t, 1.0, 0.0).astype(F32)
        for axis in (0, 1):
            table = offsets_ref[axis].astype(F32)
            turned = lax.dot_general(
                pick, table, (((1,), (1,)), ((), ())), preferred_element_type=F32
            )
            shift = jnp.dot(turned, spread, preferred_element_type=F32)
            if axis == 0:
                near = jnp.where(lane8 % 2 == 0, 0.75, 0.25).astype(F32)
            else:
                near = jnp.full((8, 128), 0.75 if t == 0 else 0.25, F32)
            for m, value in enumerate((-1.0, 0.0, 1.0, 2.0)):
                weights[t, 4 * axis + m] = jnp.where(shift == value, near, 0.0) + jnp.where(
                    shift == value - 1.0, 1.0 - near, 0.0
                )

    levels = (
        (Coarse, uc, matc, kc, dvc, dyc, xhc, yhc, ysc, xmc, ymc),
        (Fine, uf, matf, kf, dvf, dyf, xhf, yhf, ysf, xmf, ymf),
    )
    for level, u, mat, k, dv, dy_, xh, yh, ys, xm, ym in levels:
        for i in range(0, level.n, R):
            rig, met, den, lam = (level.load(mat.at[m], i, R) for m in range(4))
            scale = level.edge_scale(rig.shape)
            inverse = 1.0 / met
            light = DT / den
            a = inverse * light
            vertical = rig * inverse
            b = (lam + rig) * light
            isv = inverse * scale
            half_a = 0.5 * a
            for slot, value in (
                (WIDE, rig * met), (HALF_A, half_a), (ISV, isv), (GB, 0.5 * b), (GZ, b * isv),
                (DM, den * met), (CZU, half_a * (vertical + level.k_up(vertical))),
                (CZD, half_a * (vertical + level.k_down(vertical))),
            ):
                level.store(k.at[slot], i, R, value)

    @pl.when(second)
    def _():
        send_first_x()

    def halo_row(level, ref):
        if level is Fine:
            return Fine.load(ref, 0, 1)
        return Coarse.load(ref, 0, 1)

    def side_coefficients(level, i, r, u, mat, k, dv, dy_, xh, yh, ys, xm, ym):
        w = level.load(k.at[WIDE], i, r)
        ha = level.load(k.at[HALF_A], i, r)

        def outer(side):
            return halo_row(level, xm.at[side, 0]) * halo_row(level, xm.at[side, 1])

        cxp = ha * (w + neighbour_rows(level, k.at[WIDE], i, r, 1, lambda: outer(HI)))
        cxm = ha * (w + neighbour_rows(level, k.at[WIDE], i, r, -1, lambda: outer(LO)))
        up = level.row_of(ym.at[HI, 0], i, r) * level.row_of(ym.at[HI, 1], i, r)
        down = level.row_of(ym.at[LO, 0], i, r) * level.row_of(ym.at[LO, 1], i, r)
        cyu = ha * (w + level.j_up(w, up))
        cyd = ha * (w + level.j_down(w, down))
        total = cxp + cxm + cyu + cyd + level.load(k.at[CZU], i, r) + level.load(k.at[CZD], i, r)
        for slot, value in ((CXP, cxp), (CXM, cxm), (CYU, cyu), (CYD, cyd), (C0, total)):
            level.store(k.at[slot], i, r, value)

    def inner_coefficients(level, *rest):
        for i, r in [(1, 1)] + [(i, R) for i in range(2, level.n - 2, R)] + [(level.n - 2, 1)]:
            side_coefficients(level, i, r, *rest)

    def row_divergence(s, i, r, level, u, mat, k, dv, dy_, xh, yh, ys, xm, ym):
        now = u.at[s + 1]

        def halo(side):
            return lambda: halo_row(level, xh.at[s, side, 0])

        px = neighbour_rows(level, now.at[0], i, r, 1, halo(HI))
        mx = neighbour_rows(level, now.at[0], i, r, -1, halo(LO))
        y = level.load(now.at[1], i, r)
        z = level.load(now.at[2], i, r)
        py = level.j_up(y, level.row_of(yh.at[s, HI, 1], i, r))
        my = level.j_down(y, level.row_of(yh.at[s, LO, 1], i, r))
        isv = level.load(k.at[ISV], i, r)
        value = 0.5 * ((px - mx) + (py - my)) + isv * (level.k_up(z) - level.k_down(z))
        level.store(dv, i + 1, r, value)

    def x_side_divergence(s, dx, level, u, mat, k, dv, dy_, xh, yh, ys, xm, ym):
        cor = fcr if level is Fine else ccr
        now, n = u.at[s + 1], level.n
        side = side_of[dx]
        inside = level.load(now.at[0], 0 if dx < 0 else n - 1, 1)
        beyond = halo_row(level, xh.at[s, side, 3])
        y = halo_row(level, xh.at[s, side, 1])
        z = halo_row(level, xh.at[s, side, 2])
        py = level.j_up(y, level.corner_row(cor.at[s, corner_id[(dx, 1)]], 1))
        my = level.j_down(y, level.corner_row(cor.at[s, corner_id[(dx, -1)]], 1))
        isv = level.edge_scale(z.shape) / halo_row(level, xm.at[side, 1])
        along = (beyond - inside) if dx > 0 else (inside - beyond)
        value = 0.5 * (along + (py - my)) + isv * (level.k_up(z) - level.k_down(z))
        level.store(dv, 0 if dx < 0 else n + 1, 1, value * flag((dx, 0)))

    def y_side_divergence(s, known, level, u, mat, k, dv, dy_, xh, yh, ys, xm, ym):
        cor = fcr if level is Fine else ccr
        n = level.n
        for dy, side in side_of.items():
            x, z, beyond = yh[s, side, 0], yh[s, side, 2], yh[s, side, 3]
            inside = ys[s, side, 1]
            sub = plane_sub(level, x)
            px, mx = plane_roll(level, x, -1), plane_roll(level, x, 1)
            if 1 in known:
                px = jnp.where(sub == n - 1, level.corner_plane(cor.at[s, corner_id[(1, dy)]], 0), px)
            if -1 in known:
                mx = jnp.where(sub == 0, level.corner_plane(cor.at[s, corner_id[(-1, dy)]], 0), mx)
            isv = level.edge_scale(z.shape) / ym[side, 1]
            along = (beyond - inside) if dy > 0 else (inside - beyond)
            value = 0.5 * (along + (px - mx)) + isv * (level.plane_k_up(z) - level.plane_k_down(z))
            dy_[side] = value * flag((0, dy))

    def middle(s, level, *rest):
        n = level.n
        y_side_divergence(s, (), level, *rest)
        row_divergence(s, 1, 1, level, *rest)
        for i in range(2, n - 2, R):
            row_divergence(s, i, R, level, *rest)
        row_divergence(s, n - 2, 1, level, *rest)
        total = jnp.zeros((8, 128), F32)
        for i in range(R, first_outer(level), R):
            total = total + rates(s, i, level, *rest)
        return total

    def first_outer(level):
        return level.n - (4 if level is Fine else 2)

    def outer(s, dx, level, *rest):
        n = level.n
        x_side_divergence(s, dx, level, *rest)
        row_divergence(s, 0 if dx < 0 else n - 1, 1, level, *rest)
        return rates(s, 0 if dx < 0 else n - R, level, *rest)

    def fine_ghosts(s, known):
        sub, lane = subs((8, 128)), lanes((8, 128)) % 16

        def shifted_rows(tile, low, high0, high1):
            return [
                jnp.where(sub == 0, low, roll(tile, 1, 0)),
                tile,
                jnp.where(sub == 7, high0, roll(tile, -1, 0)),
                jnp.where(sub == 7, high1, jnp.where(sub == 6, high0, roll(tile, -2, 0))),
            ]

        def row(ref, j):
            return spread_row(ref[pl.ds(j, 1), :])

        def corner_rows(dx):
            low, high = fcr.at[s, corner_id[(dx, -1)]], fcr.at[s, corner_id[(dx, 1)]]
            return spread_row(low[2]), spread_row(high[2]), spread_row(high[3])

        own = shifted_rows(pls[s], row(ply.at[s, LO], 7), row(ply.at[s, HI], 0), row(ply.at[s, HI], 1))
        if -1 in known:
            left = shifted_rows(plx[s, LO], *corner_rows(-1))
        if 1 in known:
            right = shifted_rows(plx[s, HI], *corner_rows(1))
        totals = [jnp.zeros((8, 128), F32) for _ in (0, 1)]
        for mx in range(4):
            inner = [jnp.zeros((8, 128), F32) for _ in (0, 1)]
            for my in range(4):
                tile = roll(own[my], 2 - 2 * mx, 1) if mx != 1 else own[my]
                if mx == 0 and -1 in known:
                    tile = jnp.where(lane < 2, roll(left[my], -14, 1), tile)
                if mx >= 2 and 1 in known:
                    edge = 18 - 2 * mx
                    tile = jnp.where(lane >= edge, roll(right[my], edge, 1), tile)
                for t in (0, 1):
                    inner[t] = inner[t] + weights[t, 4 + my] * tile
            for t in (0, 1):
                totals[t] = totals[t] + weights[t, mx] * inner[t]
        for t in (0, 1):
            ghost[t] = totals[t]

    def fine_last(c, i):
        rows = []
        for t in (0, 1):
            tile = ghost[t]
            rows.append(jnp.stack([roll(tile, 127 - (16 * c + i + m), 1) for m in range(R)]))
        return jnp.stack(rows)

    def coarse_first(s, c, i):
        rows = []
        for m in range(R):
            base = 32 * (i + m)
            parts = [uf[s + 1, c, pl.ds(base + t, 8, stride=2), :] for t in (0, 1, 16, 17)]
            rows.append(0.25 * ((parts[0] + parts[1]) + (parts[2] + parts[3])))
        return roll(jnp.stack(rows), 1, 2)

    def rates(s, i, level, u, mat, k, dv, dy_, xh, yh, ys, xm, ym):
        now, old = u.at[s + 1], u.at[s]
        coef = {
            m: level.load(k.at[m], i, R) for m in (GB, GZ, DM, CZU, CZD, CXP, CXM, CYU, CYD, C0)
        }
        d_mid = level.load(dv, i + 1, R)
        gradient = [
            coef[GB] * (level.load(dv, i + 2, R) - level.load(dv, i, R)),
            coef[GB]
            * (
                level.j_up(d_mid, level.row_of(dy_.at[HI], i, R))
                - level.j_down(d_mid, level.row_of(dy_.at[LO], i, R))
            ),
            coef[GZ] * (level.k_up(d_mid) - level.k_down(d_mid)),
        ]
        energy = None
        for c in range(3):
            v = level.load(now.at[c], i, R)

            def halo(side, c=c):
                return lambda: halo_row(level, xh.at[s, side, c])

            px = neighbour_rows(level, now.at[c], i, R, 1, halo(HI))
            mx = neighbour_rows(level, now.at[c], i, R, -1, halo(LO))
            py = level.j_up(v, level.row_of(yh.at[s, HI, c], i, R))
            my = level.j_down(v, level.row_of(yh.at[s, LO, c], i, R))
            if level is Fine:
                pz, mz = level.k_up(v, fine_last(c, i)), level.k_down(v)
            else:
                pz = level.k_up(v, jnp.zeros_like(v[1]))
                mz = level.k_down(v, coarse_first(s, c, i))
            rate = (
                (coef[CXP] * px + coef[CXM] * mx)
                + (coef[CYU] * py + coef[CYD] * my)
                + (coef[CZU] * pz + coef[CZD] * mz)
                - coef[C0] * v
                + gradient[c]
            )
            after = (2.0 * v - level.load(old.at[c], i, R)) + rate
            if s < STEPS - 1:
                level.store(u.at[s + 2, c], i, R, after)
            elif level is Fine:
                level.store(fine_out.at[c], i, R, after)
            else:
                for h in (0, 1):
                    coarse_out[c, pl.ds(8 * i, 8 * R), pl.ds(128 * h, 128)] = after[h].reshape(
                        8 * R, 128
                    )
            change = after - v
            part = change * change - after * rate
            energy = part if energy is None else energy + part
        return jnp.sum(coef[DM] * energy, axis=(0, 1))

    coarse_set, fine_set = levels
    for s in range(STEPS):
        last = s == STEPS - 1
        receive(s, "cy")
        if s == 0:
            inner_coefficients(*coarse_set)
            wait_load(5)
        coarse_total = middle(s, *coarse_set)
        receive(s, "fy")
        if s == 0:
            inner_coefficients(*fine_set)
            wait_load(4)
        fine_ghosts(s, ())
        fine_total = middle(s, *fine_set)
        receive(s, "co")
        y_side_divergence(s, (-1, 1), *coarse_set)
        for dx in (-1, 1):
            receive(s, "cx", side=dx)
            if s == 0:
                side_coefficients(Coarse, 0 if dx < 0 else 7, 1, *coarse_set[1:])
            coarse_total = coarse_total + outer(s, dx, *coarse_set)
            if not last:
                pack_coarse_corners(s + 1, dx)
                send(s + 1, "co", dx=dx)
                send(s + 1, "cx", dx=dx)
        eacc[s, 1] = coarse_total
        if not last:
            pack_y(Coarse, s + 1)
            pack_plane(s + 1)
            send(s + 1, "cy", "cq", "cp")
        receive(s, "cp", "fo")
        fine_ghosts(s, (-1, 1))
        y_side_divergence(s, (-1, 1), *fine_set)
        fine_total = fine_total + rates(s, first_outer(Fine), *fine_set)
        for dx in (1, -1) if last else (-1, 1):
            receive(s, "fx", side=dx)
            if s == 0:
                side_coefficients(Fine, 0 if dx < 0 else 15, 1, *fine_set[1:])
            fine_total = fine_total + outer(s, dx, *fine_set)
            if not last:
                pack_corners(s + 1, dx)
                send(s + 1, "fo", dx=dx)
                send(s + 1, "fx", dx=dx)
        eacc[s, 0] = fine_total
        if not last:
            pack_y(Fine, s + 1)
            send(s + 1, "fy")
        if s == 0:
            round_signals(0)
        elif s == 1:
            round_wait(0)
            round_signals(1)
        else:
            round_wait(1)

    lane1 = lanes((1, 128))
    row = jnp.zeros((1, 128), F32)
    cells = (nx * ny * 16 * 16 * 128, nx * ny * 8 * 8 * 256)
    for s in range(STEPS):
        for m in (0, 1):
            value = jnp.sum(eacc[s, m], axis=0, keepdims=True)
            value = jnp.sum(value, axis=1, keepdims=True)
            row = jnp.where(lane1 == STEPS * m + s, value * (1.0 / cells[m]), row)
    erow[0] = row
    er1[me1] = row

    def rows(buffer, n, stage):
        part = buffer.at[pl.ds(0, n)]
        return pltpu.make_async_remote_copy(
            src_ref=part, dst_ref=part, send_sem=esend.at[stage], recv_sem=erecv.at[stage],
            device_id={"gx": line_x[0], "gy": gy}, device_id_type=MESH,
        )

    def pass_on(stage, slot, where):
        pltpu.make_async_remote_copy(
            src_ref=erow.at[stage], dst_ref=slot, send_sem=esend.at[stage],
            recv_sem=erecv.at[stage], device_id=where, device_id_type=MESH,
        ).start()

    for a in reversed(range(group_x)):
        for b in reversed(range(half)):
            if a or b:
                pass_on(0, er1.at[me1], {"gx": plane_x[a], "gy": plane_y[b] + 1})

    @pl.when(first_core)
    def _():
        pass_on(0, er1.at[me1], {"gx": gx, "gy": 2 * chip_y + 1})

    @pl.when(second)
    def _():
        rows(er1, n1 - 1, 0).wait_recv()
        plane = er1[0]
        for m in range(1, n1):
            plane = plane + er1[m]
        erow[1] = plane
        er2[gx_hi] = plane
        for d in far_first:
            for core in (0, 1):
                pass_on(1, er2.at[gx_hi], {"gx": line_x[d], "gy": 2 * chip_y + core})
        pass_on(1, er2.at[gx_hi], {"gx": gx, "gy": 2 * chip_y})
        if n2 > 1:
            rows(er2, n2 - 1, 1).wait_recv()

    @pl.when(first_core)
    def _():
        rows(er2, n2, 1).wait_recv()

    row = er2[0]
    for m in range(1, n2):
        row = row + er2[m]
    for m in (0, 1):
        energy_out[pl.ds(m, 1), :] = roll(row, -STEPS * m, 1)[:, 0:STEPS]

    @pl.when(second)
    def _():
        rows(er1, n1 // 2 - 1, 0).wait_send()
        rows(er1, 2 * n2 - 1, 1).wait_send()

    @pl.when(first_core)
    def _():
        rows(er1, n1 // 2, 0).wait_send()

    for d in directions:
        @pl.when(exists[d])
        def _(d=d):
            bytes_of(leaving[d], d, 0).wait_send()


def hand_out(*refs):
    copies = [pltpu.make_async_copy(refs[n], refs[3 + n], refs[6].at[n]) for n in range(3)]
    for c in copies:
        c.start()
    for c in copies:
        c.wait()


def per_device(nx, ny, group_x, *args):
    args = list(args)
    for m in range(4):
        shape = args[m].shape
        args[m] = args[m].reshape(shape[0], shape[1] * shape[2], shape[3])
    for m in range(4, 12):
        shape = args[m].shape
        args[m] = args[m].reshape(shape[0] * shape[1], shape[2])
    for m in range(13):
        args[m] = pltpu.with_memory_space_constraint(args[m], pltpu.HBM)
    vm, dma = pltpu.VMEM, pltpu.SemaphoreType.DMA
    n1, n2 = group_x * ny, nx // group_x
    scratch = [
        vm((STEPS + 1, 3, 256, 128), F32),
        vm((STEPS + 1, 3, 2, 64, 128), F32),
        vm((4, 256, 128), F32),
        vm((4, 2, 64, 128), F32),
        vm((NCOEF, 256, 128), F32),
        vm((NCOEF, 2, 64, 128), F32),
        vm((18 * 16, 128), F32),
        vm((2, 10 * 8, 128), F32),
        vm((2, 16, 128), F32),
        vm((2, 2, 8, 128), F32),
        vm((STEPS, 2, 4, 16, 128), F32),
        vm((STEPS, 2, 4, 2, 8, 128), F32),
        vm((STEPS, 2, 4, 16, 128), F32),
        vm((STEPS, 2, 4, 2, 8, 128), F32),
        vm((STEPS, 2, 4, 16, 128), F32),
        vm((STEPS, 2, 4, 2, 8, 128), F32),
        vm((2, 2, 16, 128), F32),
        vm((2, 2, 2, 8, 128), F32),
        vm((2, 2, 16, 128), F32),
        vm((2, 2, 2, 8, 128), F32),
        vm((2, 2, 16, 128), F32),
        vm((2, 2, 2, 8, 128), F32),
        vm((STEPS, 8, 128), F32),
        vm((STEPS, 2, 8, 128), F32),
        vm((STEPS, 2, 8, 128), F32),
        vm((STEPS, 8, 128), F32),
        vm((STEPS, 4, 4, 1, 128), F32),
        vm((STEPS, 4, 4, 1, 128), F32),
        vm((STEPS, 4, 4, 1, 128), F32),
        vm((STEPS, 4, 4, 1, 128), F32),
        vm((480, 128), F32),
        vm((2, 16, 16), jnp.int32),
        vm((2, 8, 8, 128), F32),
        vm((2, 8, 128), F32),
        vm((STEPS, 2, 8, 128), F32),
        vm((2, 1, 128), F32),
        vm((max(n1, 2 * n2), 1, 128), F32),
        vm((max(n2, 1), 1, 128), F32),
        dma((7,)),
        dma((8,)),
        dma((38,)),
        dma((2,)),
        dma((2,)),
        pltpu.SemaphoreType.REGULAR((2, 2)),
        pltpu.SemaphoreType.REGULAR((2, 2)),
    ]
    anywhere = pl.BlockSpec(memory_space=pltpu.HBM)
    in_vmem = pl.BlockSpec(memory_space=pltpu.VMEM)
    out_shape = (
        jax.ShapeDtypeStruct((3, 256, 128), F32),
        jax.ShapeDtypeStruct((3, 64, 256), F32),
        jax.ShapeDtypeStruct((2, STEPS), F32),
    )
    results = pl.pallas_call(
        functools.partial(kernel, nx, ny, group_x),
        out_shape=out_shape,
        in_specs=[anywhere] * 13,
        out_specs=(in_vmem, in_vmem, in_vmem),
        scratch_shapes=scratch,
        compiler_params=pltpu.CompilerParams(
            collective_id=0, has_side_effects=True, vmem_limit_bytes=32 << 20
        ),
        name="leapfrog",
    )(*args)
    fine, coarse, energy = pl.pallas_call(
        hand_out,
        out_shape=out_shape,
        in_specs=[in_vmem] * 3,
        out_specs=[anywhere] * 3,
        scratch_shapes=[dma((3,))],
        compiler_params=pltpu.CompilerParams(vmem_limit_bytes=1 << 20),
        name="hand_out",
    )(*results)
    energy = energy.T
    return fine.reshape(3, 16, 16, 128), coarse.reshape(3, 8, 8, 256), energy


def solution(mesh):
    nx, ny = mesh.shape["gx"], mesh.shape["gy"]
    group_x = next(m for m in (4, 2, 1) if nx % m == 0)
    field, cells = P(None, "gx", "gy", None), P("gx", "gy", None)
    return jax.shard_map(
        functools.partial(per_device, nx, ny, group_x),
        mesh=mesh,
        in_specs=(field,) * 4 + (cells,) * 8 + (P(None, "gx", "gy"),),
        out_specs=(field, field, P()),
        check_vma=False,
    )
```

```python
import functools
import math

import jax
import jax.numpy as jnp
from jax import lax
from jax.experimental import pallas as pl
from jax.experimental.pallas import tpu as pltpu
from jax.sharding import PartitionSpec as P

STEPS = 3
DT = 0.15
MESH = pl.DeviceIdType.MESH
F32 = jnp.float32

R = 2
LO, HI = 0, 1
(WIDE, HALF_A, ISV, GB, GZ, DM, CZU, CZD, CXP, CXM, CYU, CYD, C0) = range(13)
NCOEF = 13


def lanes(shape):
    return lax.broadcasted_iota(jnp.int32, shape, len(shape) - 1)


def subs(shape):
    return lax.broadcasted_iota(jnp.int32, shape, len(shape) - 2)


def spread_row(row):
    return jnp.broadcast_to(row, (8, 128))


def roll(x, shift, axis):
    return pltpu.roll(x, shift % x.shape[axis], axis)


class Fine:
    n = 16
    key = "f"

    @staticmethod
    def load(ref, i, r):
        parts = [ref[pl.ds(16 * i + t, 8 * r, stride=2), :].reshape(1, r, 8, 128) for t in (0, 1)]
        return jnp.concatenate(parts, axis=0)

    @staticmethod
    def store(ref, i, r, value):
        for t in (0, 1):
            ref[pl.ds(16 * i + t, 8 * r, stride=2), :] = value[t].reshape(8 * r, 128)

    @staticmethod
    def k_up(x, last=None):
        moved = roll(x, -1, 3)
        edge = x if last is None else last
        return jnp.where(lanes(x.shape) == 127, edge, moved)

    @staticmethod
    def k_down(x, first=None):
        moved = roll(x, 1, 3)
        edge = x if first is None else first
        return jnp.where(lanes(x.shape) == 0, edge, moved)

    @staticmethod
    def edge_scale(shape):
        k = lanes(shape)
        return jnp.where((k == 0) | (k == 127), 1.0, 0.5).astype(F32)

    @staticmethod
    def row_of(ref, i, r):
        return jnp.concatenate(
            [spread_row(ref[pl.ds(i + m, 1), :]).reshape(1, 8, 128) for m in range(r)], axis=0
        )

    @staticmethod
    def j_up(x, halo):
        s = subs(x.shape[1:])
        moved = jnp.where(s == 7, halo, roll(x[0], -1, 1))
        return jnp.stack([x[1], moved])

    @staticmethod
    def j_down(x, halo):
        s = subs(x.shape[1:])
        moved = jnp.where(s == 0, halo, roll(x[1], 1, 1))
        return jnp.stack([moved, x[0]])

    @staticmethod
    def plane(ref, j):
        return jnp.concatenate([ref[pl.ds(j + 128 * h, 8, stride=16), :] for h in (0, 1)], axis=0)

    @staticmethod
    def plane_k_up(x):
        return jnp.where(lanes(x.shape) == 127, x, roll(x, -1, 1))

    @staticmethod
    def plane_k_down(x):
        return jnp.where(lanes(x.shape) == 0, x, roll(x, 1, 1))

    @staticmethod
    def corner_plane(tile_ref, comp):
        row = spread_row(tile_ref[comp])
        return jnp.concatenate([row, row], axis=0)

    @staticmethod
    def corner_row(tile_ref, comp):
        return spread_row(tile_ref[comp]).reshape(1, 8, 128)


class Coarse:
    n = 8
    key = "c"

    @staticmethod
    def load(ref, i, r):
        return ref[:, pl.ds(8 * i, 8 * r), :].reshape(2, r, 8, 128)

    @staticmethod
    def store(ref, i, r, value):
        ref[:, pl.ds(8 * i, 8 * r), :] = value.reshape(2, 8 * r, 128)

    @staticmethod
    def k_up(x, last=None):
        moved = roll(x, -1, 3)
        edge = x[1] if last is None else last
        return jnp.where(lanes(x.shape) == 127, jnp.stack([moved[1], edge]), moved)

    @staticmethod
    def k_down(x, first=None):
        moved = roll(x, 1, 3)
        edge = x[0] if first is None else first
        return jnp.where(lanes(x.shape) == 0, jnp.stack([edge, moved[0]]), moved)

    @staticmethod
    def edge_scale(shape):
        k = lanes(shape)
        half = lax.broadcasted_iota(jnp.int32, shape, 0)
        ends = ((k == 0) & (half == 0)) | ((k == 127) & (half == 1))
        return jnp.where(ends, 1.0, 0.5).astype(F32)

    @staticmethod
    def row_of(ref, i, r):
        halves = []
        for h in (0, 1):
            rows = [spread_row(ref[h, pl.ds(i + m, 1), :]).reshape(1, 8, 128) for m in range(r)]
            halves.append(jnp.concatenate(rows, axis=0))
        return jnp.stack(halves)

    @staticmethod
    def j_up(x, halo):
        return jnp.where(subs(x.shape) == 7, halo, roll(x, -1, 2))

    @staticmethod
    def j_down(x, halo):
        return jnp.where(subs(x.shape) == 0, halo, roll(x, 1, 2))

    @staticmethod
    def plane(ref, j):
        return jnp.stack([ref[h, pl.ds(j, 8, stride=8), :] for h in (0, 1)])

    @staticmethod
    def plane_k_up(x):
        return Coarse.k_up(x[:, None])[:, 0]

    @staticmethod
    def plane_k_down(x):
        return Coarse.k_down(x[:, None])[:, 0]

    @staticmethod
    def corner_plane(tile_ref, comp):
        return jnp.stack([spread_row(tile_ref[2 * comp + h]) for h in (0, 1)])

    @staticmethod
    def corner_row(tile_ref, comp):
        rows = [spread_row(tile_ref[2 * comp + h]) for h in (0, 1)]
        return jnp.stack(rows)[:, None]


def plane_roll(level, x, shift):
    return roll(x, shift, 0) if level is Fine else roll(x, shift, 1)


def plane_sub(level, x):
    return subs(x.shape)


def neighbour_rows(level, ref, i, r, step, halo):
    if step > 0:
        if i + r < level.n:
            return level.load(ref, i + 1, r)
        return halo() if r == 1 else jnp.concatenate([level.load(ref, i + 1, r - 1), halo()], axis=1)
    if i > 0:
        return level.load(ref, i - 1, r)
    return halo() if r == 1 else jnp.concatenate([halo(), level.load(ref, 0, r - 1)], axis=1)


def kernel(nx, ny, group_x, *refs):
    names_in = ["fine_disp", "fine_prev", "coarse_disp", "coarse_prev"]
    for name in ("fine", "coarse"):
        names_in += [name + part for part in ("_density", "_lame", "_rigidity", "_metric")]
    hbm = dict(zip(names_in, refs[:12]))
    offsets_hbm = refs[12]
    fine_out, coarse_out, energy_out = refs[13:16]
    (
        uf, uc, matf, matc, kf, kc, dvf, dvc, dyf, dyc,
        xhf, xhc, yhf, yhc, ysf, ysc, xmf, xmc, ymf, ymc, ysmf, ysmc,
        pls, plx, ply, pex, ccs, ccr, fcs, fcr, sized, offsets_ref, weights, ghost, eacc, erow, er1, er2,
        load_sem, send_sem, recv_sem, esend, erecv, line_sem, plane_sem,
    ) = refs[16:]

    gx, gy = lax.axis_index("gx"), lax.axis_index("gy")
    exists = {
        (dx, dy): functools.reduce(
            jnp.logical_and,
            ([gx > 0] if dx < 0 else [gx < nx - 1] if dx > 0 else [])
            + ([gy > 0] if dy < 0 else [gy < ny - 1] if dy > 0 else []),
        )
        for dx, dy in ((-1, 0), (1, 0), (-1, -1), (-1, 1), (1, -1), (1, 1), (0, -1), (0, 1))
    }
    directions = list(exists)
    corners = [d for d in directions if d[0] and d[1]]
    corner_id = {d: n for n, d in enumerate(corners)}

    def flag(direction):
        return jnp.where(exists[direction], 1.0, 0.0).astype(F32)

    def device(direction):
        return {"gx": gx + direction[0], "gy": gy + direction[1]}

    groups, half = nx // group_x, ny // 2
    gx_hi, gx_lo = gx // group_x, gx % group_x
    chip_y, second = gy // 2, gy % 2 == 1
    first_core = jnp.logical_not(second)
    n1, n2 = group_x * ny, groups
    me1 = gx_lo * ny + gy
    plane_x = [gx_hi * group_x + lax.rem(gx_lo + a, group_x) for a in range(group_x)]
    plane_y = [2 * lax.rem(chip_y + b, half) for b in range(half)]
    line_x = [lax.rem(gx_hi + d, n2) * group_x + gx_lo for d in range(n2)]

    def start_load(name, dst, sem):
        src = hbm[name]
        if name.startswith("fine"):
            pltpu.make_async_copy(src, dst, load_sem.at[sem]).start()
            return
        lead = (slice(None),) * (len(src.shape) - 2)
        for h in (0, 1):
            pltpu.make_async_copy(
                src.at[lead + (slice(None), pl.ds(128 * h, 128))],
                dst.at[(slice(None), h) if lead else (h,)],
                load_sem.at[sem],
            ).start()

    plan = [
        ("fine_disp", uf.at[1], 0), ("coarse_disp", uc.at[1], 1),
        ("fine_rigidity", matf.at[0], 0), ("coarse_rigidity", matc.at[0], 1),
        ("fine_metric", matf.at[1], 0), ("coarse_metric", matc.at[1], 1),
        ("fine_density", matf.at[2], 2), ("fine_lame", matf.at[3], 2),
        ("coarse_density", matc.at[2], 3), ("coarse_lame", matc.at[3], 3),
        ("fine_prev", uf.at[0], 4), ("coarse_prev", uc.at[0], 5),
    ]
    for entry in plan:
        start_load(*entry)
    offsets_load = pltpu.make_async_copy(offsets_hbm, offsets_ref, load_sem.at[6])
    offsets_load.start()
    load_sizes = (kf.at[pl.ds(0, 5)], kc.at[pl.ds(0, 5)], kf.at[pl.ds(0, 2)], kc.at[pl.ds(0, 2)],
                  kf.at[pl.ds(0, 3)], kc.at[pl.ds(0, 3)])

    def wait_load(*sems):
        for sem in sems:
            pltpu.make_async_copy(load_sizes[sem], load_sizes[sem], load_sem.at[sem]).wait()

    barrier = pltpu.get_barrier_semaphore()

    def greet(where):
        pl.semaphore_signal(barrier, inc=1, device_id=where, device_id_type=MESH)

    far_first = sorted(range(1, n2), key=lambda d: -min(d, n2 - d))
    by_one = sorted({1, n2 - 1}) if n2 > 1 else []
    by_two = sorted({2, n2 - 2}) if n2 > 3 else []
    for d in by_one:
        greet({"gx": line_x[d], "gy": 2 * chip_y + 1})
    for d in directions:
        @pl.when(exists[d])
        def _(d=d):
            greet(device(d))

    side_of = {-1: LO, 1: HI}

    def messages(s):
        out = []
        u_f, u_c = uf.at[s + 1], uc.at[s + 1]
        for dx in (-1, 1):
            own, far = side_of[dx], side_of[-dx]
            first, second = (0, 1) if dx < 0 else (15, 14)
            out.append(("fx", (dx, 0), u_f.at[:, pl.ds(16 * first, 16)], xhf.at[s, far, pl.ds(0, 3)]))
            out.append(("fx", (dx, 0), u_f.at[0, pl.ds(16 * second, 16)], xhf.at[s, far, 3]))
            first, second = (0, 1) if dx < 0 else (7, 6)
            out.append(("cx", (dx, 0), u_c.at[:, :, pl.ds(8 * first, 8)], xhc.at[s, far, pl.ds(0, 3)]))
            out.append(("cx", (dx, 0), u_c.at[0, :, pl.ds(8 * second, 8)], xhc.at[s, far, 3]))
            out.append(("cp", (dx, 0), pex.at[s], plx.at[s, far]))
            if s == 0:
                first = 0 if dx < 0 else 15
                out.append(("mfx", (dx, 0), matf.at[pl.ds(0, 2), pl.ds(16 * first, 16)], xmf.at[far]))
                first = 0 if dx < 0 else 7
                out.append(("mcx", (dx, 0), matc.at[pl.ds(0, 2), :, pl.ds(8 * first, 8)], xmc.at[far]))
        for dy in (-1, 1):
            own, far = side_of[dy], side_of[-dy]
            out.append(("fy", (0, dy), ysf.at[s, own], yhf.at[s, far]))
            out.append(("cy", (0, dy), ysc.at[s, own], yhc.at[s, far]))
            out.append(("cq", (0, dy), pls.at[s], ply.at[s, far]))
            if s == 0:
                out.append(("mfy", (0, dy), ysmf.at[own], ymf.at[far]))
                out.append(("mcy", (0, dy), ysmc.at[own], ymc.at[far]))
        for d in corners:
            back = corner_id[(-d[0], -d[1])]
            out.append(("co", d, ccs.at[s, corner_id[d]], ccr.at[s, back]))
            out.append(("fo", d, fcs.at[s, corner_id[d]], fcr.at[s, back]))
        return out

    wait_with = {"mfx": "fx", "mcx": "cx", "cq": "fy", "mfy": "fy", "mcy": "cy"}
    slots, copies, arriving, leaving = {}, [], [], dict.fromkeys(directions, 0)
    for s in range(STEPS):
        entries, rows_of = [], {}
        for group, d, src, dst in messages(s):
            name = wait_with.get(group, group)
            key = (s if name == "cp" else s % 2, name, d)
            slot = slots.setdefault(key, len(slots))
            rows = math.prod(src.shape) // 128
            rows_of[key] = rows_of.get(key, 0) + rows
            leaving[d] += rows

            def copy(src=src, dst=dst, slot=slot, d=d):
                return pltpu.make_async_remote_copy(
                    src_ref=src, dst_ref=dst,
                    send_sem=send_sem.at[directions.index(d)], recv_sem=recv_sem.at[slot],
                    device_id=device(d), device_id_type=MESH,
                )

            entries.append((group, d, copy))
        copies.append(entries)
        arriving.append(rows_of)

    def bytes_of(rows, d, slot):
        part = sized.at[pl.ds(0, rows)]
        return pltpu.make_async_remote_copy(
            src_ref=part, dst_ref=part,
            send_sem=send_sem.at[directions.index(d)], recv_sem=recv_sem.at[slot],
            device_id=device(d), device_id_type=MESH,
        )

    def send(s, *wanted, dx=None):
        for d in directions:
            mine = [c for g, e, c in copies[s] if g in wanted and e == d]
            if mine and dx in (None, d[0]):
                @pl.when(exists[d])
                def _(mine=mine):
                    for c in mine:
                        c().start()

    def receive(s, *wanted, side=None):
        for d in directions:
            mine = [k for k in arriving[s] if k[1] in wanted and k[2] == d]
            if mine and (side is None or d[0] == -side):
                @pl.when(exists[(-d[0], -d[1])])
                def _(mine=mine, d=d):
                    for k in mine:
                        bytes_of(arriving[s][k], d, slots[k]).wait_recv()

    def round_signals(stage):
        away = 2 << stage
        for side, ok, to in ((LO, gy + away < ny, gy + away), (HI, gy >= away, gy - away)):
            if ny > 5:
                @pl.when(ok)
                def _(side=side, to=to):
                    pl.semaphore_signal(
                        plane_sem.at[stage, side], inc=1,
                        device_id={"gx": gx, "gy": to}, device_id_type=MESH,
                    )
        if n2 > 3:
            @pl.when(second)
            def _():
                for m, d in enumerate((by_one, by_two)[stage]):
                    pl.semaphore_signal(
                        line_sem.at[stage, m], inc=1,
                        device_id={"gx": line_x[d], "gy": gy}, device_id_type=MESH,
                    )

    def round_wait(stage):
        away = 2 << stage
        for side, ok in ((LO, gy >= away), (HI, gy + away < ny)):
            if ny > 5:
                @pl.when(ok)
                def _(side=side):
                    pl.semaphore_wait(plane_sem.at[stage, side], 1)
        if n2 > 3:
            @pl.when(second)
            def _():
                for m in range(len((by_one, by_two)[stage])):
                    pl.semaphore_wait(line_sem.at[stage, m], 1)

    def pack_y(level, s):
        u, out = (uf, ysf) if level is Fine else (uc, ysc)
        last = 15 if level is Fine else 7
        for side, (j0, j1) in ((LO, (0, 1)), (HI, (last, last - 1))):
            for c in range(3):
                out[s, side, c] = level.plane(u.at[s + 1, c], j0)
            out[s, side, 3] = level.plane(u.at[s + 1, 1], j1)

    def plane_tile(s, tile, rows):
        lane = lanes((8, 128))
        for c in range(3):
            for i in rows:
                column = uc[s + 1, c, 0, pl.ds(8 * i, 8), 0:1]
                at = 16 * c + 2 * i
                tile = jnp.where((lane == at) | (lane == at + 1), column, tile)
        return tile

    def pack_coarse_corners(s, side):
        for (dx, dy), n in corner_id.items():
            if dx != side:
                continue
            ci, cj = (0 if dx < 0 else 7), (0 if dy < 0 else 7)
            for c in (0, 1):
                for h in (0, 1):
                    ccs[s, n, 2 * c + h] = uc[s + 1, c, h, pl.ds(8 * ci + cj, 1), :]

    def pack_plane(s):
        edge = plane_tile(s, jnp.zeros((8, 128), F32), (0, 1, 7))
        pex[s] = edge
        pls[s] = plane_tile(s, edge, range(2, 7))
        for (dx, dy), n in corner_id.items():
            for m, j in enumerate((0, 1) if dy < 0 else (7, 7)):
                fcs[s, n, 2 + m] = edge[j : j + 1]

    def pack_corners(s, side):
        for (dx, dy), n in corner_id.items():
            if dx != side:
                continue
            fi, fj = (0 if dx < 0 else 15), (0 if dy < 0 else 15)
            for c in (0, 1):
                fcs[s, n, c] = uf[s + 1, c, pl.ds(16 * fi + fj, 1), :]

    for dx in (-1, 1):
        @pl.when(jnp.logical_not(exists[(dx, 0)]))
        def _(side=side_of[dx]):
            for s in range(STEPS):
                xhf[s, side] = jnp.zeros(xhf.shape[2:], F32)
                xhc[s, side] = jnp.zeros(xhc.shape[2:], F32)
                plx[s, side] = jnp.zeros((8, 128), F32)
            xmf[side, 0] = jnp.zeros(xmf.shape[2:], F32)
            xmf[side, 1] = jnp.ones(xmf.shape[2:], F32)
            xmc[side, 0] = jnp.zeros(xmc.shape[2:], F32)
            xmc[side, 1] = jnp.ones(xmc.shape[2:], F32)
    for dy in (-1, 1):
        @pl.when(jnp.logical_not(exists[(0, dy)]))
        def _(side=side_of[dy]):
            for s in range(STEPS):
                yhf[s, side] = jnp.zeros(yhf.shape[2:], F32)
                yhc[s, side] = jnp.zeros(yhc.shape[2:], F32)
                ply[s, side] = jnp.zeros((8, 128), F32)
            ymf[side, 0] = jnp.zeros(ymf.shape[2:], F32)
            ymf[side, 1] = jnp.ones(ymf.shape[2:], F32)
            ymc[side, 0] = jnp.zeros(ymc.shape[2:], F32)
            ymc[side, 1] = jnp.ones(ymc.shape[2:], F32)
    for d in corners:
        @pl.when(jnp.logical_not(exists[d]))
        def _(n=corner_id[d]):
            for s in range(STEPS):
                ccr[s, n] = jnp.zeros(ccr.shape[2:], F32)
                fcr[s, n] = jnp.zeros(fcr.shape[2:], F32)

    wait_load(0, 1)
    for c in (0, 1):
        for side, jf, jc in ((LO, 0, 0), (HI, 15, 7)):
            ysmf[side, c] = Fine.plane(matf.at[c], jf)
            ysmc[side, c] = Coarse.plane(matc.at[c], jc)
    pack_y(Fine, 0)
    pack_y(Coarse, 0)
    for dx in (-1, 1):
        pack_coarse_corners(0, dx)
        pack_corners(0, dx)
    pack_plane(0)

    greeted = jnp.where(second, 2 * len(by_one), 0).astype(jnp.int32)
    for d in directions:
        greeted = greeted + jnp.where(exists[d], 1, 0).astype(jnp.int32)
    pl.semaphore_wait(barrier, greeted)

    def send_first_x():
        send(0, "cx", "mcx")
        send(0, "cp", "fx", "mfx")

    send(0, "co", "fo")

    @pl.when(first_core)
    def _():
        send_first_x()

    send(0, "cy", "mcy", "cq", "fy", "mfy")

    wait_load(2, 3)
    offsets_load.wait()
    lane8 = lanes((8, 128))
    spread = jnp.where(
        (lanes((16, 128)) % 16 == subs((16, 128))) & (lanes((16, 128)) < 48), 1.0, 0.0
    ).astype(F32)
    for t in (0, 1):
        pick = jnp.where(lanes((8, 16)) == 2 * subs((8, 16)) + t, 1.0, 0.0).astype(F32)
        for axis in (0, 1):
            table = offsets_ref[axis].astype(F32)
            turned = lax.dot_general(
                pick, table, (((1,), (1,)), ((), ())), preferred_element_type=F32
            )
            shift = jnp.dot(turned, spread, preferred_element_type=F32)
            if axis == 0:
                near = jnp.where(lane8 % 2 == 0, 0.75, 0.25).astype(F32)
            else:
                near = jnp.full((8, 128), 0.75 if t == 0 else 0.25, F32)
            for m, value in enumerate((-1.0, 0.0, 1.0, 2.0)):
                weights[t, 4 * axis + m] = jnp.where(shift == value, near, 0.0) + jnp.where(
                    shift == value - 1.0, 1.0 - near, 0.0
                )

    levels = (
        (Coarse, uc, matc, kc, dvc, dyc, xhc, yhc, ysc, xmc, ymc),
        (Fine, uf, matf, kf, dvf, dyf, xhf, yhf, ysf, xmf, ymf),
    )
    for level, u, mat, k, dv, dy_, xh, yh, ys, xm, ym in levels:
        for i in range(0, level.n, R):
            rig, met, den, lam = (level.load(mat.at[m], i, R) for m in range(4))
            scale = level.edge_scale(rig.shape)
            inverse = 1.0 / met
            light = DT / den
            a = inverse * light
            vertical = rig * inverse
            b = (lam + rig) * light
            isv = inverse * scale
            half_a = 0.5 * a
            for slot, value in (
                (WIDE, rig * met), (HALF_A, half_a), (ISV, isv), (GB, 0.5 * b), (GZ, b * isv),
                (DM, den * met), (CZU, half_a * (vertical + level.k_up(vertical))),
                (CZD, half_a * (vertical + level.k_down(vertical))),
            ):
                level.store(k.at[slot], i, R, value)

    @pl.when(second)
    def _():
        send_first_x()

    def halo_row(level, ref):
        if level is Fine:
            return Fine.load(ref, 0, 1)
        return Coarse.load(ref, 0, 1)

    def side_coefficients(level, i, r, u, mat, k, dv, dy_, xh, yh, ys, xm, ym):
        w = level.load(k.at[WIDE], i, r)
        ha = level.load(k.at[HALF_A], i, r)

        def outer(side):
            return halo_row(level, xm.at[side, 0]) * halo_row(level, xm.at[side, 1])

        cxp = ha * (w + neighbour_rows(level, k.at[WIDE], i, r, 1, lambda: outer(HI)))
        cxm = ha * (w + neighbour_rows(level, k.at[WIDE], i, r, -1, lambda: outer(LO)))
        up = level.row_of(ym.at[HI, 0], i, r) * level.row_of(ym.at[HI, 1], i, r)
        down = level.row_of(ym.at[LO, 0], i, r) * level.row_of(ym.at[LO, 1], i, r)
        cyu = ha * (w + level.j_up(w, up))
        cyd = ha * (w + level.j_down(w, down))
        total = cxp + cxm + cyu + cyd + level.load(k.at[CZU], i, r) + level.load(k.at[CZD], i, r)
        for slot, value in ((CXP, cxp), (CXM, cxm), (CYU, cyu), (CYD, cyd), (C0, total)):
            level.store(k.at[slot], i, r, value)

    def inner_coefficients(level, *rest):
        for i, r in [(1, 1)] + [(i, R) for i in range(2, level.n - 2, R)] + [(level.n - 2, 1)]:
            side_coefficients(level, i, r, *rest)

    def row_divergence(s, i, r, level, u, mat, k, dv, dy_, xh, yh, ys, xm, ym):
        now = u.at[s + 1]

        def halo(side):
            return lambda: halo_row(level, xh.at[s, side, 0])

        px = neighbour_rows(level, now.at[0], i, r, 1, halo(HI))
        mx = neighbour_rows(level, now.at[0], i, r, -1, halo(LO))
        y = level.load(now.at[1], i, r)
        z = level.load(now.at[2], i, r)
        py = level.j_up(y, level.row_of(yh.at[s, HI, 1], i, r))
        my = level.j_down(y, level.row_of(yh.at[s, LO, 1], i, r))
        isv = level.load(k.at[ISV], i, r)
        value = 0.5 * ((px - mx) + (py - my)) + isv * (level.k_up(z) - level.k_down(z))
        level.store(dv, i + 1, r, value)

    def x_side_divergence(s, dx, level, u, mat, k, dv, dy_, xh, yh, ys, xm, ym):
        cor = fcr if level is Fine else ccr
        now, n = u.at[s + 1], level.n
        side = side_of[dx]
        inside = level.load(now.at[0], 0 if dx < 0 else n - 1, 1)
        beyond = halo_row(level, xh.at[s, side, 3])
        y = halo_row(level, xh.at[s, side, 1])
        z = halo_row(level, xh.at[s, side, 2])
        py = level.j_up(y, level.corner_row(cor.at[s, corner_id[(dx, 1)]], 1))
        my = level.j_down(y, level.corner_row(cor.at[s, corner_id[(dx, -1)]], 1))
        isv = level.edge_scale(z.shape) / halo_row(level, xm.at[side, 1])
        along = (beyond - inside) if dx > 0 else (inside - beyond)
        value = 0.5 * (along + (py - my)) + isv * (level.k_up(z) - level.k_down(z))
        level.store(dv, 0 if dx < 0 else n + 1, 1, value * flag((dx, 0)))

    def y_side_divergence(s, known, level, u, mat, k, dv, dy_, xh, yh, ys, xm, ym):
        cor = fcr if level is Fine else ccr
        n = level.n
        for dy, side in side_of.items():
            x, z, beyond = yh[s, side, 0], yh[s, side, 2], yh[s, side, 3]
            inside = ys[s, side, 1]
            sub = plane_sub(level, x)
            px, mx = plane_roll(level, x, -1), plane_roll(level, x, 1)
            if 1 in known:
                px = jnp.where(sub == n - 1, level.corner_plane(cor.at[s, corner_id[(1, dy)]], 0), px)
            if -1 in known:
                mx = jnp.where(sub == 0, level.corner_plane(cor.at[s, corner_id[(-1, dy)]], 0), mx)
            isv = level.edge_scale(z.shape) / ym[side, 1]
            along = (beyond - inside) if dy > 0 else (inside - beyond)
            value = 0.5 * (along + (px - mx)) + isv * (level.plane_k_up(z) - level.plane_k_down(z))
            dy_[side] = value * flag((0, dy))

    def middle(s, level, *rest):
        n = level.n
        y_side_divergence(s, (), level, *rest)
        row_divergence(s, 1, 1, level, *rest)
        for i in range(2, n - 2, R):
            row_divergence(s, i, R, level, *rest)
        row_divergence(s, n - 2, 1, level, *rest)
        total = jnp.zeros((8, 128), F32)
        for i in range(R, first_outer(level), R):
            total = total + rates(s, i, level, *rest)
        return total

    def first_outer(level):
        return level.n - (4 if level is Fine else 2)

    def outer(s, dx, level, *rest):
        n = level.n
        x_side_divergence(s, dx, level, *rest)
        row_divergence(s, 0 if dx < 0 else n - 1, 1, level, *rest)
        return rates(s, 0 if dx < 0 else n - R, level, *rest)

    def fine_ghosts(s, known):
        sub, lane = subs((8, 128)), lanes((8, 128)) % 16

        def shifted_rows(tile, low, high0, high1):
            return [
                jnp.where(sub == 0, low, roll(tile, 1, 0)),
                tile,
                jnp.where(sub == 7, high0, roll(tile, -1, 0)),
                jnp.where(sub == 7, high1, jnp.where(sub == 6, high0, roll(tile, -2, 0))),
            ]

        def row(ref, j):
            return spread_row(ref[pl.ds(j, 1), :])

        def corner_rows(dx):
            low, high = fcr.at[s, corner_id[(dx, -1)]], fcr.at[s, corner_id[(dx, 1)]]
            return spread_row(low[2]), spread_row(high[2]), spread_row(high[3])

        own = shifted_rows(pls[s], row(ply.at[s, LO], 7), row(ply.at[s, HI], 0), row(ply.at[s, HI], 1))
        if -1 in known:
            left = shifted_rows(plx[s, LO], *corner_rows(-1))
        if 1 in known:
            right = shifted_rows(plx[s, HI], *corner_rows(1))
        totals = [jnp.zeros((8, 128), F32) for _ in (0, 1)]
        for mx in range(4):
            inner = [jnp.zeros((8, 128), F32) for _ in (0, 1)]
            for my in range(4):
                tile = roll(own[my], 2 - 2 * mx, 1) if mx != 1 else own[my]
                if mx == 0 and -1 in known:
                    tile = jnp.where(lane < 2, roll(left[my], -14, 1), tile)
                if mx >= 2 and 1 in known:
                    edge = 18 - 2 * mx
                    tile = jnp.where(lane >= edge, roll(right[my], edge, 1), tile)
                for t in (0, 1):
                    inner[t] = inner[t] + weights[t, 4 + my] * tile
            for t in (0, 1):
                totals[t] = totals[t] + weights[t, mx] * inner[t]
        for t in (0, 1):
            ghost[t] = totals[t]

    def fine_last(c, i):
        rows = []
        for t in (0, 1):
            tile = ghost[t]
            rows.append(jnp.stack([roll(tile, 127 - (16 * c + i + m), 1) for m in range(R)]))
        return jnp.stack(rows)

    def coarse_first(s, c, i):
        rows = []
        for m in range(R):
            base = 32 * (i + m)
            parts = [uf[s + 1, c, pl.ds(base + t, 8, stride=2), :] for t in (0, 1, 16, 17)]
            rows.append(0.25 * ((parts[0] + parts[1]) + (parts[2] + parts[3])))
        return roll(jnp.stack(rows), 1, 2)

    def rates(s, i, level, u, mat, k, dv, dy_, xh, yh, ys, xm, ym):
        now, old = u.at[s + 1], u.at[s]
        coef = {
            m: level.load(k.at[m], i, R) for m in (GB, GZ, DM, CZU, CZD, CXP, CXM, CYU, CYD, C0)
        }
        d_mid = level.load(dv, i + 1, R)
        gradient = [
            coef[GB] * (level.load(dv, i + 2, R) - level.load(dv, i, R)),
            coef[GB]
            * (
                level.j_up(d_mid, level.row_of(dy_.at[HI], i, R))
                - level.j_down(d_mid, level.row_of(dy_.at[LO], i, R))
            ),
            coef[GZ] * (level.k_up(d_mid) - level.k_down(d_mid)),
        ]
        energy = None
        for c in range(3):
            v = level.load(now.at[c], i, R)

            def halo(side, c=c):
                return lambda: halo_row(level, xh.at[s, side, c])

            px = neighbour_rows(level, now.at[c], i, R, 1, halo(HI))
            mx = neighbour_rows(level, now.at[c], i, R, -1, halo(LO))
            py = level.j_up(v, level.row_of(yh.at[s, HI, c], i, R))
            my = level.j_down(v, level.row_of(yh.at[s, LO, c], i, R))
            if level is Fine:
                pz, mz = level.k_up(v, fine_last(c, i)), level.k_down(v)
            else:
                pz = level.k_up(v, jnp.zeros_like(v[1]))
                mz = level.k_down(v, coarse_first(s, c, i))
            rate = (
                (coef[CXP] * px + coef[CXM] * mx)
                + (coef[CYU] * py + coef[CYD] * my)
                + (coef[CZU] * pz + coef[CZD] * mz)
                - coef[C0] * v
                + gradient[c]
            )
            after = (2.0 * v - level.load(old.at[c], i, R)) + rate
            if s < STEPS - 1:
                level.store(u.at[s + 2, c], i, R, after)
            elif level is Fine:
                level.store(fine_out.at[c], i, R, after)
            else:
                for h in (0, 1):
                    coarse_out[c, pl.ds(8 * i, 8 * R), pl.ds(128 * h, 128)] = after[h].reshape(
                        8 * R, 128
                    )
            change = after - v
            part = change * change - after * rate
            energy = part if energy is None else energy + part
        return jnp.sum(coef[DM] * energy, axis=(0, 1))

    coarse_set, fine_set = levels
    for s in range(STEPS):
        last = s == STEPS - 1
        receive(s, "cy")
        if s == 0:
            inner_coefficients(*coarse_set)
            wait_load(5)
        coarse_total = middle(s, *coarse_set)
        receive(s, "fy")
        if s == 0:
            inner_coefficients(*fine_set)
            wait_load(4)
        fine_ghosts(s, ())
        fine_total = middle(s, *fine_set)
        receive(s, "co")
        y_side_divergence(s, (-1, 1), *coarse_set)
        for dx in (-1, 1):
            receive(s, "cx", side=dx)
            if s == 0:
                side_coefficients(Coarse, 0 if dx < 0 else 7, 1, *coarse_set[1:])
            coarse_total = coarse_total + outer(s, dx, *coarse_set)
            if not last:
                pack_coarse_corners(s + 1, dx)
                send(s + 1, "co", dx=dx)
                send(s + 1, "cx", dx=dx)
        eacc[s, 1] = coarse_total
        if not last:
            pack_y(Coarse, s + 1)
            pack_plane(s + 1)
            send(s + 1, "cy", "cq", "cp")
        receive(s, "cp", "fo")
        fine_ghosts(s, (-1, 1))
        y_side_divergence(s, (-1, 1), *fine_set)
        fine_total = fine_total + rates(s, first_outer(Fine), *fine_set)
        for dx in (1, -1) if last else (-1, 1):
            receive(s, "fx", side=dx)
            if s == 0:
                side_coefficients(Fine, 0 if dx < 0 else 15, 1, *fine_set[1:])
            fine_total = fine_total + outer(s, dx, *fine_set)
            if not last:
                pack_corners(s + 1, dx)
                send(s + 1, "fo", dx=dx)
                send(s + 1, "fx", dx=dx)
        eacc[s, 0] = fine_total
        if not last:
            pack_y(Fine, s + 1)
            send(s + 1, "fy")
        if s == 0:
            round_signals(0)
        elif s == 1:
            round_wait(0)
            round_signals(1)
        else:
            round_wait(1)

    lane1 = lanes((1, 128))
    row = jnp.zeros((1, 128), F32)
    cells = (nx * ny * 16 * 16 * 128, nx * ny * 8 * 8 * 256)
    for s in range(STEPS):
        for m in (0, 1):
            value = jnp.sum(eacc[s, m], axis=0, keepdims=True)
            value = jnp.sum(value, axis=1, keepdims=True)
            row = jnp.where(lane1 == STEPS * m + s, value * (1.0 / cells[m]), row)
    erow[0] = row
    er1[me1] = row

    def rows(buffer, n, stage):
        part = buffer.at[pl.ds(0, n)]
        return pltpu.make_async_remote_copy(
            src_ref=part, dst_ref=part, send_sem=esend.at[stage], recv_sem=erecv.at[stage],
            device_id={"gx": line_x[0], "gy": gy}, device_id_type=MESH,
        )

    def pass_on(stage, slot, where):
        pltpu.make_async_remote_copy(
            src_ref=erow.at[stage], dst_ref=slot, send_sem=esend.at[stage],
            recv_sem=erecv.at[stage], device_id=where, device_id_type=MESH,
        ).start()

    for a in reversed(range(group_x)):
        for b in reversed(range(half)):
            if a or b:
                pass_on(0, er1.at[me1], {"gx": plane_x[a], "gy": plane_y[b] + 1})

    @pl.when(first_core)
    def _():
        pass_on(0, er1.at[me1], {"gx": gx, "gy": 2 * chip_y + 1})

    @pl.when(second)
    def _():
        rows(er1, n1 - 1, 0).wait_recv()
        plane = er1[0]
        for m in range(1, n1):
            plane = plane + er1[m]
        erow[1] = plane
        er2[gx_hi] = plane
        for d in far_first:
            for core in (0, 1):
                pass_on(1, er2.at[gx_hi], {"gx": line_x[d], "gy": 2 * chip_y + core})
        pass_on(1, er2.at[gx_hi], {"gx": gx, "gy": 2 * chip_y})
        if n2 > 1:
            rows(er2, n2 - 1, 1).wait_recv()

    @pl.when(first_core)
    def _():
        rows(er2, n2, 1).wait_recv()

    row = er2[0]
    for m in range(1, n2):
        row = row + er2[m]
    for m in (0, 1):
        energy_out[pl.ds(m, 1), :] = roll(row, -STEPS * m, 1)[:, 0:STEPS]

    @pl.when(second)
    def _():
        rows(er1, n1 // 2 - 1, 0).wait_send()
        rows(er1, 2 * n2 - 1, 1).wait_send()

    @pl.when(first_core)
    def _():
        rows(er1, n1 // 2, 0).wait_send()

    for d in directions:
        @pl.when(exists[d])
        def _(d=d):
            bytes_of(leaving[d], d, 0).wait_send()


def hand_out(*refs):
    pairs = [(refs[n].at[c], refs[3 + n].at[c]) for n in (0, 1) for c in range(3)]
    pairs.append((refs[2], refs[5]))
    copies = [pltpu.make_async_copy(a, b, refs[6].at[n]) for n, (a, b) in enumerate(pairs)]
    for c in copies:
        c.start()
    for c in copies:
        c.wait()


def per_device(nx, ny, group_x, *args):
    args = list(args)
    for m in range(4):
        shape = args[m].shape
        args[m] = args[m].reshape(shape[0], shape[1] * shape[2], shape[3])
    for m in range(4, 12):
        shape = args[m].shape
        args[m] = args[m].reshape(shape[0] * shape[1], shape[2])
    for m in range(13):
        args[m] = pltpu.with_memory_space_constraint(args[m], pltpu.HBM)
    vm, dma = pltpu.VMEM, pltpu.SemaphoreType.DMA
    n1, n2 = group_x * ny, nx // group_x
    scratch = [
        vm((STEPS + 1, 3, 256, 128), F32),
        vm((STEPS + 1, 3, 2, 64, 128), F32),
        vm((4, 256, 128), F32),
        vm((4, 2, 64, 128), F32),
        vm((NCOEF, 256, 128), F32),
        vm((NCOEF, 2, 64, 128), F32),
        vm((18 * 16, 128), F32),
        vm((2, 10 * 8, 128), F32),
        vm((2, 16, 128), F32),
        vm((2, 2, 8, 128), F32),
        vm((STEPS, 2, 4, 16, 128), F32),
        vm((STEPS, 2, 4, 2, 8, 128), F32),
        vm((STEPS, 2, 4, 16, 128), F32),
        vm((STEPS, 2, 4, 2, 8, 128), F32),
        vm((STEPS, 2, 4, 16, 128), F32),
        vm((STEPS, 2, 4, 2, 8, 128), F32),
        vm((2, 2, 16, 128), F32),
        vm((2, 2, 2, 8, 128), F32),
        vm((2, 2, 16, 128), F32),
        vm((2, 2, 2, 8, 128), F32),
        vm((2, 2, 16, 128), F32),
        vm((2, 2, 2, 8, 128), F32),
        vm((STEPS, 8, 128), F32),
        vm((STEPS, 2, 8, 128), F32),
        vm((STEPS, 2, 8, 128), F32),
        vm((STEPS, 8, 128), F32),
        vm((STEPS, 4, 4, 1, 128), F32),
        vm((STEPS, 4, 4, 1, 128), F32),
        vm((STEPS, 4, 4, 1, 128), F32),
        vm((STEPS, 4, 4, 1, 128), F32),
        vm((480, 128), F32),
        vm((2, 16, 16), jnp.int32),
        vm((2, 8, 8, 128), F32),
        vm((2, 8, 128), F32),
        vm((STEPS, 2, 8, 128), F32),
        vm((2, 1, 128), F32),
        vm((max(n1, 2 * n2), 1, 128), F32),
        vm((max(n2, 1), 1, 128), F32),
        dma((7,)),
        dma((8,)),
        dma((38,)),
        dma((2,)),
        dma((2,)),
        pltpu.SemaphoreType.REGULAR((2, 2)),
        pltpu.SemaphoreType.REGULAR((2, 2)),
    ]
    anywhere = pl.BlockSpec(memory_space=pltpu.HBM)
    in_vmem = pl.BlockSpec(memory_space=pltpu.VMEM)
    out_shape = (
        jax.ShapeDtypeStruct((3, 256, 128), F32),
        jax.ShapeDtypeStruct((3, 64, 256), F32),
        jax.ShapeDtypeStruct((2, STEPS), F32),
    )
    results = pl.pallas_call(
        functools.partial(kernel, nx, ny, group_x),
        out_shape=out_shape,
        in_specs=[anywhere] * 13,
        out_specs=(in_vmem, in_vmem, in_vmem),
        scratch_shapes=scratch,
        compiler_params=pltpu.CompilerParams(
            collective_id=0, has_side_effects=True, vmem_limit_bytes=32 << 20
        ),
        name="leapfrog",
    )(*args)
    fine, coarse, energy = pl.pallas_call(
        hand_out,
        out_shape=out_shape,
        in_specs=[in_vmem] * 3,
        out_specs=[anywhere] * 3,
        scratch_shapes=[dma((7,))],
        compiler_params=pltpu.CompilerParams(vmem_limit_bytes=1 << 20),
        name="hand_out",
    )(*results)
    energy = energy.T
    return fine.reshape(3, 16, 16, 128), coarse.reshape(3, 8, 8, 256), energy


def solution(mesh):
    nx, ny = mesh.shape["gx"], mesh.shape["gy"]
    group_x = next(m for m in (4, 2, 1) if nx % m == 0)
    field, cells = P(None, "gx", "gy", None), P("gx", "gy", None)
    return jax.shard_map(
        functools.partial(per_device, nx, ny, group_x),
        mesh=mesh,
        in_specs=(field,) * 4 + (cells,) * 8 + (P(None, "gx", "gy"),),
        out_specs=(field, field, P()),
        check_vma=False,
    )
```
